8 devices in a mesh: data: 1 (over z), expert: 8 (over y, x, core).
Axes of the slice: x: 2, y: 2, z: 1, core: 2. Of those that a mesh axis runs over, the one named last changes fastest.
Arguments:
- x_tokens: bfloat16 [512, 1024], P(('data', 'expert'))
- y_mid: bfloat16 [512, 1024], P(('data', 'expert'))
- dy_out: bfloat16 [512, 1024], P(('data', 'expert'))
- experts_one: int32 [512, 8], P(('data', 'expert'))
- gates_one: float32 [512, 8], P(('data', 'expert'))
- slots_one: int32 [512, 8], P(('data', 'expert'))
- experts_two: int32 [512, 8], P(('data', 'expert'))
- gates_two: float32 [512, 8], P(('data', 'expert'))
- slots_two: int32 [512, 8], P(('data', 'expert'))
- w_gate_one: bfloat16 [32, 1024, 512], P('expert')
- w_up_one: bfloat16 [32, 1024, 512], P('expert')
- w_down_one: bfloat16 [32, 512, 1024], P('expert')
- w_gate_two: bfloat16 [32, 1024, 512], P('expert')
- w_up_two: bfloat16 [32, 1024, 512], P('expert')
- w_down_two: bfloat16 [32, 512, 1024], P('expert')
Outputs:
- output 1: bfloat16 [512, 1024], P(('data', 'expert'))
- output 2: float32 [32, 1024, 512], P(('data', 'expert'))
- output 3: float32 [32, 1024, 512], P(('data', 'expert'))
- output 4: float32 [32, 512, 1024], P(('data', 'expert'))
- output 5: float32 [32, 1024, 512], P(('data', 'expert'))
- output 6: float32 [32, 1024, 512], P(('data', 'expert'))
- output 7: float32 [32, 512, 1024], P(('data', 'expert'))
All inputs are finite; a program needn't handle non-finite values.
Results may differ from the reference program's by a relative error of at most 0.0131849.
Values are sent between devices in bfloat16 or wider.
A program may use at most 1 GiB of HBM per device.

```python
import jax
import jax.numpy as jnp
from jax import lax

MODEL_DIM = 1024
FFN_DIM = 512
EXPERTS = 32
TOP_K = 8
TOKENS_DEV = 64
GROUP_SIZE = 8

TOKENS_PART = GROUP_SIZE * TOKENS_DEV
CAPACITY = 8 * ((3 * TOP_K * TOKENS_DEV + 16 * EXPERTS - 1) // (16 * EXPERTS))
TOTAL_ROWS = GROUP_SIZE * EXPERTS * CAPACITY


def draw_routing(key):
    key_noise, key_bias, key_hot = jax.random.split(key, 3)
    noise_int = jax.random.randint(key_noise, (TOKENS_PART, EXPERTS), 0, 4096)
    expert_bias = jax.random.randint(key_bias, (EXPERTS,), 0, 512)
    hot_expert = jax.random.randint(key_hot, (), 0, EXPERTS)
    expert_ids = jnp.arange(EXPERTS, dtype=jnp.int32)
    local_tok = jnp.arange(TOKENS_PART, dtype=jnp.int32) % TOKENS_DEV
    boost_int = jnp.where((local_tok[:, None] < CAPACITY) & (expert_ids[None, :] == hot_expert), 8192, 0)
    score_int = (noise_int + expert_bias[None, :] + boost_int) * EXPERTS + expert_ids[None, :]
    top_vals, experts = lax.top_k(score_int, TOP_K)
    flat_ids = experts.reshape(GROUP_SIZE, TOKENS_DEV * TOP_K)
    onehot = (flat_ids[:, :, None] == expert_ids[None, None, :]).astype(jnp.int32)
    slot_rank = jnp.sum((jnp.cumsum(onehot, axis=1) - 1) * onehot, axis=2)
    slots = jnp.where(slot_rank < CAPACITY, slot_rank, -1).reshape(TOKENS_PART, TOP_K)
    return experts.astype(jnp.int32), slots.astype(jnp.int32)


def draw_weight(key, shape, fan_in):
    return (jax.random.normal(key, shape, jnp.float32) * fan_in ** -0.5).astype(jnp.bfloat16)


def setup_inputs(seed: int = 0, part: int = 0) -> dict:
    key_part = jax.random.fold_in(jax.random.key(seed), part)
    keys = jax.random.split(key_part, 7)
    shared = jax.random.split(jax.random.key(seed + 1), 6)
    tok_shape = (TOKENS_PART, MODEL_DIM)
    route_shape = (TOKENS_PART, TOP_K)
    up_shape = (EXPERTS, MODEL_DIM, FFN_DIM)
    down_shape = (EXPERTS, FFN_DIM, MODEL_DIM)
    gate_scale = TOP_K ** -0.5
    experts_one, slots_one = draw_routing(keys[3])
    experts_two, slots_two = draw_routing(keys[4])
    return {
        "x_tokens": jax.random.normal(keys[0], tok_shape, jnp.float32).astype(jnp.bfloat16),
        "y_mid": jax.random.normal(keys[1], tok_shape, jnp.float32).astype(jnp.bfloat16),
        "dy_out": jax.random.normal(keys[2], tok_shape, jnp.float32).astype(jnp.bfloat16),
        "experts_one": experts_one,
        "gates_one": jax.random.uniform(keys[5], route_shape, jnp.float32, 0.5, 1.5) * gate_scale,
        "slots_one": slots_one,
        "experts_two": experts_two,
        "gates_two": jax.random.uniform(keys[6], route_shape, jnp.float32, 0.5, 1.5) * gate_scale,
        "slots_two": slots_two,
        "w_gate_one": draw_weight(shared[0], up_shape, MODEL_DIM),
        "w_up_one": draw_weight(shared[1], up_shape, MODEL_DIM),
        "w_down_one": draw_weight(shared[2], down_shape, FFN_DIM),
        "w_gate_two": draw_weight(shared[3], up_shape, MODEL_DIM),
        "w_up_two": draw_weight(shared[4], up_shape, MODEL_DIM),
        "w_down_two": draw_weight(shared[5], down_shape, FFN_DIM),
    }


def expert_grads(operands):
    x_rows, z_rows, w_gate, w_up, w_down = operands
    gate_act = jnp.dot(x_rows, w_gate, preferred_element_type=jnp.float32).astype(jnp.bfloat16).astype(jnp.float32)
    up_act = jnp.dot(x_rows, w_up, preferred_element_type=jnp.float32).astype(jnp.bfloat16).astype(jnp.float32)
    sig_gate = jax.nn.sigmoid(gate_act)
    silu_gate = gate_act * sig_gate
    hidden = (silu_gate * up_act).astype(jnp.bfloat16)
    d_hidden = jnp.dot(z_rows, w_down.T, preferred_element_type=jnp.float32)
    dw_down = jnp.dot(hidden.T, z_rows, preferred_element_type=jnp.float32)
    d_gate = (d_hidden * up_act * sig_gate * (1.0 + gate_act * (1.0 - sig_gate))).astype(jnp.bfloat16)
    d_up = (d_hidden * silu_gate).astype(jnp.bfloat16)
    dx_rows = (jnp.dot(d_gate, w_gate.T, preferred_element_type=jnp.float32) + jnp.dot(d_up, w_up.T, preferred_element_type=jnp.float32)).astype(jnp.bfloat16)
    dw_gate = jnp.dot(x_rows.T, d_gate, preferred_element_type=jnp.float32)
    dw_up = jnp.dot(x_rows.T, d_up, preferred_element_type=jnp.float32)
    return dx_rows, dw_gate, dw_up, dw_down


def layer_backward(inputs, cotangent, experts, gates, slots, w_gate, w_up, w_down):
    source = jnp.arange(TOKENS_PART, dtype=jnp.int32) // TOKENS_DEV
    target = jnp.where(slots >= 0, (source[:, None] * EXPERTS + experts) * CAPACITY + slots, TOTAL_ROWS).reshape(-1)
    x_copies = jnp.repeat(inputs, TOP_K, axis=0)
    z_copies = (gates[:, :, None] * cotangent[:, None, :].astype(jnp.float32)).astype(jnp.bfloat16).reshape(TOKENS_PART * TOP_K, MODEL_DIM)
    x_buffer = jnp.zeros((TOTAL_ROWS + 1, MODEL_DIM), jnp.bfloat16).at[target].add(x_copies)
    z_buffer = jnp.zeros((TOTAL_ROWS + 1, MODEL_DIM), jnp.bfloat16).at[target].add(z_copies)
    by_source = (GROUP_SIZE, EXPERTS, CAPACITY, MODEL_DIM)
    by_expert = (EXPERTS, GROUP_SIZE * CAPACITY, MODEL_DIM)
    x_rows = x_buffer[:TOTAL_ROWS].reshape(by_source).transpose(1, 0, 2, 3).reshape(by_expert)
    z_rows = z_buffer[:TOTAL_ROWS].reshape(by_source).transpose(1, 0, 2, 3).reshape(by_expert)
    dx_rows, dw_gate, dw_up, dw_down = lax.map(expert_grads, (x_rows, z_rows, w_gate, w_up, w_down))
    returned = dx_rows.reshape(EXPERTS, GROUP_SIZE, CAPACITY, MODEL_DIM).transpose(1, 0, 2, 3).reshape(TOTAL_ROWS, MODEL_DIM)
    returned = jnp.concatenate([returned, jnp.zeros((1, MODEL_DIM), jnp.bfloat16)], axis=0)
    per_copy = returned[target].reshape(TOKENS_PART, TOP_K, MODEL_DIM).astype(jnp.float32)
    return jnp.sum(per_copy, axis=1), dw_gate, dw_up, dw_down


def reference(x_tokens, y_mid, dy_out, experts_one, gates_one, slots_one, experts_two, gates_two, slots_two, w_gate_one, w_up_one, w_down_one, w_gate_two, w_up_two, w_down_two):
    grads_two = layer_backward(y_mid, dy_out, experts_two, gates_two, slots_two, w_gate_two, w_up_two, w_down_two)
    dy_mid = (dy_out.astype(jnp.float32) + grads_two[0]).astype(jnp.bfloat16)
    grads_one = layer_backward(x_tokens, dy_mid, experts_one, gates_one, slots_one, w_gate_one, w_up_one, w_down_one)
    dx_tokens = (dy_mid.astype(jnp.float32) + grads_one[0]).astype(jnp.bfloat16)
    return (dx_tokens, grads_one[1], grads_one[2], grads_one[3], grads_two[1], grads_two[2], grads_two[3])
```

```python
import functools
import jax
import jax.numpy as jnp
from jax import lax
from jax.experimental import pallas as pl
from jax.experimental.pallas import tpu as pltpu
from jax.sharding import PartitionSpec as P

MESH = pl.DeviceIdType.MESH
F32 = jnp.float32
BF16 = jnp.bfloat16

TOK = 64
CHIPS = 4
DEVS = 8
D = 1024
F = 512
E = 4
CAP = 24
PAIR = 2 * CAP
ROWS = CHIPS * PAIR
PROWS = E * PAIR
CH = 4
CW = D // CH
VMEM_LIMIT = 66_000_000

S_ROUTE, S_Y, S_DY, S_X, S_D1 = 0, 1, 2, 3, 4
N_STREAMS = S_D1 + CH


def nt_dot(a, b):
    return lax.dot_general(a, b, (((1,), (1,)), ((), ())), preferred_element_type=F32)


def tn_dot(a, b):
    return lax.dot_general(a, b, (((0,), (0,)), ((), ())), preferred_element_type=F32)


def nn_dot(a, b):
    return jnp.dot(a, b, preferred_element_type=F32)


def main_kernel(
    route_ref, x_ref, y_ref, dy_ref, w1b_hbm, w3b_hbm, w2b_hbm, w1a_hbm, w3a_hbm, w2a_hbm,
    dx_ref, xrb_hbm, zrb_hbm, hb_hbm, dab_hbm, dbb_hbm, xra_hbm, zra_hbm, ha_hbm, daa_hbm, dba_hbm,
    w_vm, route_g, y_g, dy_g, x_g, d1_g, d1_own,
    xr, zr, act_s, act_f, hid, da, db, dxp, perm, perm_t, gate,
    part, mate_recv, far_recv,
    w_sem, ag_send, ag_recv, rs_send, rs_recv, out_sem,
):
    me = lax.axis_index("expert")
    core = lax.rem(me, 2)
    xpos = lax.rem(me // 2, 2)
    ypos = me // 4
    chip = me // 2
    mate = me + 1 - 2 * core
    nx = me + 2 - 4 * xpos
    ny = me + 4 - 8 * ypos
    nd = ny + 2 - 4 * xpos
    far = (nx, ny, nd)

    def remote(src, dst, send, recv, dev):
        return pltpu.make_async_remote_copy(src_ref=src, dst_ref=dst, send_sem=send, recv_sem=recv, device_id={"expert": dev}, device_id_type=MESH)

    w_hbm = (w1b_hbm, w3b_hbm, w2b_hbm, w1a_hbm, w3a_hbm, w2a_hbm)

    def w_copy(i):
        return pltpu.make_async_copy(w_hbm[i], w_vm[i], w_sem.at[i])

    for i in range(3):
        w_copy(i).start()

    barrier = pltpu.get_barrier_semaphore()
    for dev in (mate,) + far:
        pl.semaphore_signal(barrier, inc=1, device_id={"expert": dev}, device_id_type=MESH)
    pl.semaphore_wait(barrier, 4)

    sends = []

    def ag_start(stream, src, buf):
        for k, dev in enumerate(far + (mate,)):
            c = remote(src, buf.at[me], ag_send.at[stream, k], ag_recv.at[stream, k], dev)
            c.start()
            sends.append(c)

    def ag_pass_on(stream, buf):
        for k, dev in enumerate(far):
            remote(buf.at[dev], buf.at[dev], ag_send.at[stream, k], ag_recv.at[stream, k], dev).wait_recv()
            c = remote(buf.at[dev], buf.at[dev], ag_send.at[stream, 4 + k], ag_recv.at[stream, 4 + k], mate)
            c.start()
            sends.append(c)

    def ag_finish(stream, buf):
        remote(buf.at[mate], buf.at[mate], ag_send.at[stream, 3], ag_recv.at[stream, 3], mate).wait_recv()
        for k, dev in enumerate(far):
            dev_mate = dev + 1 - 2 * core
            remote(buf.at[dev_mate], buf.at[dev_mate], ag_send.at[stream, 4 + k], ag_recv.at[stream, 4 + k], mate).wait_recv()

    ag_start(S_ROUTE, route_ref, route_g)
    ag_start(S_Y, y_ref, y_g)
    ag_start(S_DY, dy_ref, dy_g)
    ag_start(S_X, x_ref, x_g)
    for i in range(3, 6):
        w_copy(i).start()
    route_g[me] = route_ref[...]
    y_g[me] = y_ref[...]
    dy_g[me] = dy_ref[...]
    x_g[me] = x_ref[...]

    outs = []

    def out_start(src, dst):
        c = pltpu.make_async_copy(src, dst, out_sem.at[len(outs)])
        c.start()
        outs.append(c)

    def build_routes(layer):
        base = (me * PROWS).astype(F32)
        row_id = lax.broadcasted_iota(jnp.int32, (PROWS, 2 * TOK), 0).astype(F32)
        for p in range(CHIPS):
            target = jnp.maximum(route_g[2 * p, layer, 0:8, :], route_g[2 * p + 1, layer, 0:8, :]) - base
            gates = route_g[2 * p, layer, 8:16, :] + route_g[2 * p + 1, layer, 8:16, :]
            hit = jnp.zeros((PROWS, 2 * TOK), F32)
            gsum = jnp.zeros((PROWS, 2 * TOK), F32)
            for j in range(8):
                m = row_id == target[j : j + 1, :]
                hit = jnp.where(m, 1.0, hit)
                gsum = jnp.where(m, gates[j : j + 1, :], gsum)
            perm[p] = hit.astype(BF16)
            perm_t[p] = hit.T.astype(BF16)
            gate[p] = jnp.sum(gsum, axis=1, keepdims=True)

    def gather_rows(tokens, dst, layer, cols, gated):
        for p in range(CHIPS):
            got = nn_dot(perm[p], tokens(p))
            if gated:
                got = got * gate[p]
            got = got.astype(BF16)
            for e in range(E):
                dst[layer, e, p * PAIR : (p + 1) * PAIR, cols] = got[e * PAIR : (e + 1) * PAIR]

    def forward_expert(layer, e):
        w1, w3 = w_vm[3 * layer], w_vm[3 * layer + 1]
        rows = xr[layer, e]
        a = nn_dot(rows, w1[e]).astype(BF16).astype(F32)
        b = nn_dot(rows, w3[e]).astype(BF16).astype(F32)
        sig = jax.nn.sigmoid(a)
        s = a * sig
        act_s[e] = s
        act_f[e] = b * (sig * (1.0 + a * (1.0 - sig)))
        hid[layer, e] = (s * b).astype(BF16)

    def hidden_grads(layer):
        w2 = w_vm[3 * layer + 2]

        @pl.loop(0, E)
        def _(e):
            dh = nt_dot(zr[layer, e], w2[e])
            da[layer, e] = (dh * act_f[e]).astype(BF16)
            db[layer, e] = (dh * act_s[e]).astype(BF16)

    def row_chunk(layer, k):
        w1, w3 = w_vm[3 * layer], w_vm[3 * layer + 1]
        cols = slice(k * CW, (k + 1) * CW)

        @pl.loop(0, E)
        def _(e):
            g = nt_dot(da[layer, e], w1[e, cols, :]) + nt_dot(db[layer, e], w3[e, cols, :])
            g = g.astype(BF16)
            for p in range(CHIPS):
                dxp[k % 2, p, e] = g[p * PAIR : (p + 1) * PAIR]

        for p in range(CHIPS):
            r = nn_dot(perm_t[p], dxp[k % 2, p].reshape(PROWS, CW))
            part[layer, k, 0, p] = r[:TOK]
            part[layer, k, 1, p] = r[TOK:]
        c = mate_copy(layer, k)
        c.start()
        sends.append(c)

    def mate_copy(layer, k):
        return remote(part.at[layer, k, 1 - core], mate_recv.at[layer, k], rs_send.at[layer, k, 3], rs_recv.at[layer, k, 3], mate)

    def far_copy(layer, k, i):
        dev = far[i]
        return remote(part.at[layer, k, core, dev // 2], far_recv.at[layer, k, i], rs_send.at[layer, k, i], rs_recv.at[layer, k, i], dev)

    def mate_sum(layer, k):
        mate_copy(layer, k).wait_recv()
        for p in range(CHIPS):
            part[layer, k, core, p] = part[layer, k, core, p] + mate_recv[layer, k, p]
        for i in range(3):
            c = far_copy(layer, k, i)
            c.start()
            sends.append(c)

    def far_sum(layer, k):
        for i in range(3):
            far_copy(layer, k, i).wait_recv()
        return part[layer, k, core, chip] + (far_recv[layer, k, 0] + far_recv[layer, k, 1] + far_recv[layer, k, 2])

    def pair_of(buf, p):
        return buf[2 * p : 2 * p + 2].reshape(2 * TOK, buf.shape[-1])

    ag_pass_on(S_ROUTE, route_g)
    ag_finish(S_ROUTE, route_g)
    build_routes(0)
    ag_pass_on(S_Y, y_g)
    ag_finish(S_Y, y_g)
    gather_rows(lambda p: pair_of(y_g, p), xr, 0, slice(None), False)
    out_start(xr.at[0], xrb_hbm)
    w_copy(0).wait()
    w_copy(1).wait()

    @pl.loop(0, E)
    def _(e):
        forward_expert(0, e)

    out_start(hid.at[0], hb_hbm)
    ag_pass_on(S_DY, dy_g)
    ag_finish(S_DY, dy_g)
    gather_rows(lambda p: pair_of(dy_g, p), zr, 0, slice(None), True)
    out_start(zr.at[0], zrb_hbm)
    w_copy(2).wait()
    hidden_grads(0)
    out_start(da.at[0], dab_hbm)
    out_start(db.at[0], dbb_hbm)
    for k in range(CH):
        row_chunk(0, k)
        if k >= 1:
            mate_sum(0, k - 1)
    mate_sum(0, CH - 1)

    ag_pass_on(S_X, x_g)
    build_routes(1)
    ag_finish(S_X, x_g)
    gather_rows(lambda p: pair_of(x_g, p), xr, 1, slice(None), False)
    out_start(xr.at[1], xra_hbm)
    for i in range(3, 6):
        w_copy(i).wait()

    def mid_grad(k):
        cols = slice(k * CW, (k + 1) * CW)
        mine = (dy_ref[:, cols].astype(F32) + far_sum(0, k)).astype(BF16)
        d1_own[k] = mine
        d1_g[k, me] = mine
        ag_start(S_D1 + k, d1_own.at[k], d1_g.at[k])

    for k in range(CH):
        forward_expert(1, k)
        mid_grad(k)
    out_start(hid.at[1], ha_hbm)
    for k in range(CH):
        ag_pass_on(S_D1 + k, d1_g.at[k])
    for k in range(CH):
        ag_finish(S_D1 + k, d1_g.at[k])
        gather_rows(lambda p: d1_g[k, 2 * p : 2 * p + 2].reshape(2 * TOK, CW), zr, 1, slice(k * CW, (k + 1) * CW), True)
    out_start(zr.at[1], zra_hbm)
    hidden_grads(1)
    out_start(da.at[1], daa_hbm)
    out_start(db.at[1], dba_hbm)
    for k in range(CH):
        row_chunk(1, k)
        if k >= 1:
            mate_sum(1, k - 1)
    mate_sum(1, CH - 1)
    for k in range(CH):
        dx_ref[:, k * CW : (k + 1) * CW] = (d1_own[k].astype(F32) + far_sum(1, k)).astype(BF16)
    for c in sends:
        c.wait_send()
    for c in outs:
        c.wait()


def main_call(route, x, y, dy, weights_two, weights_one):
    vm = pl.BlockSpec(memory_space=pltpu.VMEM)
    hbm = pl.BlockSpec(memory_space=pl.ANY)
    rows_d = jax.ShapeDtypeStruct((E, ROWS, D), BF16)
    rows_f = jax.ShapeDtypeStruct((E, ROWS, F), BF16)
    saved = (rows_d, rows_d, rows_f, rows_f, rows_f)
    w_up = pltpu.VMEM((E, D, F), BF16)
    w_dn = pltpu.VMEM((E, F, D), BF16)
    dma = pltpu.SemaphoreType.DMA
    return pl.pallas_call(
        main_kernel,
        out_shape=(jax.ShapeDtypeStruct((TOK, D), BF16),) + saved + saved,
        in_specs=[vm] * 4 + [hbm] * 6,
        out_specs=(vm,) + (hbm,) * 10,
        scratch_shapes=[
            (w_up, w_up, w_dn, w_up, w_up, w_dn),
            pltpu.VMEM((DEVS, 2, 16, 2 * TOK), F32),
            pltpu.VMEM((DEVS, TOK, D), BF16),
            pltpu.VMEM((DEVS, TOK, D), BF16),
            pltpu.VMEM((DEVS, TOK, D), BF16),
            pltpu.VMEM((CH, DEVS, TOK, CW), BF16),
            pltpu.VMEM((CH, TOK, CW), BF16),
            pltpu.VMEM((2, E, ROWS, D), BF16),
            pltpu.VMEM((2, E, ROWS, D), BF16),
            pltpu.VMEM((E, ROWS, F), F32),
            pltpu.VMEM((E, ROWS, F), F32),
            pltpu.VMEM((2, E, ROWS, F), BF16),
            pltpu.VMEM((2, E, ROWS, F), BF16),
            pltpu.VMEM((2, E, ROWS, F), BF16),
            pltpu.VMEM((2, CHIPS, E, PAIR, CW), BF16),
            pltpu.VMEM((CHIPS, PROWS, 2 * TOK), BF16),
            pltpu.VMEM((CHIPS, 2 * TOK, PROWS), BF16),
            pltpu.VMEM((CHIPS, PROWS, 1), F32),
            pltpu.VMEM((2, CH, 2, CHIPS, TOK, CW), F32),
            pltpu.VMEM((2, CH, CHIPS, TOK, CW), F32),
            pltpu.VMEM((2, CH, 3, TOK, CW), F32),
            dma((6,)),
            dma((N_STREAMS, 7)),
            dma((N_STREAMS, 7)),
            dma((2, CH, 4)),
            dma((2, CH, 4)),
            dma((10,)),
        ],
        compiler_params=pltpu.CompilerParams(collective_id=0, has_side_effects=True, vmem_limit_bytes=VMEM_LIMIT),
        name="moe_backward",
    )(route, x, y, dy, *weights_two, *weights_one)


def wgrad_kernel(x_ref, z_ref, h_ref, da_ref, db_ref, dw1_ref, dw3_ref, dw2_ref):
    x = x_ref[0]
    dw1_ref[0] = tn_dot(x, da_ref[0])
    dw3_ref[0] = tn_dot(x, db_ref[0])
    dw2_ref[0] = tn_dot(h_ref[0], z_ref[0])


def wgrad_call(xr, zr, hid, da, db, name):
    split = 2
    whole_d = pl.BlockSpec((1, ROWS, D), lambda e, j: (e, 0, 0))
    whole_f = pl.BlockSpec((1, ROWS, F), lambda e, j: (e, 0, 0))
    part_d = pl.BlockSpec((1, ROWS, D // split), lambda e, j: (e, 0, j))
    part_f = pl.BlockSpec((1, ROWS, F // split), lambda e, j: (e, 0, j))
    up = pl.BlockSpec((1, D // split, F), lambda e, j: (e, j, 0))
    dn = pl.BlockSpec((1, F // split, D), lambda e, j: (e, j, 0))
    return pl.pallas_call(
        wgrad_kernel,
        grid=(E, split),
        out_shape=(jax.ShapeDtypeStruct((E, D, F), F32), jax.ShapeDtypeStruct((E, D, F), F32), jax.ShapeDtypeStruct((E, F, D), F32)),
        in_specs=[part_d, whole_d, part_f, whole_f, whole_f],
        out_specs=(up, up, dn),
        compiler_params=pltpu.CompilerParams(vmem_limit_bytes=40_000_000),
        cost_estimate=pl.CostEstimate(flops=6 * E * ROWS * D * F, bytes_accessed=12 * E * D * F, transcendentals=0),
        name=name,
    )(xr, zr, hid, da, db)


def route_of(experts, gates, slots, core):
    code = jnp.where(slots >= 0, experts * PAIR + core * CAP + slots, -1).astype(F32).T
    gate = gates.T
    lane_core = lax.broadcasted_iota(jnp.int32, (8, 2 * TOK), 1) // TOK
    mine = lane_core == core
    code = jnp.where(mine, jnp.concatenate([code, code], axis=1), -1.0)
    gate = jnp.where(mine, jnp.concatenate([gate, gate], axis=1), 0.0)
    return jnp.concatenate([code, gate], axis=0)


def solution(mesh):
    tok_spec = P(("data", "expert"), None)
    weight_spec = P("expert", None, None)
    grad_spec = P(("data", "expert"), None, None)

    def local_step(x_tokens, y_mid, dy_out, experts_one, gates_one, slots_one, experts_two, gates_two, slots_two, w_gate_one, w_up_one, w_down_one, w_gate_two, w_up_two, w_down_two):
        core = lax.rem(lax.axis_index("expert"), 2)
        route = jnp.stack([route_of(experts_two, gates_two, slots_two, core), route_of(experts_one, gates_one, slots_one, core)])
        got = main_call(route, x_tokens, y_mid, dy_out, (w_gate_two, w_up_two, w_down_two), (w_gate_one, w_up_one, w_down_one))
        grads_two = wgrad_call(*got[1:6], "wgrad_two")
        grads_one = wgrad_call(*got[6:11], "wgrad_one")
        return (got[0],) + tuple(grads_one) + tuple(grads_two)

    return jax.shard_map(local_step, mesh=mesh, in_specs=(tok_spec,) * 9 + (weight_spec,) * 6, out_specs=(tok_spec,) + (grad_spec,) * 6, check_vma=False)
```

```python
import functools
import jax
import jax.numpy as jnp
from jax import lax
from jax.experimental import pallas as pl
from jax.experimental.pallas import tpu as pltpu
from jax.sharding import PartitionSpec as P

MESH = pl.DeviceIdType.MESH
scope = jax.named_scope
F32 = jnp.float32
BF16 = jnp.bfloat16

TOK = 64
CHIPS = 4
DEVS = 8
D = 1024
F = 512
E = 4
CAP = 24
PAIR = 2 * CAP
ROWS = CHIPS * PAIR
PROWS = E * PAIR
CH = 4
CW = D // CH
VMEM_LIMIT = 66_000_000

S_ROUTE, S_Y, S_DY, S_X, S_D1 = 0, 1, 2, 3, 4
N_STREAMS = S_D1 + CH


def nt_dot(a, b):
    return lax.dot_general(a, b, (((1,), (1,)), ((), ())), preferred_element_type=F32)


def tn_dot(a, b):
    return lax.dot_general(a, b, (((0,), (0,)), ((), ())), preferred_element_type=F32)


def nn_dot(a, b):
    return jnp.dot(a, b, preferred_element_type=F32)


def main_kernel(
    route_ref, x_ref, y_ref, dy_ref, w1b_hbm, w3b_hbm, w2b_hbm, w1a_hbm, w3a_hbm, w2a_hbm,
    own_hbm, d1_hbm, far0_hbm, far1_hbm, far2_hbm, xrb_hbm, zrb_hbm, hb_hbm, dab_hbm, dbb_hbm, xra_hbm, zra_hbm, ha_hbm, daa_hbm, dba_hbm,
    w_vm, route_g, y_g, dy_g, x_g, d1_g, d1_own,
    xr, zr, act_s, act_f, hid, da, db, dxp, perm, perm_t, gate,
    part, mate_recv, far_recv,
    w_sem, ag_send, ag_recv, rs_send, rs_recv, out_sem,
):
    me = lax.axis_index("expert")
    core = lax.rem(me, 2)
    xpos = lax.rem(me // 2, 2)
    ypos = me // 4
    chip = me // 2
    mate = me + 1 - 2 * core
    nx = me + 2 - 4 * xpos
    ny = me + 4 - 8 * ypos
    nd = ny + 2 - 4 * xpos
    far = (nx, ny, nd)

    def remote(src, dst, send, recv, dev):
        return pltpu.make_async_remote_copy(src_ref=src, dst_ref=dst, send_sem=send, recv_sem=recv, device_id={"expert": dev}, device_id_type=MESH)

    w_hbm = (w1b_hbm, w3b_hbm, w2b_hbm, w1a_hbm, w3a_hbm, w2a_hbm)

    def w_copy(i):
        return pltpu.make_async_copy(w_hbm[i], w_vm[i], w_sem.at[i])

    for i in range(3):
        w_copy(i).start()

    barrier = pltpu.get_barrier_semaphore()
    for dev in (mate,) + far:
        pl.semaphore_signal(barrier, inc=1, device_id={"expert": dev}, device_id_type=MESH)
    pl.semaphore_wait(barrier, 4)

    sends = []

    def ag_start(stream, src, buf):
        for k, dev in enumerate(far + (mate,)):
            c = remote(src, buf.at[me], ag_send.at[stream, k], ag_recv.at[stream, k], dev)
            c.start()
            sends.append(c)

    def ag_pass_on(stream, buf):
        for k, dev in enumerate(far):
            remote(buf.at[dev], buf.at[dev], ag_send.at[stream, k], ag_recv.at[stream, k], dev).wait_recv()
            c = remote(buf.at[dev], buf.at[dev], ag_send.at[stream, 4 + k], ag_recv.at[stream, 4 + k], mate)
            c.start()
            sends.append(c)

    def ag_finish(stream, buf):
        remote(buf.at[mate], buf.at[mate], ag_send.at[stream, 3], ag_recv.at[stream, 3], mate).wait_recv()
        for k, dev in enumerate(far):
            dev_mate = dev + 1 - 2 * core
            remote(buf.at[dev_mate], buf.at[dev_mate], ag_send.at[stream, 4 + k], ag_recv.at[stream, 4 + k], mate).wait_recv()

    ag_start(S_ROUTE, route_ref, route_g)
    ag_start(S_Y, y_ref, y_g)
    ag_start(S_DY, dy_ref, dy_g)
    ag_start(S_X, x_ref, x_g)
    for i in range(3, 6):
        w_copy(i).start()
    route_g[me] = route_ref[...]
    y_g[me] = y_ref[...]
    dy_g[me] = dy_ref[...]
    x_g[me] = x_ref[...]

    outs = []

    def out_start(src, dst):
        c = pltpu.make_async_copy(src, dst, out_sem.at[len(outs)])
        c.start()
        outs.append(c)

    def build_routes(layer):
        base = (me * PROWS).astype(F32)
        row_id = lax.broadcasted_iota(jnp.int32, (PROWS, 2 * TOK), 0).astype(F32)
        for p in range(CHIPS):
            target = jnp.maximum(route_g[2 * p, layer, 0:8, :], route_g[2 * p + 1, layer, 0:8, :]) - base
            gates = route_g[2 * p, layer, 8:16, :] + route_g[2 * p + 1, layer, 8:16, :]
            hit = jnp.zeros((PROWS, 2 * TOK), F32)
            gsum = jnp.zeros((PROWS, 2 * TOK), F32)
            for j in range(8):
                m = row_id == target[j : j + 1, :]
                hit = jnp.where(m, 1.0, hit)
                gsum = jnp.where(m, gates[j : j + 1, :], gsum)
            perm[p] = hit.astype(BF16)
            perm_t[p] = hit.T.astype(BF16)
            gate[p] = jnp.sum(gsum, axis=1, keepdims=True)

    def gather_rows(tokens, dst, layer, cols, gated):
        for p in range(CHIPS):
            got = nn_dot(perm[p], tokens(p))
            if gated:
                got = got * gate[p]
            got = got.astype(BF16)
            for e in range(E):
                dst[layer, e, p * PAIR : (p + 1) * PAIR, cols] = got[e * PAIR : (e + 1) * PAIR]

    def forward_expert(layer, e):
        w1, w3 = w_vm[3 * layer], w_vm[3 * layer + 1]
        rows = xr[layer, e]
        a = nn_dot(rows, w1[e]).astype(BF16).astype(F32)
        b = nn_dot(rows, w3[e]).astype(BF16).astype(F32)
        sig = jax.nn.sigmoid(a)
        s = a * sig
        act_s[e] = s
        act_f[e] = b * (sig * (1.0 + a * (1.0 - sig)))
        hid[layer, e] = (s * b).astype(BF16)

    def hidden_grads(layer):
        w2 = w_vm[3 * layer + 2]

        @pl.loop(0, E)
        def _(e):
            dh = nt_dot(zr[layer, e], w2[e])
            da[layer, e] = (dh * act_f[e]).astype(BF16)
            db[layer, e] = (dh * act_s[e]).astype(BF16)

    def row_chunk(layer, k):
        w1, w3 = w_vm[3 * layer], w_vm[3 * layer + 1]
        cols = slice(k * CW, (k + 1) * CW)

        @pl.loop(0, E)
        def _(e):
            g = nt_dot(da[layer, e], w1[e, cols, :]) + nt_dot(db[layer, e], w3[e, cols, :])
            g = g.astype(BF16)
            for p in range(CHIPS):
                dxp[k % 2, p, e] = g[p * PAIR : (p + 1) * PAIR]

        for p in range(CHIPS):
            r = nn_dot(perm_t[p], dxp[k % 2, p].reshape(PROWS, CW))
            part[layer, k, 0, p] = r[:TOK]
            part[layer, k, 1, p] = r[TOK:]
        c = mate_copy(layer, k)
        c.start()
        sends.append(c)

    def mate_copy(layer, k):
        return remote(part.at[layer, k, 1 - core], mate_recv.at[layer, k], rs_send.at[layer, k, 3], rs_recv.at[layer, k, 3], mate)

    def far_copy(layer, k, i):
        dev = far[i]
        return remote(part.at[layer, k, core, dev // 2], far_recv.at[layer, k, i], rs_send.at[layer, k, i], rs_recv.at[layer, k, i], dev)

    def mate_sum(layer, k):
        mate_copy(layer, k).wait_recv()
        for p in range(CHIPS):
            part[layer, k, core, p] = part[layer, k, core, p] + mate_recv[layer, k, p]
        if layer == 1:
            cols = pl.ds(k * CW, CW)
            out_start(part.at[layer, k, core, chip], own_hbm.at[:, cols])
            for i, out in enumerate((far0_hbm, far1_hbm, far2_hbm)):
                out_start(part.at[layer, k, core, far[i] // 2], out.at[:, cols])
            return
        for i in range(3):
            c = far_copy(layer, k, i)
            c.start()
            sends.append(c)

    def far_sum(layer, k):
        for i in range(3):
            far_copy(layer, k, i).wait_recv()
        return part[layer, k, core, chip] + (far_recv[layer, k, 0] + far_recv[layer, k, 1] + far_recv[layer, k, 2])

    def pair_of(buf, p):
        return buf[2 * p : 2 * p + 2].reshape(2 * TOK, buf.shape[-1])

    with scope("route_two"):
        ag_pass_on(S_ROUTE, route_g)
        ag_finish(S_ROUTE, route_g)
        build_routes(0)
    with scope("wait_y"):
        ag_pass_on(S_Y, y_g)
        ag_finish(S_Y, y_g)
    with scope("rows_y"):
        gather_rows(lambda p: pair_of(y_g, p), xr, 0, slice(None), False)
        out_start(xr.at[0], xrb_hbm)
        w_copy(0).wait()
        w_copy(1).wait()

    with scope("forward_two"):
        @pl.loop(0, E)
        def _(e):
            forward_expert(0, e)

        out_start(hid.at[0], hb_hbm)
    with scope("wait_dy"):
        ag_pass_on(S_DY, dy_g)
        ag_finish(S_DY, dy_g)
    with scope("rows_dy"):
        gather_rows(lambda p: pair_of(dy_g, p), zr, 0, slice(None), True)
        out_start(zr.at[0], zrb_hbm)
        w_copy(2).wait()
    with scope("hidden_two"):
        hidden_grads(0)
        out_start(da.at[0], dab_hbm)
        out_start(db.at[0], dbb_hbm)
    for k in range(CH):
        with scope(f"chunk_two_{k}"):
            row_chunk(0, k)
        if k >= 1:
            with scope(f"mate_two_{k - 1}"):
                mate_sum(0, k - 1)
    with scope("mate_two_last"):
        mate_sum(0, CH - 1)

    with scope("wait_x"):
        ag_pass_on(S_X, x_g)
        build_routes(1)
        ag_finish(S_X, x_g)
    with scope("rows_x"):
        gather_rows(lambda p: pair_of(x_g, p), xr, 1, slice(None), False)
        out_start(xr.at[1], xra_hbm)
        for i in range(3, 6):
            w_copy(i).wait()

    def mid_grad(k):
        cols = slice(k * CW, (k + 1) * CW)
        mine = (dy_ref[:, cols].astype(F32) + far_sum(0, k)).astype(BF16)
        d1_own[k] = mine
        d1_g[k, me] = mine
        out_start(d1_own.at[k], d1_hbm.at[:, pl.ds(k * CW, CW)])
        ag_start(S_D1 + k, d1_own.at[k], d1_g.at[k])

    for k in range(CH):
        with scope(f"forward_one_{k}"):
            forward_expert(1, k)
        with scope(f"mid_{k}"):
            mid_grad(k)
    out_start(hid.at[1], ha_hbm)
    for k in range(CH):
        with scope(f"pass_on_{k}"):
            ag_pass_on(S_D1 + k, d1_g.at[k])
    for k in range(CH):
        with scope(f"finish_{k}"):
            ag_finish(S_D1 + k, d1_g.at[k])
        with scope(f"rows_d1_{k}"):
            gather_rows(lambda p: d1_g[k, 2 * p : 2 * p + 2].reshape(2 * TOK, CW), zr, 1, slice(k * CW, (k + 1) * CW), True)
    out_start(zr.at[1], zra_hbm)
    with scope("hidden_one"):
        hidden_grads(1)
        out_start(da.at[1], daa_hbm)
        out_start(db.at[1], dba_hbm)
    for k in range(CH):
        with scope(f"chunk_one_{k}"):
            row_chunk(1, k)
        if k >= 1:
            with scope(f"mate_one_{k - 1}"):
                mate_sum(1, k - 1)
    with scope("mate_one_last"):
        mate_sum(1, CH - 1)
    with scope("drain"):
        for c in sends:
            c.wait_send()
        for c in outs:
            c.wait()


def main_call(route, x, y, dy, weights_two, weights_one):
    vm = pl.BlockSpec(memory_space=pltpu.VMEM)
    hbm = pl.BlockSpec(memory_space=pl.ANY)
    rows_d = jax.ShapeDtypeStruct((E, ROWS, D), BF16)
    rows_f = jax.ShapeDtypeStruct((E, ROWS, F), BF16)
    sums = jax.ShapeDtypeStruct((TOK, D), F32)
    saved = (rows_d, rows_d, rows_f, rows_f, rows_f)
    w_up = pltpu.VMEM((E, D, F), BF16)
    w_dn = pltpu.VMEM((E, F, D), BF16)
    dma = pltpu.SemaphoreType.DMA
    return pl.pallas_call(
        main_kernel,
        out_shape=(sums, jax.ShapeDtypeStruct((TOK, D), BF16), sums, sums, sums) + saved + saved,
        in_specs=[vm] * 4 + [hbm] * 6,
        out_specs=(hbm,) * 15,
        scratch_shapes=[
            (w_up, w_up, w_dn, w_up, w_up, w_dn),
            pltpu.VMEM((DEVS, 2, 16, 2 * TOK), F32),
            pltpu.VMEM((DEVS, TOK, D), BF16),
            pltpu.VMEM((DEVS, TOK, D), BF16),
            pltpu.VMEM((DEVS, TOK, D), BF16),
            pltpu.VMEM((CH, DEVS, TOK, CW), BF16),
            pltpu.VMEM((CH, TOK, CW), BF16),
            pltpu.VMEM((2, E, ROWS, D), BF16),
            pltpu.VMEM((2, E, ROWS, D), BF16),
            pltpu.VMEM((E, ROWS, F), F32),
            pltpu.VMEM((E, ROWS, F), F32),
            pltpu.VMEM((2, E, ROWS, F), BF16),
            pltpu.VMEM((2, E, ROWS, F), BF16),
            pltpu.VMEM((2, E, ROWS, F), BF16),
            pltpu.VMEM((2, CHIPS, E, PAIR, CW), BF16),
            pltpu.VMEM((CHIPS, PROWS, 2 * TOK), BF16),
            pltpu.VMEM((CHIPS, 2 * TOK, PROWS), BF16),
            pltpu.VMEM((CHIPS, PROWS, 1), F32),
            pltpu.VMEM((2, CH, 2, CHIPS, TOK, CW), F32),
            pltpu.VMEM((2, CH, CHIPS, TOK, CW), F32),
            pltpu.VMEM((2, CH, 3, TOK, CW), F32),
            dma((6,)),
            dma((N_STREAMS, 7)),
            dma((N_STREAMS, 7)),
            dma((2, CH, 4)),
            dma((2, CH, 4)),
            dma((10 + 5 * CH,)),
        ],
        compiler_params=pltpu.CompilerParams(collective_id=0, has_side_effects=True, vmem_limit_bytes=VMEM_LIMIT),
        name="moe_backward",
    )(route, x, y, dy, *weights_two, *weights_one)


def wgrad_kernel(x_ref, z_ref, h_ref, da_ref, db_ref, dw1_ref, dw3_ref, dw2_ref):
    x = x_ref[0]
    dw1_ref[0] = tn_dot(x, da_ref[0])
    dw3_ref[0] = tn_dot(x, db_ref[0])
    dw2_ref[0] = tn_dot(h_ref[0], z_ref[0])


def wgrad_call(xr, zr, hid, da, db, name):
    split = 2
    whole_d = pl.BlockSpec((1, ROWS, D), lambda e, j: (e, 0, 0))
    whole_f = pl.BlockSpec((1, ROWS, F), lambda e, j: (e, 0, 0))
    part_d = pl.BlockSpec((1, ROWS, D // split), lambda e, j: (e, 0, j))
    part_f = pl.BlockSpec((1, ROWS, F // split), lambda e, j: (e, 0, j))
    up = pl.BlockSpec((1, D // split, F), lambda e, j: (e, j, 0))
    dn = pl.BlockSpec((1, F // split, D), lambda e, j: (e, j, 0))
    return pl.pallas_call(
        wgrad_kernel,
        grid=(E, split),
        out_shape=(jax.ShapeDtypeStruct((E, D, F), F32), jax.ShapeDtypeStruct((E, D, F), F32), jax.ShapeDtypeStruct((E, F, D), F32)),
        in_specs=[part_d, whole_d, part_f, whole_f, whole_f],
        out_specs=(up, up, dn),
        compiler_params=pltpu.CompilerParams(vmem_limit_bytes=VMEM_LIMIT),
        cost_estimate=pl.CostEstimate(flops=6 * E * ROWS * D * F, bytes_accessed=12 * E * D * F, transcendentals=0),
        name=name,
    )(xr, zr, hid, da, db)


def route_of(experts, gates, slots, core):
    code = jnp.where(slots >= 0, experts * PAIR + core * CAP + slots, -1).astype(F32).T
    gate = gates.T
    lane_core = lax.broadcasted_iota(jnp.int32, (8, 2 * TOK), 1) // TOK
    mine = lane_core == core
    code = jnp.where(mine, jnp.concatenate([code, code], axis=1), -1.0)
    gate = jnp.where(mine, jnp.concatenate([gate, gate], axis=1), 0.0)
    return jnp.concatenate([code, gate], axis=0)


def solution(mesh):
    tok_spec = P(("data", "expert"), None)
    weight_spec = P("expert", None, None)
    grad_spec = P(("data", "expert"), None, None)

    def local_step(x_tokens, y_mid, dy_out, experts_one, gates_one, slots_one, experts_two, gates_two, slots_two, w_gate_one, w_up_one, w_down_one, w_gate_two, w_up_two, w_down_two):
        core = lax.rem(lax.axis_index("expert"), 2)
        route = jnp.stack([route_of(experts_two, gates_two, slots_two, core), route_of(experts_one, gates_one, slots_one, core)])
        got = main_call(route, x_tokens, y_mid, dy_out, (w_gate_two, w_up_two, w_down_two), (w_gate_one, w_up_one, w_down_one))
        own, d1 = got[0:2]
        far = [lax.ppermute(got[2 + i], "expert", [(d, d ^ flip) for d in range(DEVS)]) for i, flip in enumerate((2, 4, 6))]
        grads_two = wgrad_call(*got[5:10], "wgrad_two")
        grads_one = wgrad_call(*got[10:15], "wgrad_one")
        dx = (d1.astype(F32) + (own + (far[0] + far[1] + far[2]))).astype(BF16)
        return (dx,) + tuple(grads_one) + tuple(grads_two)

    return jax.shard_map(local_step, mesh=mesh, in_specs=(tok_spec,) * 9 + (weight_spec,) * 6, out_specs=(tok_spec,) + (grad_spec,) * 6, check_vma=False)
```

```python
import functools
import jax
import jax.numpy as jnp
from jax import lax
from jax.experimental import pallas as pl
from jax.experimental.pallas import tpu as pltpu
from jax.sharding import PartitionSpec as P

MESH = pl.DeviceIdType.MESH
scope = jax.named_scope
F32 = jnp.float32
BF16 = jnp.bfloat16

TOK = 64
CHIPS = 4
DEVS = 8
D = 1024
F = 512
E = 4
CAP = 24
PAIR = 2 * CAP
ROWS = CHIPS * PAIR
PROWS = E * PAIR
CH = 4
CW = D // CH
MAIN_VMEM = 48_000_000
WGRAD_VMEM = 40_000_000

S_ROUTE, S_Y, S_DY, S_X, S_D1 = 0, 1, 2, 3, 4
N_STREAMS = S_D1 + CH

SETS = 2
HALVES = 2


def nt_dot(a, b):
    return lax.dot_general(a, b, (((1,), (1,)), ((), ())), preferred_element_type=F32)


def tn_dot(a, b):
    return lax.dot_general(a, b, (((0,), (0,)), ((), ())), preferred_element_type=F32)


def nn_dot(a, b):
    return jnp.dot(a, b, preferred_element_type=F32)


def main_kernel(
    route_ref, x_ref, y_ref, dy_ref, w1b_hbm, w3b_hbm, w2b_hbm, w1a_hbm, w3a_hbm, w2a_hbm,
    own_hbm, d1_hbm, far0_hbm, far1_hbm, far2_hbm,
    xr_two, zr_two, hid_two, da_two, db_two, xr_one, zr_one, hid_one, da_one, db_one,
    w_vm, route_g, y_g, dy_g, x_g, d1_g, d1_own,
    act_s, act_f, dxp, perm, perm_t, gate,
    part, mate_recv, far_recv,
    w_sem, ag_send, ag_recv, rs_send, rs_recv, out_sem,
):
    xr, zr, hid = (xr_two, xr_one), (zr_two, zr_one), (hid_two, hid_one)
    da, db = (da_two, da_one), (db_two, db_one)
    me = lax.axis_index("expert")
    core = lax.rem(me, 2)
    xpos = lax.rem(me // 2, 2)
    ypos = me // 4
    chip = me // 2
    mate = me + 1 - 2 * core
    nx = me + 2 - 4 * xpos
    ny = me + 4 - 8 * ypos
    nd = ny + 2 - 4 * xpos
    far = (nx, ny, nd)

    def remote(src, dst, send, recv, dev):
        return pltpu.make_async_remote_copy(src_ref=src, dst_ref=dst, send_sem=send, recv_sem=recv, device_id={"expert": dev}, device_id_type=MESH)

    w_hbm = (w1b_hbm, w3b_hbm, w2b_hbm, w1a_hbm, w3a_hbm, w2a_hbm)

    def w_copy(i):
        return pltpu.make_async_copy(w_hbm[i], w_vm[i], w_sem.at[i])

    for i in range(3):
        w_copy(i).start()

    barrier = pltpu.get_barrier_semaphore()
    for dev in (mate,) + far:
        pl.semaphore_signal(barrier, inc=1, device_id={"expert": dev}, device_id_type=MESH)
    pl.semaphore_wait(barrier, 4)

    sends = []

    def ag_start(stream, src, buf):
        for k, dev in enumerate(far + (mate,)):
            c = remote(src, buf.at[me], ag_send.at[stream, k], ag_recv.at[stream, k], dev)
            c.start()
            sends.append(c)

    def ag_pass_on(stream, buf):
        for k, dev in enumerate(far):
            remote(buf.at[dev], buf.at[dev], ag_send.at[stream, k], ag_recv.at[stream, k], dev).wait_recv()
            c = remote(buf.at[dev], buf.at[dev], ag_send.at[stream, 4 + k], ag_recv.at[stream, 4 + k], mate)
            c.start()
            sends.append(c)

    def ag_finish(stream, buf):
        remote(buf.at[mate], buf.at[mate], ag_send.at[stream, 3], ag_recv.at[stream, 3], mate).wait_recv()
        for k, dev in enumerate(far):
            dev_mate = dev + 1 - 2 * core
            remote(buf.at[dev_mate], buf.at[dev_mate], ag_send.at[stream, 4 + k], ag_recv.at[stream, 4 + k], mate).wait_recv()

    ag_start(S_ROUTE, route_ref, route_g)
    ag_start(S_Y, y_ref, y_g)
    ag_start(S_DY, dy_ref, dy_g)
    ag_start(S_X, x_ref, x_g)
    for i in range(3, 6):
        w_copy(i).start()
    route_g[me] = route_ref[...]
    y_g[me] = y_ref[...]
    dy_g[me] = dy_ref[...]
    x_g[me] = x_ref[...]

    outs = []

    def out_start(src, dst):
        c = pltpu.make_async_copy(src, dst, out_sem.at[len(outs)])
        c.start()
        outs.append(c)

    def build_routes(layer):
        base = (me * PROWS).astype(F32)
        row_id = lax.broadcasted_iota(jnp.int32, (PROWS, 2 * TOK), 0).astype(F32)
        for p in range(CHIPS):
            target = jnp.maximum(route_g[2 * p, layer, 0:8, :], route_g[2 * p + 1, layer, 0:8, :]) - base
            gates = route_g[2 * p, layer, 8:16, :] + route_g[2 * p + 1, layer, 8:16, :]
            hit = jnp.zeros((PROWS, 2 * TOK), F32)
            gsum = jnp.zeros((PROWS, 2 * TOK), F32)
            for j in range(8):
                m = row_id == target[j : j + 1, :]
                hit = jnp.where(m, 1.0, hit)
                gsum = jnp.where(m, gates[j : j + 1, :], gsum)
            perm[p] = hit.astype(BF16)
            perm_t[p] = hit.T.astype(BF16)
            gate[p] = jnp.sum(gsum, axis=1, keepdims=True)

    def gather_rows(tokens, dst, layer, cols, gated):
        for p in range(CHIPS):
            got = nn_dot(perm[p], tokens(p))
            if gated:
                got = got * gate[p]
            got = got.astype(BF16)
            for e in range(E):
                dst[layer][e, p * PAIR : (p + 1) * PAIR, cols] = got[e * PAIR : (e + 1) * PAIR]

    def forward_expert(layer, e):
        w1, w3 = w_vm[3 * layer], w_vm[3 * layer + 1]
        rows = xr[layer][e]
        a = nn_dot(rows, w1[e]).astype(BF16).astype(F32)
        b = nn_dot(rows, w3[e]).astype(BF16).astype(F32)
        sig = jax.nn.sigmoid(a)
        s = a * sig
        act_s[e] = s
        act_f[e] = b * (sig * (1.0 + a * (1.0 - sig)))
        hid[layer][e] = (s * b).astype(BF16)

    def hidden_grads(layer):
        w2 = w_vm[3 * layer + 2]

        @pl.loop(0, E)
        def _(e):
            dh = nt_dot(zr[layer][e], w2[e])
            da[layer][e] = (dh * act_f[e]).astype(BF16)
            db[layer][e] = (dh * act_s[e]).astype(BF16)

    def row_chunk(layer, k):
        w1, w3 = w_vm[3 * layer], w_vm[3 * layer + 1]
        cols = slice(k * CW, (k + 1) * CW)

        @pl.loop(0, E)
        def _(e):
            g = nt_dot(da[layer][e], w1[e, cols, :]) + nt_dot(db[layer][e], w3[e, cols, :])
            g = g.astype(BF16)
            for p in range(CHIPS):
                dxp[k % 2, p, e] = g[p * PAIR : (p + 1) * PAIR]

        for p in range(CHIPS):
            r = nn_dot(perm_t[p], dxp[k % 2, p].reshape(PROWS, CW))
            part[layer, k, 0, p] = r[:TOK]
            part[layer, k, 1, p] = r[TOK:]
        c = mate_copy(layer, k)
        c.start()
        sends.append(c)

    def mate_copy(layer, k):
        return remote(part.at[layer, k, 1 - core], mate_recv.at[layer, k], rs_send.at[layer, k, 3], rs_recv.at[layer, k, 3], mate)

    def far_copy(layer, k, i):
        dev = far[i]
        return remote(part.at[layer, k, core, dev // 2], far_recv.at[layer, k, i], rs_send.at[layer, k, i], rs_recv.at[layer, k, i], dev)

    def mate_sum(layer, k):
        mate_copy(layer, k).wait_recv()
        for p in range(CHIPS):
            part[layer, k, core, p] = part[layer, k, core, p] + mate_recv[layer, k, p]
        if layer == 1:
            cols = pl.ds(k * CW, CW)
            out_start(part.at[layer, k, core, chip], own_hbm.at[:, cols])
            for i, out in enumerate((far0_hbm, far1_hbm, far2_hbm)):
                out_start(part.at[layer, k, core, far[i] // 2], out.at[:, cols])
            return
        for i in range(3):
            c = far_copy(layer, k, i)
            c.start()
            sends.append(c)

    def far_sum(layer, k):
        for i in range(3):
            far_copy(layer, k, i).wait_recv()
        return part[layer, k, core, chip] + (far_recv[layer, k, 0] + far_recv[layer, k, 1] + far_recv[layer, k, 2])

    def pair_of(buf, p):
        return buf[2 * p : 2 * p + 2].reshape(2 * TOK, buf.shape[-1])

    with scope("route_two"):
        ag_pass_on(S_ROUTE, route_g)
        ag_finish(S_ROUTE, route_g)
        build_routes(0)
    with scope("wait_y"):
        ag_pass_on(S_Y, y_g)
        ag_finish(S_Y, y_g)
    with scope("rows_y"):
        gather_rows(lambda p: pair_of(y_g, p), xr, 0, slice(None), False)
        w_copy(0).wait()
        w_copy(1).wait()

    with scope("forward_two"):
        @pl.loop(0, E)
        def _(e):
            forward_expert(0, e)

    with scope("wait_dy"):
        ag_pass_on(S_DY, dy_g)
        ag_finish(S_DY, dy_g)
    with scope("rows_dy"):
        gather_rows(lambda p: pair_of(dy_g, p), zr, 0, slice(None), True)
        w_copy(2).wait()
    with scope("hidden_two"):
        hidden_grads(0)
    for k in range(CH):
        with scope(f"chunk_two_{k}"):
            row_chunk(0, k)
        if k >= 1:
            with scope(f"mate_two_{k - 1}"):
                mate_sum(0, k - 1)
    with scope("mate_two_last"):
        mate_sum(0, CH - 1)

    with scope("wait_x"):
        ag_pass_on(S_X, x_g)
        build_routes(1)
        ag_finish(S_X, x_g)
    with scope("rows_x"):
        gather_rows(lambda p: pair_of(x_g, p), xr, 1, slice(None), False)
        for i in range(3, 6):
            w_copy(i).wait()

    def mid_grad(k):
        cols = slice(k * CW, (k + 1) * CW)
        mine = (dy_ref[:, cols].astype(F32) + far_sum(0, k)).astype(BF16)
        d1_own[k] = mine
        d1_g[k, me] = mine
        out_start(d1_own.at[k], d1_hbm.at[:, pl.ds(k * CW, CW)])
        ag_start(S_D1 + k, d1_own.at[k], d1_g.at[k])

    for k in range(CH):
        with scope(f"forward_one_{k}"):
            forward_expert(1, k)
        with scope(f"mid_{k}"):
            mid_grad(k)
    for k in range(CH):
        with scope(f"pass_on_{k}"):
            ag_pass_on(S_D1 + k, d1_g.at[k])
    for k in range(CH):
        with scope(f"finish_{k}"):
            ag_finish(S_D1 + k, d1_g.at[k])
        with scope(f"rows_d1_{k}"):
            gather_rows(lambda p: d1_g[k, 2 * p : 2 * p + 2].reshape(2 * TOK, CW), zr, 1, slice(k * CW, (k + 1) * CW), True)
    with scope("hidden_one"):
        hidden_grads(1)
    for k in range(CH):
        with scope(f"chunk_one_{k}"):
            row_chunk(1, k)
        if k >= 1:
            with scope(f"mate_one_{k - 1}"):
                mate_sum(1, k - 1)
    with scope("mate_one_last"):
        mate_sum(1, CH - 1)
    with scope("drain"):
        for c in sends:
            c.wait_send()
        for c in outs:
            c.wait()


def main_call(route, x, y, dy, weights_two, weights_one):
    vm = pl.BlockSpec(memory_space=pltpu.VMEM)
    hbm = pl.BlockSpec(memory_space=pl.ANY)
    rows_d = pltpu.VMEM((E, ROWS, D), BF16)
    rows_f = pltpu.VMEM((E, ROWS, F), BF16)
    sums = jax.ShapeDtypeStruct((TOK, D), F32)
    saved = (rows_d, rows_d, rows_f, rows_f, rows_f)
    w_up = pltpu.VMEM((E, D, F), BF16)
    w_dn = pltpu.VMEM((E, F, D), BF16)
    dma = pltpu.SemaphoreType.DMA
    return pl.pallas_call(
        main_kernel,
        out_shape=(sums, jax.ShapeDtypeStruct((TOK, D), BF16), sums, sums, sums) + saved + saved,
        in_specs=[vm] * 4 + [hbm] * 6,
        out_specs=(hbm,) * 5 + (vm,) * 10,
        scratch_shapes=[
            (w_up, w_up, w_dn, w_up, w_up, w_dn),
            pltpu.VMEM((DEVS, 2, 16, 2 * TOK), F32),
            pltpu.VMEM((DEVS, TOK, D), BF16),
            pltpu.VMEM((DEVS, TOK, D), BF16),
            pltpu.VMEM((DEVS, TOK, D), BF16),
            pltpu.VMEM((CH, DEVS, TOK, CW), BF16),
            pltpu.VMEM((CH, TOK, CW), BF16),
            pltpu.VMEM((E, ROWS, F), F32),
            pltpu.VMEM((E, ROWS, F), F32),
            pltpu.VMEM((2, CHIPS, E, PAIR, CW), BF16),
            pltpu.VMEM((CHIPS, PROWS, 2 * TOK), BF16),
            pltpu.VMEM((CHIPS, 2 * TOK, PROWS), BF16),
            pltpu.VMEM((CHIPS, PROWS, 1), F32),
            pltpu.VMEM((2, CH, 2, CHIPS, TOK, CW), F32),
            pltpu.VMEM((2, CH, CHIPS, TOK, CW), F32),
            pltpu.VMEM((2, CH, 3, TOK, CW), F32),
            dma((6,)),
            dma((N_STREAMS, 7)),
            dma((N_STREAMS, 7)),
            dma((2, CH, 4)),
            dma((2, CH, 4)),
            dma((5 * CH,)),
        ],
        compiler_params=pltpu.CompilerParams(collective_id=0, has_side_effects=True, vmem_limit_bytes=MAIN_VMEM),
        name="moe_backward",
    )(route, x, y, dy, *weights_two, *weights_one)


def wgrad_kernel(*refs):
    saved, outs, bufs, out_sem = (refs[0:5], refs[5:10]), (refs[10:13], refs[13:16]), refs[16:19], refs[19]

    def out_copy(layer, m, e, slot, h):
        n = bufs[m].shape[1] // HALVES
        rows = pl.ds(h * n, n)
        return pltpu.make_async_copy(bufs[m].at[slot, rows], outs[layer][m].at[e, rows], out_sem.at[slot, m, h])

    for layer in range(2):
        xr, zr, hid, da, db = saved[layer]

        @pl.loop(0, E)
        def _(e):
            i = layer * E + e
            slot = lax.rem(i, SETS)
            for m, lhs, rhs in ((2, hid, zr), (0, xr, da), (1, xr, db)):
                n = bufs[m].shape[1] // HALVES
                for h in range(HALVES):
                    rows = slice(h * n, (h + 1) * n)

                    @pl.when(i >= SETS)
                    def _():
                        out_copy(layer, m, e, slot, h).wait()

                    bufs[m][slot, rows] = tn_dot(lhs[e, :, rows], rhs[e])
                    out_copy(layer, m, e, slot, h).start()

    for i in range(2 * E - SETS, 2 * E):
        for m in (2, 0, 1):
            for h in range(HALVES):
                out_copy(i // E, m, i % E, i % SETS, h).wait()


def wgrad_call(*saved):
    up = jax.ShapeDtypeStruct((E, D, F), F32)
    dn = jax.ShapeDtypeStruct((E, F, D), F32)
    hbm = pl.BlockSpec(memory_space=pl.ANY)
    return pl.pallas_call(
        wgrad_kernel,
        out_shape=(up, up, dn) * 2,
        in_specs=[pl.BlockSpec(memory_space=pltpu.VMEM)] * 10,
        out_specs=(hbm,) * 6,
        scratch_shapes=[
            pltpu.VMEM((SETS, D, F), F32),
            pltpu.VMEM((SETS, D, F), F32),
            pltpu.VMEM((SETS, F, D), F32),
            pltpu.SemaphoreType.DMA((SETS, 3, HALVES)),
        ],
        compiler_params=pltpu.CompilerParams(vmem_limit_bytes=WGRAD_VMEM),
        cost_estimate=pl.CostEstimate(flops=12 * E * ROWS * D * F, bytes_accessed=24 * E * D * F, transcendentals=0),
        name="weight_grads",
    )(*saved)


def route_of(experts, gates, slots, core):
    code = jnp.where(slots >= 0, experts * PAIR + core * CAP + slots, -1).astype(F32).T
    gate = gates.T
    lane_core = lax.broadcasted_iota(jnp.int32, (8, 2 * TOK), 1) // TOK
    mine = lane_core == core
    code = jnp.where(mine, jnp.concatenate([code, code], axis=1), -1.0)
    gate = jnp.where(mine, jnp.concatenate([gate, gate], axis=1), 0.0)
    return jnp.concatenate([code, gate], axis=0)


def solution(mesh):
    tok_spec = P(("data", "expert"), None)
    weight_spec = P("expert", None, None)
    grad_spec = P(("data", "expert"), None, None)

    def local_step(x_tokens, y_mid, dy_out, experts_one, gates_one, slots_one, experts_two, gates_two, slots_two, w_gate_one, w_up_one, w_down_one, w_gate_two, w_up_two, w_down_two):
        core = lax.rem(lax.axis_index("expert"), 2)
        route = jnp.stack([route_of(experts_two, gates_two, slots_two, core), route_of(experts_one, gates_one, slots_one, core)])
        got = main_call(route, x_tokens, y_mid, dy_out, (w_gate_two, w_up_two, w_down_two), (w_gate_one, w_up_one, w_down_one))
        own, d1 = got[0:2]
        far = [lax.ppermute(got[2 + i], "expert", [(d, d ^ flip) for d in range(DEVS)]) for i, flip in enumerate((2, 4, 6))]
        grads = wgrad_call(*got[5:15])
        dx = (d1.astype(F32) + (own + (far[0] + far[1] + far[2]))).astype(BF16)
        return (dx,) + tuple(grads[3:6]) + tuple(grads[0:3])

    return jax.shard_map(local_step, mesh=mesh, in_specs=(tok_spec,) * 9 + (weight_spec,) * 6, out_specs=(tok_spec,) + (grad_spec,) * 6, check_vma=False)
```

```python
import functools
import jax
import jax.numpy as jnp
from jax import lax
from jax.experimental import pallas as pl
from jax.experimental.pallas import tpu as pltpu
from jax.sharding import PartitionSpec as P

MESH = pl.DeviceIdType.MESH
scope = jax.named_scope
F32 = jnp.float32
BF16 = jnp.bfloat16

TOK = 64
CHIPS = 4
DEVS = 8
D = 1024
F = 512
E = 4
CAP = 24
PAIR = 2 * CAP
ROWS = CHIPS * PAIR
PROWS = E * PAIR
CH = 4
CW = D // CH
MAIN_VMEM = 48_000_000
WGRAD_VMEM = 40_000_000

S_ROUTE, S_Y, S_DY, S_X, S_D1 = 0, 1, 2, 3, 4
N_STREAMS = S_D1 + CH

SETS = 2
HALVES = 2


def nt_dot(a, b):
    return lax.dot_general(a, b, (((1,), (1,)), ((), ())), preferred_element_type=F32)


def tn_dot(a, b):
    return lax.dot_general(a, b, (((0,), (0,)), ((), ())), preferred_element_type=F32)


def nn_dot(a, b):
    return jnp.dot(a, b, preferred_element_type=F32)


def main_kernel(
    experts_b, gates_b, slots_b, experts_a, gates_a, slots_a,
    x_hbm, y_hbm, dy_hbm, w1b_hbm, w3b_hbm, w2b_hbm, w1a_hbm, w3a_hbm, w2a_hbm,
    own_hbm, d1_hbm, far0_hbm, far1_hbm, far2_hbm,
    xr_two, zr_two, hid_two, da_two, db_two, xr_one, zr_one, hid_one, da_one, db_one,
    w_vm, choice_i, choice_f, route_own, route_g, y_g, dy_g, x_g, d1_g, d1_own,
    act_s, act_f, dh_sum, dxp, perm, perm_t, gate,
    part, mate_recv, near_recv, last_recv,
    in_sem, w_sem, ag_send, ag_recv, rs_send, rs_recv, out_sem,
):
    xr, zr, hid = (xr_two, xr_one), (zr_two, zr_one), (hid_two, hid_one)
    da, db = (da_two, da_one), (db_two, db_one)
    me = lax.axis_index("expert")
    core = lax.rem(me, 2)
    xpos = lax.rem(me // 2, 2)
    ypos = me // 4
    mate = me + 1 - 2 * core
    nx = me + 2 - 4 * xpos
    ny = me + 4 - 8 * ypos
    nd = ny + 2 - 4 * xpos
    na = nx + core * (ny - nx)
    nb = ny + core * (nx - ny)

    def remote(src, dst, send, recv, dev):
        return pltpu.make_async_remote_copy(src_ref=src, dst_ref=dst, send_sem=send, recv_sem=recv, device_id={"expert": dev}, device_id_type=MESH)

    barrier = pltpu.get_barrier_semaphore()
    for dev in (mate, nx, ny, nd):
        pl.semaphore_signal(barrier, inc=1, device_id={"expert": dev}, device_id_type=MESH)

    choices = [
        pltpu.make_async_copy(src, dst, in_sem.at[i])
        for i, (src, dst) in enumerate((
            (experts_b, choice_i.at[0]), (slots_b, choice_i.at[1]), (gates_b, choice_f.at[0]),
            (experts_a, choice_i.at[2]), (slots_a, choice_i.at[3]), (gates_a, choice_f.at[1]),
        ))
    ]
    tiles = [
        pltpu.make_async_copy(src, dst.at[me], in_sem.at[6 + i])
        for i, (src, dst) in enumerate(((y_hbm, y_g), (dy_hbm, dy_g), (x_hbm, x_g)))
    ]
    w_hbm = (w1b_hbm, w3b_hbm, w2b_hbm, w1a_hbm, w3a_hbm, w2a_hbm)

    def w_copy(i):
        return pltpu.make_async_copy(w_hbm[i], w_vm[i], w_sem.at[i])

    for c in choices + tiles:
        c.start()

    for c in choices:
        c.wait()
    for layer in range(2):
        lanes = slice(layer * TOK, (layer + 1) * TOK)
        slot = choice_i[2 * layer + 1]
        code = jnp.where(slot >= 0, choice_i[2 * layer] * PAIR + core * CAP + slot, -1).astype(F32)
        route_own[0:8, lanes] = code
        route_own[8:16, lanes] = choice_f[layer]
    route_g[me] = route_own[...]
    for c in tiles:
        c.wait()
    pl.semaphore_wait(barrier, 4)

    sends = []

    def send(c):
        c.start()
        sends.append(c)

    far = ((0, na), (1, nb), (3, nd))

    def ag_copy(stream, k, src, dst, dev):
        return remote(src, dst, ag_send.at[stream, k], ag_recv.at[stream, k], dev)

    def ag_start(stream, src, buf):
        for k, dev in far + ((2, mate),):
            send(ag_copy(stream, k, src, buf.at[me], dev))

    def ag_got(stream, k, buf, dev):
        ag_copy(stream, k, buf.at[dev], buf.at[dev], mate).wait_recv()

    def ag_pass_on(stream, buf):
        for i, (k, dev) in enumerate(far):
            ag_got(stream, k, buf, dev)
            send(ag_copy(stream, 4 + i, buf.at[dev], buf.at[dev], mate))

    def ag_finish(stream, buf):
        flip = 1 - 2 * core
        for k, dev in ((2, mate), (4, nb + flip), (5, na + flip), (6, nd + flip)):
            ag_got(stream, k, buf, dev)

    outs = []

    def out_start(src, dst):
        c = pltpu.make_async_copy(src, dst, out_sem.at[len(outs)])
        c.start()
        outs.append(c)

    def build_routes(layer):
        base = (me * PROWS).astype(F32)
        row_id = lax.broadcasted_iota(jnp.int32, (PROWS, 2 * TOK), 0).astype(F32)
        lane = lax.broadcasted_iota(jnp.int32, (16, 2 * TOK), 1)
        for p in range(CHIPS):
            halves = [route_g[2 * p], route_g[2 * p + 1]]
            halves[1 - layer] = pltpu.roll(halves[1 - layer], TOK, 1)
            both = jnp.where(lane < TOK, halves[0], halves[1])
            target = both[0:8] - base
            gates = both[8:16]
            hit = jnp.zeros((PROWS, 2 * TOK), F32)
            gsum = jnp.zeros((PROWS, 2 * TOK), F32)
            for j in range(8):
                m = row_id == target[j : j + 1, :]
                hit = jnp.where(m, 1.0, hit)
                gsum = jnp.where(m, gates[j : j + 1, :], gsum)
            perm[p] = hit.astype(BF16)
            perm_t[p] = hit.T.astype(BF16)
            gate[p] = jnp.sum(gsum, axis=1, keepdims=True)

    def gather_rows(tokens, dst, layer, cols, gated):
        for p in range(CHIPS):
            got = nn_dot(perm[p], tokens(p))
            if gated:
                got = got * gate[p]
            got = got.astype(BF16)
            for e in range(E):
                dst[layer][e, p * PAIR : (p + 1) * PAIR, cols] = got[e * PAIR : (e + 1) * PAIR]

    def forward_expert(layer, e):
        w1, w3 = w_vm[3 * layer], w_vm[3 * layer + 1]
        rows = xr[layer][e]
        a = nn_dot(rows, w1[e]).astype(BF16).astype(F32)
        b = nn_dot(rows, w3[e]).astype(BF16).astype(F32)
        sig = jax.nn.sigmoid(a)
        s = a * sig
        act_s[e] = s
        act_f[e] = b * (sig * (1.0 + a * (1.0 - sig)))
        hid[layer][e] = (s * b).astype(BF16)

    def hidden_expert(layer, e, dh):
        da[layer][e] = (dh * act_f[e]).astype(BF16)
        db[layer][e] = (dh * act_s[e]).astype(BF16)

    def row_chunk(layer, k):
        w1, w3 = w_vm[3 * layer], w_vm[3 * layer + 1]
        cols = slice(k * CW, (k + 1) * CW)
        for e in range(E):
            g = nt_dot(da[layer][e], w1[e, cols, :]) + nt_dot(db[layer][e], w3[e, cols, :])
            g = g.astype(BF16)
            for p in range(CHIPS):
                dxp[k % 2, p, e] = g[p * PAIR : (p + 1) * PAIR]
        for p in range(CHIPS):
            r = nn_dot(perm_t[p], dxp[k % 2, p].reshape(PROWS, CW))
            part[layer, k, 0, p] = r[:TOK]
            part[layer, k, 1, p] = r[TOK:]
        send(mate_copy(layer, k))

    def rs_copy(layer, k, i, src, dst, dev):
        return remote(src, dst, rs_send.at[layer, k, i], rs_recv.at[layer, k, i], dev)

    def mate_copy(layer, k):
        return rs_copy(layer, k, 0, part.at[layer, k, 1 - core], mate_recv.at[layer, k], mate)

    def near_copy(k, i):
        return rs_copy(0, k, 1 + i, part.at[0, k, core, (nd, na)[i] // 2], near_recv.at[k, i], na)

    def last_copy(k):
        return rs_copy(0, k, 3, part.at[0, k, core, nb // 2], last_recv.at[k], nb)

    def mate_sum(layer, k):
        mate_copy(layer, k).wait_recv()
        for p in range(CHIPS):
            part[layer, k, core, p] = part[layer, k, core, p] + mate_recv[layer, k, p]

    def near_start(k):
        mate_sum(0, k)
        send(near_copy(k, 0))
        send(near_copy(k, 1))

    def last_start(k):
        near_copy(k, 0).wait_recv()
        part[0, k, core, nb // 2] = part[0, k, core, nb // 2] + near_recv[k, 0]
        send(last_copy(k))

    def sums_out(k):
        mate_sum(1, k)
        cols = pl.ds(k * CW, CW)
        for dev, out in ((me, own_hbm), (nx, far0_hbm), (ny, far1_hbm), (nd, far2_hbm)):
            out_start(part.at[1, k, core, dev // 2], out.at[:, cols])

    def pair_of(buf, p):
        return buf[2 * p : 2 * p + 2].reshape(2 * TOK, buf.shape[-1])

    with scope("start"):
        ag_start(S_ROUTE, route_own, route_g)
        ag_start(S_Y, y_g.at[me], y_g)
        ag_start(S_DY, dy_g.at[me], dy_g)
        for i in range(6):
            w_copy(i).start()

    with scope("route"):
        ag_pass_on(S_ROUTE, route_g)
        ag_finish(S_ROUTE, route_g)
    with scope("build_two"):
        build_routes(0)
    with scope("wait_y"):
        ag_pass_on(S_Y, y_g)
        ag_finish(S_Y, y_g)
    with scope("rows_y"):
        gather_rows(lambda p: pair_of(y_g, p), xr, 0, slice(None), False)
    with scope("forward_two"):
        w_copy(0).wait()
        w_copy(1).wait()
        for e in range(E):
            forward_expert(0, e)
    with scope("wait_dy"):
        ag_start(S_X, x_g.at[me], x_g)
        ag_pass_on(S_DY, dy_g)
        ag_finish(S_DY, dy_g)
    with scope("rows_dy"):
        gather_rows(lambda p: pair_of(dy_g, p), zr, 0, slice(None), True)
    with scope("hidden_two"):
        w_copy(2).wait()
        for e in range(E):
            hidden_expert(0, e, nt_dot(zr[0][e], w_vm[2][e]))
    for k in range(CH):
        with scope(f"chunk_two_{k}"):
            row_chunk(0, k)
        if k >= 1:
            with scope(f"near_{k - 1}"):
                near_start(k - 1)
    with scope(f"near_{CH - 1}"):
        near_start(CH - 1)
    with scope("last_0"):
        last_start(0)

    with scope("wait_x"):
        ag_pass_on(S_X, x_g)
    with scope("build_one"):
        build_routes(1)
    with scope("last_1"):
        last_start(1)
    with scope("rows_x"):
        ag_finish(S_X, x_g)
        gather_rows(lambda p: pair_of(x_g, p), xr, 1, slice(None), False)
    with scope("last_2"):
        last_start(2)
    with scope("forward_one_0"):
        for i in range(3, 6):
            w_copy(i).wait()
        forward_expert(1, 0)
    with scope("last_3"):
        last_start(3)

    def mid_grad(k):
        cols = slice(k * CW, (k + 1) * CW)
        near_copy(k, 1).wait_recv()
        last_copy(k).wait_recv()
        total = part[0, k, core, me // 2] + near_recv[k, 1] + last_recv[k]
        mine = (dy_g[me, :, cols].astype(F32) + total).astype(BF16)
        d1_own[k] = mine
        d1_g[k, me] = mine
        out_start(d1_own.at[k], d1_hbm.at[:, pl.ds(k * CW, CW)])
        ag_start(S_D1 + k, d1_own.at[k], d1_g.at[k])

    def mid_rows(k):
        cols = slice(k * CW, (k + 1) * CW)
        gather_rows(lambda p: pair_of(d1_g.at[k], p), zr, 1, cols, True)

    def hidden_part(k):
        cols = slice(k * CW, (k + 1) * CW)
        for e in range(E):
            dh = nt_dot(zr[1][e, :, cols], w_vm[5][e, :, cols])
            if k > 0:
                dh = dh_sum[e] + dh
            if k < CH - 1:
                dh_sum[e] = dh
            else:
                hidden_expert(1, e, dh)

    for k in range(CH):
        with scope(f"mid_{k}"):
            mid_grad(k)
    for k in range(1, E):
        with scope(f"forward_one_{k}"):
            forward_expert(1, k)
    with scope("pass_on_0"):
        ag_pass_on(S_D1, d1_g.at[0])
    for k in range(CH):
        if k + 1 < CH:
            with scope(f"pass_on_{k + 1}"):
                ag_pass_on(S_D1 + k + 1, d1_g.at[k + 1])
        with scope(f"finish_{k}"):
            ag_finish(S_D1 + k, d1_g.at[k])
        with scope(f"rows_d1_{k}"):
            mid_rows(k)
            hidden_part(k)
    for k in range(CH):
        with scope(f"chunk_one_{k}"):
            row_chunk(1, k)
        if k >= 1:
            with scope(f"mate_one_{k - 1}"):
                sums_out(k - 1)
    with scope("mate_one_last"):
        sums_out(CH - 1)
    with scope("drain"):
        for c in sends:
            c.wait_send()
        for c in outs:
            c.wait()


def main_call(routing, x, y, dy, weights_two, weights_one):
    vm = pl.BlockSpec(memory_space=pltpu.VMEM)
    hbm = pl.BlockSpec(memory_space=pl.ANY)
    rows_d = pltpu.VMEM((E, ROWS, D), BF16)
    rows_f = pltpu.VMEM((E, ROWS, F), BF16)
    sums = jax.ShapeDtypeStruct((TOK, D), F32)
    saved = (rows_d, rows_d, rows_f, rows_f, rows_f)
    w_up = pltpu.VMEM((E, D, F), BF16)
    w_dn = pltpu.VMEM((E, F, D), BF16)
    dma = pltpu.SemaphoreType.DMA
    return pl.pallas_call(
        main_kernel,
        out_shape=(sums, jax.ShapeDtypeStruct((TOK, D), BF16), sums, sums, sums) + saved + saved,
        in_specs=[hbm] * 15,
        out_specs=(hbm,) * 5 + (vm,) * 10,
        scratch_shapes=[
            (w_up, w_up, w_dn, w_up, w_up, w_dn),
            pltpu.VMEM((4, 8, TOK), jnp.int32),
            pltpu.VMEM((2, 8, TOK), F32),
            pltpu.VMEM((16, 2 * TOK), F32),
            pltpu.VMEM((DEVS, 16, 2 * TOK), F32),
            pltpu.VMEM((DEVS, TOK, D), BF16),
            pltpu.VMEM((DEVS, TOK, D), BF16),
            pltpu.VMEM((DEVS, TOK, D), BF16),
            pltpu.VMEM((CH, DEVS, TOK, CW), BF16),
            pltpu.VMEM((CH, TOK, CW), BF16),
            pltpu.VMEM((E, ROWS, F), F32),
            pltpu.VMEM((E, ROWS, F), F32),
            pltpu.VMEM((E, ROWS, F), F32),
            pltpu.VMEM((2, CHIPS, E, PAIR, CW), BF16),
            pltpu.VMEM((CHIPS, PROWS, 2 * TOK), BF16),
            pltpu.VMEM((CHIPS, 2 * TOK, PROWS), BF16),
            pltpu.VMEM((CHIPS, PROWS, 1), F32),
            pltpu.VMEM((2, CH, 2, CHIPS, TOK, CW), F32),
            pltpu.VMEM((2, CH, CHIPS, TOK, CW), F32),
            pltpu.VMEM((CH, 2, TOK, CW), F32),
            pltpu.VMEM((CH, TOK, CW), F32),
            dma((9,)),
            dma((6,)),
            dma((N_STREAMS, 7)),
            dma((N_STREAMS, 7)),
            dma((2, CH, 4)),
            dma((2, CH, 4)),
            dma((5 * CH,)),
        ],
        compiler_params=pltpu.CompilerParams(collective_id=0, has_side_effects=True, vmem_limit_bytes=MAIN_VMEM),
        name="moe_backward",
    )(*routing, x, y, dy, *weights_two, *weights_one)


def wgrad_kernel(*refs):
    saved, outs, bufs, out_sem = (refs[0:5], refs[5:10]), (refs[10:13], refs[13:16]), refs[16:19], refs[19]

    def out_copy(layer, m, e, slot, h):
        n = bufs[m].shape[1] // HALVES
        rows = pl.ds(h * n, n)
        return pltpu.make_async_copy(bufs[m].at[slot, rows], outs[layer][m].at[e, rows], out_sem.at[slot, m, h])

    for layer in range(2):
        xr, zr, hid, da, db = saved[layer]

        @pl.loop(0, E)
        def _(e):
            i = layer * E + e
            slot = lax.rem(i, SETS)
            for m, lhs, rhs in ((2, hid, zr), (0, xr, da), (1, xr, db)):
                n = bufs[m].shape[1] // HALVES
                for h in range(HALVES):
                    rows = slice(h * n, (h + 1) * n)

                    @pl.when(i >= SETS)
                    def _():
                        out_copy(layer, m, e, slot, h).wait()

                    bufs[m][slot, rows] = tn_dot(lhs[e, :, rows], rhs[e])
                    out_copy(layer, m, e, slot, h).start()

    for i in range(2 * E - SETS, 2 * E):
        for m in (2, 0, 1):
            for h in range(HALVES):
                out_copy(i // E, m, i % E, i % SETS, h).wait()


def wgrad_call(*saved):
    up = jax.ShapeDtypeStruct((E, D, F), F32)
    dn = jax.ShapeDtypeStruct((E, F, D), F32)
    hbm = pl.BlockSpec(memory_space=pl.ANY)
    return pl.pallas_call(
        wgrad_kernel,
        out_shape=(up, up, dn) * 2,
        in_specs=[pl.BlockSpec(memory_space=pltpu.VMEM)] * 10,
        out_specs=(hbm,) * 6,
        scratch_shapes=[
            pltpu.VMEM((SETS, D, F), F32),
            pltpu.VMEM((SETS, D, F), F32),
            pltpu.VMEM((SETS, F, D), F32),
            pltpu.SemaphoreType.DMA((SETS, 3, HALVES)),
        ],
        compiler_params=pltpu.CompilerParams(vmem_limit_bytes=WGRAD_VMEM),
        cost_estimate=pl.CostEstimate(flops=12 * E * ROWS * D * F, bytes_accessed=24 * E * D * F, transcendentals=0),
        name="weight_grads",
    )(*saved)


def solution(mesh):
    tok_spec = P(("data", "expert"), None)
    weight_spec = P("expert", None, None)
    grad_spec = P(("data", "expert"), None, None)

    def local_step(x_tokens, y_mid, dy_out, experts_one, gates_one, slots_one, experts_two, gates_two, slots_two, w_gate_one, w_up_one, w_down_one, w_gate_two, w_up_two, w_down_two):
        routing = [a.T for a in (experts_two, gates_two, slots_two, experts_one, gates_one, slots_one)]
        got = main_call(routing, x_tokens, y_mid, dy_out, (w_gate_two, w_up_two, w_down_two), (w_gate_one, w_up_one, w_down_one))
        own, d1 = got[0:2]
        far = [lax.ppermute(got[2 + i], "expert", [(d, d ^ flip) for d in range(DEVS)]) for i, flip in enumerate((2, 4, 6))]
        grads = wgrad_call(*got[5:15])
        dx = (d1.astype(F32) + (own + (far[0] + far[1] + far[2]))).astype(BF16)
        return (dx,) + tuple(grads[3:6]) + tuple(grads[0:3])

    return jax.shard_map(local_step, mesh=mesh, in_specs=(tok_spec,) * 9 + (weight_spec,) * 6, out_specs=(tok_spec,) + (grad_spec,) * 6, check_vma=False)
```

```python
import functools
import jax
import jax.numpy as jnp
from jax import lax
from jax.experimental import pallas as pl
from jax.experimental.pallas import tpu as pltpu
from jax.sharding import PartitionSpec as P

MESH = pl.DeviceIdType.MESH
scope = jax.named_scope
F32 = jnp.float32
BF16 = jnp.bfloat16

TOK = 64
CHIPS = 4
DEVS = 8
D = 1024
F = 512
E = 4
CAP = 24
PAIR = 2 * CAP
ROWS = CHIPS * PAIR
PROWS = E * PAIR
CH = 4
CW = D // CH
MAIN_VMEM = 48_000_000
WGRAD_VMEM = 40_000_000

S_ROUTE, S_Y, S_DY, S_X, S_D1 = 0, 1, 2, 3, 4
N_STREAMS = S_D1 + CH

SETS = 2
HALVES = 1


def nt_dot(a, b):
    return lax.dot_general(a, b, (((1,), (1,)), ((), ())), preferred_element_type=F32)


def tn_dot(a, b):
    return lax.dot_general(a, b, (((0,), (0,)), ((), ())), preferred_element_type=F32)


def nn_dot(a, b):
    return jnp.dot(a, b, preferred_element_type=F32)


def main_kernel(
    experts_b, gates_b, slots_b, experts_a, gates_a, slots_a,
    x_hbm, y_hbm, dy_hbm, w1b_hbm, w3b_hbm, w2b_hbm, w1a_hbm, w3a_hbm, w2a_hbm,
    own_ref, d1_ref, far0_ref, far1_ref, far2_ref,
    xr_two, zr_two, hid_two, da_two, db_two, xr_one, zr_one, hid_one, da_one, db_one,
    w_vm, choice_i, choice_f, route_own, route_g, y_g, dy_g, x_g, d1_g,
    act_s, act_f, dh_sum, dxp, perm, perm_t, gate,
    part, mate_recv, near_recv, last_recv,
    choice_sem, tile_sem, w_sem, send_sem, ag_recv, mate_sem, near_sem, last_sem,
):
    xr, zr, hid = (xr_two, xr_one), (zr_two, zr_one), (hid_two, hid_one)
    da, db = (da_two, da_one), (db_two, db_one)
    me = lax.axis_index("expert")
    core = lax.rem(me, 2)
    xpos = lax.rem(me // 2, 2)
    ypos = me // 4
    mate = me + 1 - 2 * core
    nx = me + 2 - 4 * xpos
    ny = me + 4 - 8 * ypos
    nd = ny + 2 - 4 * xpos
    na = nx + core * (ny - nx)
    nb = ny + core * (nx - ny)

    def remote(src, dst, send, recv, dev):
        return pltpu.make_async_remote_copy(src_ref=src, dst_ref=dst, send_sem=send, recv_sem=recv, device_id={"expert": dev}, device_id_type=MESH)

    barrier = pltpu.get_barrier_semaphore()
    for dev in (mate, nx, ny, nd):
        pl.semaphore_signal(barrier, inc=1, device_id={"expert": dev}, device_id_type=MESH)

    choices = [
        pltpu.make_async_copy(src, dst, choice_sem.at[i])
        for i, src, dst in (
            (0, experts_b, choice_i.at[0]), (0, slots_b, choice_i.at[1]), (1, gates_b, choice_f.at[0]),
            (0, experts_a, choice_i.at[2]), (0, slots_a, choice_i.at[3]), (1, gates_a, choice_f.at[1]),
        )
    ]
    tiles = [
        pltpu.make_async_copy(src, dst.at[me], tile_sem.at[i])
        for i, (src, dst) in enumerate(((y_hbm, y_g), (dy_hbm, dy_g), (x_hbm, x_g)))
    ]
    w_hbm = (w1b_hbm, w3b_hbm, w2b_hbm, w1a_hbm, w3a_hbm, w2a_hbm)

    def w_copy(i):
        return pltpu.make_async_copy(w_hbm[i], w_vm[i], w_sem.at[i])

    for c in choices + tiles:
        c.start()

    for i, whole in enumerate((choice_i, choice_f)):
        pltpu.make_async_copy(whole, whole, choice_sem.at[i]).wait()
    for layer in range(2):
        lanes = slice(layer * TOK, (layer + 1) * TOK)
        slot = choice_i[2 * layer + 1]
        code = jnp.where(slot >= 0, choice_i[2 * layer] * PAIR + core * CAP + slot, -1).astype(F32)
        route_own[0:8, lanes] = code
        route_own[8:16, lanes] = choice_f[layer]
    route_g[me] = route_own[...]
    for c in tiles:
        c.wait()
    pl.semaphore_wait(barrier, 4)

    far = ((0, na), (1, nb), (3, nd))

    def ag_send(stream, k, src, dst, dev):
        remote(src, dst, send_sem.at[min(stream, S_D1)], ag_recv.at[stream, k], dev).start()

    def ag_start(stream, src, buf):
        for k, dev in far + ((2, mate),):
            ag_send(stream, k, src, buf.at[me], dev)

    def ag_got(stream, k, buf):
        remote(buf, buf, send_sem.at[min(stream, S_D1)], ag_recv.at[stream, k], mate).wait_recv()

    def ag_pass_on(stream, buf):
        for k, dev in far:
            ag_got(stream, k, buf.at[dev])
            ag_send(stream, 2, buf.at[dev], buf.at[dev], mate)

    def ag_finish(stream, buf):
        ag_got(stream, 2, buf.at[pl.ds(0, CHIPS)])

    def build_routes(layer):
        base = (me * PROWS).astype(F32)
        row_id = lax.broadcasted_iota(jnp.int32, (PROWS, 2 * TOK), 0).astype(F32)
        lane = lax.broadcasted_iota(jnp.int32, (16, 2 * TOK), 1)
        for p in range(CHIPS):
            halves = [route_g[2 * p], route_g[2 * p + 1]]
            halves[1 - layer] = pltpu.roll(halves[1 - layer], TOK, 1)
            both = jnp.where(lane < TOK, halves[0], halves[1])
            target = both[0:8] - base
            gates = both[8:16]
            hit = jnp.zeros((PROWS, 2 * TOK), F32)
            gsum = jnp.zeros((PROWS, 2 * TOK), F32)
            for j in range(8):
                m = row_id == target[j : j + 1, :]
                hit = jnp.where(m, 1.0, hit)
                gsum = jnp.where(m, gates[j : j + 1, :], gsum)
            perm[p] = hit.astype(BF16)
            perm_t[p] = hit.T.astype(BF16)
            gate[p] = jnp.sum(gsum, axis=1, keepdims=True)

    def gather_rows(tokens, dst, layer, cols, gated):
        for p in range(CHIPS):
            got = nn_dot(perm[p], tokens(p))
            if gated:
                got = got * gate[p]
            got = got.astype(BF16)
            for e in range(E):
                dst[layer][e, p * PAIR : (p + 1) * PAIR, cols] = got[e * PAIR : (e + 1) * PAIR]

    def forward_expert(layer, e):
        w1, w3 = w_vm[3 * layer], w_vm[3 * layer + 1]
        rows = xr[layer][e]
        a = nn_dot(rows, w1[e]).astype(BF16).astype(F32)
        b = nn_dot(rows, w3[e]).astype(BF16).astype(F32)
        sig = jax.nn.sigmoid(a)
        s = a * sig
        act_s[e] = s
        act_f[e] = b * (sig * (1.0 + a * (1.0 - sig)))
        hid[layer][e] = (s * b).astype(BF16)

    def hidden_expert(layer, e, dh):
        da[layer][e] = (dh * act_f[e]).astype(BF16)
        db[layer][e] = (dh * act_s[e]).astype(BF16)

    def row_chunk(layer, k):
        w1, w3 = w_vm[3 * layer], w_vm[3 * layer + 1]
        cols = slice(k * CW, (k + 1) * CW)
        for e in range(E):
            g = nt_dot(da[layer][e], w1[e, cols, :]) + nt_dot(db[layer][e], w3[e, cols, :])
            g = g.astype(BF16)
            for p in range(CHIPS):
                dxp[k % 2, p, e] = g[p * PAIR : (p + 1) * PAIR]
        for p in range(CHIPS):
            r = nn_dot(perm_t[p], dxp[k % 2, p].reshape(PROWS, CW))
            part[layer, k, 0, p] = r[:TOK]
            part[layer, k, 1, p] = r[TOK:]
        mate_copy(layer, k).start()

    def mate_copy(layer, k):
        return remote(part.at[layer, k, 1 - core], mate_recv.at[layer, k], send_sem.at[S_D1 + 1], mate_sem.at[layer, k], mate)

    def near_copy(k, i):
        return remote(part.at[0, k, core, (nd, na)[i] // 2], near_recv.at[k, i], send_sem.at[S_D1 + 2], near_sem.at[k, i], na)

    def last_copy(k):
        return remote(part.at[0, k, core, nb // 2], last_recv.at[k], send_sem.at[S_D1 + 3], last_sem.at[k], nb)

    def near_start(k):
        mate_copy(0, k).wait_recv()
        for p in range(CHIPS):
            part[0, k, core, p] = part[0, k, core, p] + mate_recv[0, k, p]
        near_copy(k, 0).start()
        near_copy(k, 1).start()

    def last_start(k):
        near_copy(k, 0).wait_recv()
        part[0, k, core, nb // 2] = part[0, k, core, nb // 2] + near_recv[k, 0]
        last_copy(k).start()

    def sums_out(k):
        mate_copy(1, k).wait_recv()
        cols = slice(k * CW, (k + 1) * CW)
        for dev, out in ((me, own_ref), (nx, far0_ref), (ny, far1_ref), (nd, far2_ref)):
            out[:, cols] = part[1, k, core, dev // 2] + mate_recv[1, k, dev // 2]

    def pair_of(buf, p):
        return buf[2 * p : 2 * p + 2].reshape(2 * TOK, buf.shape[-1])

    with scope("start"):
        ag_start(S_ROUTE, route_own, route_g)
        ag_start(S_Y, y_g.at[me], y_g)
        ag_start(S_DY, dy_g.at[me], dy_g)
        for i in range(6):
            w_copy(i).start()

    with scope("route"):
        ag_pass_on(S_ROUTE, route_g)
        ag_finish(S_ROUTE, route_g)
    with scope("build_two"):
        build_routes(0)
    with scope("wait_y"):
        ag_pass_on(S_Y, y_g)
        ag_finish(S_Y, y_g)
    with scope("rows_y"):
        gather_rows(lambda p: pair_of(y_g, p), xr, 0, slice(None), False)
    with scope("forward_two"):
        w_copy(0).wait()
        w_copy(1).wait()
        for e in range(E):
            forward_expert(0, e)
    with scope("wait_dy"):
        ag_start(S_X, x_g.at[me], x_g)
        ag_pass_on(S_DY, dy_g)
        ag_finish(S_DY, dy_g)
    with scope("rows_dy"):
        gather_rows(lambda p: pair_of(dy_g, p), zr, 0, slice(None), True)
    with scope("hidden_two"):
        w_copy(2).wait()
        for e in range(E):
            hidden_expert(0, e, nt_dot(zr[0][e], w_vm[2][e]))
    for k in range(CH):
        with scope(f"chunk_two_{k}"):
            row_chunk(0, k)
        if k >= 1:
            with scope(f"near_{k - 1}"):
                near_start(k - 1)
    with scope(f"near_{CH - 1}"):
        near_start(CH - 1)
    with scope("last_0"):
        last_start(0)

    with scope("wait_x"):
        ag_pass_on(S_X, x_g)
    with scope("build_one"):
        build_routes(1)
    with scope("last_1"):
        last_start(1)
    with scope("rows_x"):
        ag_finish(S_X, x_g)
        gather_rows(lambda p: pair_of(x_g, p), xr, 1, slice(None), False)
    with scope("last_2"):
        last_start(2)
    with scope("forward_one_0"):
        for i in range(3, 6):
            w_copy(i).wait()
        forward_expert(1, 0)
    with scope("last_3"):
        last_start(3)

    def mid_grad(k):
        cols = slice(k * CW, (k + 1) * CW)
        near_copy(k, 1).wait_recv()
        last_copy(k).wait_recv()
        total = part[0, k, core, me // 2] + near_recv[k, 1] + last_recv[k]
        mine = (dy_g[me, :, cols].astype(F32) + total).astype(BF16)
        d1_ref[:, cols] = mine
        d1_g[k, me] = mine
        ag_start(S_D1 + k, d1_g.at[k, me], d1_g.at[k])

    def mid_rows(k):
        cols = slice(k * CW, (k + 1) * CW)
        gather_rows(lambda p: pair_of(d1_g.at[k], p), zr, 1, cols, True)

    def hidden_part(k):
        cols = slice(k * CW, (k + 1) * CW)
        for e in range(E):
            dh = nt_dot(zr[1][e, :, cols], w_vm[5][e, :, cols])
            if k > 0:
                dh = dh_sum[e] + dh
            if k < CH - 1:
                dh_sum[e] = dh
            else:
                hidden_expert(1, e, dh)

    for k in range(CH):
        with scope(f"mid_{k}"):
            mid_grad(k)
    for k in range(1, E):
        with scope(f"forward_one_{k}"):
            forward_expert(1, k)
    with scope("pass_on_0"):
        ag_pass_on(S_D1, d1_g.at[0])
    for k in range(CH):
        if k + 1 < CH:
            with scope(f"pass_on_{k + 1}"):
                ag_pass_on(S_D1 + k + 1, d1_g.at[k + 1])
        with scope(f"finish_{k}"):
            ag_finish(S_D1 + k, d1_g.at[k])
        with scope(f"rows_d1_{k}"):
            mid_rows(k)
            hidden_part(k)
    for k in range(CH):
        with scope(f"chunk_one_{k}"):
            row_chunk(1, k)
        if k >= 2:
            with scope(f"mate_one_{k - 2}"):
                sums_out(k - 2)
    with scope("mate_one_late"):
        sums_out(CH - 2)
    with scope("mate_one_last"):
        sums_out(CH - 1)
    with scope("drain"):
        seven = pl.ds(0, DEVS - 1)
        sent = (
            (S_ROUTE, route_g.at[seven]), (S_Y, y_g.at[seven]), (S_DY, dy_g.at[seven]), (S_X, x_g.at[seven]), (S_D1, d1_g.at[:, seven]),
            (S_D1 + 1, mate_recv), (S_D1 + 2, near_recv), (S_D1 + 3, last_recv),
        )
        for i, whole in sent:
            remote(whole, whole, send_sem.at[i], ag_recv.at[0, 0], mate).wait_send()


def main_call(routing, x, y, dy, weights_two, weights_one):
    vm = pl.BlockSpec(memory_space=pltpu.VMEM)
    hbm = pl.BlockSpec(memory_space=pl.ANY)
    rows_d = pltpu.VMEM((E, ROWS, D), BF16)
    rows_f = pltpu.VMEM((E, ROWS, F), BF16)
    sums = pltpu.VMEM((TOK, D), F32)
    saved = (rows_d, rows_d, rows_f, rows_f, rows_f)
    w_up = pltpu.VMEM((E, D, F), BF16)
    w_dn = pltpu.VMEM((E, F, D), BF16)
    dma = pltpu.SemaphoreType.DMA
    return pl.pallas_call(
        main_kernel,
        out_shape=(sums, pltpu.VMEM((TOK, D), BF16), sums, sums, sums) + saved + saved,
        in_specs=[hbm] * 15,
        out_specs=(vm,) * 15,
        scratch_shapes=[
            (w_up, w_up, w_dn, w_up, w_up, w_dn),
            pltpu.VMEM((4, 8, TOK), jnp.int32),
            pltpu.VMEM((2, 8, TOK), F32),
            pltpu.VMEM((16, 2 * TOK), F32),
            pltpu.VMEM((DEVS, 16, 2 * TOK), F32),
            pltpu.VMEM((DEVS, TOK, D), BF16),
            pltpu.VMEM((DEVS, TOK, D), BF16),
            pltpu.VMEM((DEVS, TOK, D), BF16),
            pltpu.VMEM((CH, DEVS, TOK, CW), BF16),
            pltpu.VMEM((E, ROWS, F), F32),
            pltpu.VMEM((E, ROWS, F), F32),
            pltpu.VMEM((E, ROWS, F), F32),
            pltpu.VMEM((2, CHIPS, E, PAIR, CW), BF16),
            pltpu.VMEM((CHIPS, PROWS, 2 * TOK), BF16),
            pltpu.VMEM((CHIPS, 2 * TOK, PROWS), BF16),
            pltpu.VMEM((CHIPS, PROWS, 1), F32),
            pltpu.VMEM((2, CH, 2, CHIPS, TOK, CW), F32),
            pltpu.VMEM((2, CH, CHIPS, TOK, CW), F32),
            pltpu.VMEM((CH, 2, TOK, CW), F32),
            pltpu.VMEM((CH, TOK, CW), F32),
            dma((2,)),
            dma((3,)),
            dma((6,)),
            dma((S_D1 + 4,)),
            dma((N_STREAMS, 4)),
            dma((2, CH)),
            dma((CH, 2)),
            dma((CH,)),
        ],
        compiler_params=pltpu.CompilerParams(collective_id=0, has_side_effects=True, vmem_limit_bytes=MAIN_VMEM),
        name="moe_backward",
    )(*routing, x, y, dy, *weights_two, *weights_one)


def wgrad_kernel(*refs):
    saved, outs, bufs, out_sem = (refs[0:5], refs[5:10]), (refs[10:13], refs[13:16]), refs[16:19], refs[19]

    def out_copy(layer, m, e, slot, h):
        n = bufs[m].shape[1] // HALVES
        rows = pl.ds(h * n, n)
        return pltpu.make_async_copy(bufs[m].at[slot, rows], outs[layer][m].at[e, rows], out_sem.at[slot, m, h])

    for layer in range(2):
        xr, zr, hid, da, db = saved[layer]

        @pl.loop(0, E)
        def _(e):
            i = layer * E + e
            slot = lax.rem(i, SETS)
            for m, lhs, rhs in ((2, hid, zr), (0, xr, da), (1, xr, db)):
                n = bufs[m].shape[1] // HALVES
                for h in range(HALVES):
                    rows = slice(h * n, (h + 1) * n)

                    @pl.when(i >= SETS)
                    def _():
                        out_copy(layer, m, e, slot, h).wait()

                    bufs[m][slot, rows] = tn_dot(lhs[e, :, rows], rhs[e])
                    out_copy(layer, m, e, slot, h).start()

    for i in range(2 * E - SETS, 2 * E):
        for m in (2, 0, 1):
            for h in range(HALVES):
                out_copy(i // E, m, i % E, i % SETS, h).wait()


def wgrad_call(*saved):
    up = jax.ShapeDtypeStruct((E, D, F), F32)
    dn = jax.ShapeDtypeStruct((E, F, D), F32)
    hbm = pl.BlockSpec(memory_space=pl.ANY)
    return pl.pallas_call(
        wgrad_kernel,
        out_shape=(up, up, dn) * 2,
        in_specs=[pl.BlockSpec(memory_space=pltpu.VMEM)] * 10,
        out_specs=(hbm,) * 6,
        scratch_shapes=[
            pltpu.VMEM((SETS, D, F), F32),
            pltpu.VMEM((SETS, D, F), F32),
            pltpu.VMEM((SETS, F, D), F32),
            pltpu.SemaphoreType.DMA((SETS, 3, HALVES)),
        ],
        compiler_params=pltpu.CompilerParams(vmem_limit_bytes=WGRAD_VMEM),
        cost_estimate=pl.CostEstimate(flops=12 * E * ROWS * D * F, bytes_accessed=24 * E * D * F, transcendentals=0),
        name="weight_grads",
    )(*saved)


def solution(mesh):
    tok_spec = P(("data", "expert"), None)
    weight_spec = P("expert", None, None)
    grad_spec = P(("data", "expert"), None, None)

    def local_step(x_tokens, y_mid, dy_out, experts_one, gates_one, slots_one, experts_two, gates_two, slots_two, w_gate_one, w_up_one, w_down_one, w_gate_two, w_up_two, w_down_two):
        routing = [a.T for a in (experts_two, gates_two, slots_two, experts_one, gates_one, slots_one)]
        got = main_call(routing, x_tokens, y_mid, dy_out, (w_gate_two, w_up_two, w_down_two), (w_gate_one, w_up_one, w_down_one))
        own, d1 = got[0:2]
        far = [lax.ppermute(got[2 + i], "expert", [(d, d ^ flip) for d in range(DEVS)]) for i, flip in enumerate((2, 4, 6))]
        grads = wgrad_call(*got[5:15])
        dx = (d1.astype(F32) + (own + (far[0] + far[1] + far[2]))).astype(BF16)
        return (dx,) + tuple(grads[3:6]) + tuple(grads[0:3])

    return jax.shard_map(local_step, mesh=mesh, in_specs=(tok_spec,) * 9 + (weight_spec,) * 6, out_specs=(tok_spec,) + (grad_spec,) * 6, check_vma=False)
```

```python
import functools
import jax
import jax.numpy as jnp
from jax import lax
from jax.experimental import pallas as pl
from jax.experimental.pallas import tpu as pltpu
from jax.sharding import PartitionSpec as P

MESH = pl.DeviceIdType.MESH
scope = jax.named_scope
F32 = jnp.float32
BF16 = jnp.bfloat16

TOK = 64
CHIPS = 4
DEVS = 8
D = 1024
F = 512
E = 4
CAP = 24
PAIR = 2 * CAP
ROWS = CHIPS * PAIR
PROWS = E * PAIR
CH = 4
CW = D // CH
MAIN_VMEM = 48_000_000
WGRAD_VMEM = 40_000_000

S_ROUTE, S_Y, S_DY, S_X, S_D1 = 0, 1, 2, 3, 4
N_STREAMS = S_D1 + CH

SETS = 2
HALVES = 1


def nt_dot(a, b):
    return lax.dot_general(a, b, (((1,), (1,)), ((), ())), preferred_element_type=F32)


def tn_dot(a, b):
    return lax.dot_general(a, b, (((0,), (0,)), ((), ())), preferred_element_type=F32)


def nn_dot(a, b):
    return jnp.dot(a, b, preferred_element_type=F32)


def main_kernel(
    experts_b, gates_b, slots_b, experts_a, gates_a, slots_a,
    x_hbm, y_hbm, dy_hbm, w1b_hbm, w3b_hbm, w2b_hbm, w1a_hbm, w3a_hbm, w2a_hbm,
    own_ref, d1_ref, far0_ref, far1_ref, far2_ref,
    xr_two, zr_two, hid_two, da_two, db_two, xr_one, zr_one, hid_one, da_one, db_one,
    w_vm, choice_i, choice_f, route_own, route_g, y_g, dy_g, x_g, d1_g,
    act_s, act_f, dh_sum, dxp, perm, perm_t, gate,
    part, mate_recv, near_recv, last_recv,
    choice_sem, tile_sem, w_sem, send_sem, ag_recv, mate_sem, near_sem, last_sem,
):
    xr, zr, hid = (xr_two, xr_one), (zr_two, zr_one), (hid_two, hid_one)
    da, db = (da_two, da_one), (db_two, db_one)
    me = lax.axis_index("expert")
    core = lax.rem(me, 2)
    xpos = lax.rem(me // 2, 2)
    ypos = me // 4
    mate = me + 1 - 2 * core
    nx = me + 2 - 4 * xpos
    ny = me + 4 - 8 * ypos
    nd = ny + 2 - 4 * xpos
    na = nx + core * (ny - nx)
    nb = ny + core * (nx - ny)

    def remote(src, dst, send, recv, dev):
        return pltpu.make_async_remote_copy(src_ref=src, dst_ref=dst, send_sem=send, recv_sem=recv, device_id={"expert": dev}, device_id_type=MESH)

    barrier = pltpu.get_barrier_semaphore()
    for dev in (mate, nx, ny, nd):
        pl.semaphore_signal(barrier, inc=1, device_id={"expert": dev}, device_id_type=MESH)

    choices = [
        pltpu.make_async_copy(src, dst, choice_sem.at[i])
        for i, src, dst in (
            (0, experts_b, choice_i.at[0]), (0, slots_b, choice_i.at[1]), (1, gates_b, choice_f.at[0]),
            (0, experts_a, choice_i.at[2]), (0, slots_a, choice_i.at[3]), (1, gates_a, choice_f.at[1]),
        )
    ]
    tiles = [
        pltpu.make_async_copy(src, dst.at[me], tile_sem.at[i])
        for i, (src, dst) in enumerate(((y_hbm, y_g), (dy_hbm, dy_g), (x_hbm, x_g)))
    ]
    w_hbm = (w1b_hbm, w3b_hbm, w2b_hbm, w1a_hbm, w3a_hbm, w2a_hbm)

    def w_copy(i):
        return pltpu.make_async_copy(w_hbm[i], w_vm[i], w_sem.at[i])

    for c in choices + tiles:
        c.start()

    for i, whole in enumerate((choice_i, choice_f)):
        pltpu.make_async_copy(whole, whole, choice_sem.at[i]).wait()
    for layer in range(2):
        lanes = slice(layer * TOK, (layer + 1) * TOK)
        slot = choice_i[2 * layer + 1]
        code = jnp.where(slot >= 0, choice_i[2 * layer] * PAIR + core * CAP + slot, -1).astype(F32)
        route_own[0:8, lanes] = code
        route_own[8:16, lanes] = choice_f[layer]
    route_g[me] = route_own[...]
    for c in tiles:
        c.wait()
    pl.semaphore_wait(barrier, 4)

    far = ((0, na), (1, nb), (3, nd))

    def ag_send(stream, k, src, dst, dev):
        remote(src, dst, send_sem.at[min(stream, S_D1)], ag_recv.at[stream, k], dev).start()

    def ag_start(stream, src, buf):
        for k, dev in far + ((2, mate),):
            ag_send(stream, k, src, buf.at[me], dev)

    def ag_got(stream, k, buf):
        remote(buf, buf, send_sem.at[min(stream, S_D1)], ag_recv.at[stream, k], mate).wait_recv()

    def ag_pass_on(stream, buf):
        for k, dev in far:
            ag_got(stream, k, buf.at[dev])
            ag_send(stream, 2, buf.at[dev], buf.at[dev], mate)

    def ag_finish(stream, buf):
        ag_got(stream, 2, buf.at[pl.ds(0, CHIPS)])

    def ring_start(stream, buf):
        for k, dev in ((0, na), (1, nb), (2, mate)):
            ag_send(stream, k, buf.at[me], buf.at[me], dev)

    def ring_step(stream, buf):
        ag_got(stream, 0, buf.at[na])
        ag_send(stream, 3, buf.at[na], buf.at[na], nb)
        ag_send(stream, 2, buf.at[na], buf.at[na], mate)
        ag_got(stream, 1, buf.at[nb])
        ag_send(stream, 2, buf.at[nb], buf.at[nb], mate)

    def ring_last(stream, buf):
        ag_got(stream, 3, buf.at[nd])
        ag_send(stream, 2, buf.at[nd], buf.at[nd], mate)

    def build_routes(layer):
        base = (me * PROWS).astype(F32)
        row_id = lax.broadcasted_iota(jnp.int32, (PROWS, 2 * TOK), 0).astype(F32)
        lane = lax.broadcasted_iota(jnp.int32, (16, 2 * TOK), 1)
        for p in range(CHIPS):
            halves = [route_g[2 * p], route_g[2 * p + 1]]
            halves[1 - layer] = pltpu.roll(halves[1 - layer], TOK, 1)
            both = jnp.where(lane < TOK, halves[0], halves[1])
            target = both[0:8] - base
            gates = both[8:16]
            hit = jnp.zeros((PROWS, 2 * TOK), F32)
            gsum = jnp.zeros((PROWS, 2 * TOK), F32)
            for j in range(8):
                m = row_id == target[j : j + 1, :]
                hit = jnp.where(m, 1.0, hit)
                gsum = jnp.where(m, gates[j : j + 1, :], gsum)
            perm[p] = hit.astype(BF16)
            perm_t[p] = hit.T.astype(BF16)
            gate[p] = jnp.sum(gsum, axis=1, keepdims=True)

    def gather_rows(tokens, dst, layer, cols, gated):
        for p in range(CHIPS):
            got = nn_dot(perm[p], tokens(p))
            if gated:
                got = got * gate[p]
            got = got.astype(BF16)
            for e in range(E):
                dst[layer][e, p * PAIR : (p + 1) * PAIR, cols] = got[e * PAIR : (e + 1) * PAIR]

    def forward_expert(layer, e):
        w1, w3 = w_vm[3 * layer], w_vm[3 * layer + 1]
        rows = xr[layer][e]
        a = nn_dot(rows, w1[e]).astype(BF16).astype(F32)
        b = nn_dot(rows, w3[e]).astype(BF16).astype(F32)
        sig = jax.nn.sigmoid(a)
        s = a * sig
        act_s[e] = s
        act_f[e] = b * (sig * (1.0 + a * (1.0 - sig)))
        hid[layer][e] = (s * b).astype(BF16)

    def hidden_expert(layer, e, dh):
        da[layer][e] = (dh * act_f[e]).astype(BF16)
        db[layer][e] = (dh * act_s[e]).astype(BF16)

    def row_chunk(layer, k):
        w1, w3 = w_vm[3 * layer], w_vm[3 * layer + 1]
        cols = slice(k * CW, (k + 1) * CW)
        for e in range(E):
            g = nt_dot(da[layer][e], w1[e, cols, :]) + nt_dot(db[layer][e], w3[e, cols, :])
            g = g.astype(BF16)
            for p in range(CHIPS):
                dxp[k % 2, p, e] = g[p * PAIR : (p + 1) * PAIR]
        for p in range(CHIPS):
            r = nn_dot(perm_t[p], dxp[k % 2, p].reshape(PROWS, CW))
            part[layer, k, 0, p] = r[:TOK]
            part[layer, k, 1, p] = r[TOK:]
        mate_copy(layer, k).start()

    def mate_copy(layer, k):
        return remote(part.at[layer, k, 1 - core], mate_recv.at[layer, k], send_sem.at[S_D1 + 1], mate_sem.at[layer, k], mate)

    def near_copy(k, i):
        return remote(part.at[0, k, core, (nd, na)[i] // 2], near_recv.at[k, i], send_sem.at[S_D1 + 2], near_sem.at[k, i], na)

    def last_copy(k):
        return remote(part.at[0, k, core, nb // 2], last_recv.at[k], send_sem.at[S_D1 + 3], last_sem.at[k], nb)

    def near_start(k):
        mate_copy(0, k).wait_recv()
        for p in range(CHIPS):
            part[0, k, core, p] = part[0, k, core, p] + mate_recv[0, k, p]
        near_copy(k, 0).start()
        near_copy(k, 1).start()

    def last_start(k):
        near_copy(k, 0).wait_recv()
        part[0, k, core, nb // 2] = part[0, k, core, nb // 2] + near_recv[k, 0]
        last_copy(k).start()

    def sums_out(k):
        mate_copy(1, k).wait_recv()
        cols = slice(k * CW, (k + 1) * CW)
        for dev, out in ((me, own_ref), (nx, far0_ref), (ny, far1_ref), (nd, far2_ref)):
            out[:, cols] = part[1, k, core, dev // 2] + mate_recv[1, k, dev // 2]

    def pair_of(buf, p):
        return buf[2 * p : 2 * p + 2].reshape(2 * TOK, buf.shape[-1])

    with scope("start"):
        ag_start(S_ROUTE, route_own, route_g)
        ring_start(S_Y, y_g)
        ring_start(S_DY, dy_g)
        for i in range(6):
            w_copy(i).start()

    with scope("route"):
        ag_pass_on(S_ROUTE, route_g)
        ag_finish(S_ROUTE, route_g)
    with scope("step_y"):
        ring_step(S_Y, y_g)
    with scope("build_two"):
        build_routes(0)
    with scope("step_dy"):
        ring_step(S_DY, dy_g)
    with scope("wait_y"):
        ring_last(S_Y, y_g)
        ag_finish(S_Y, y_g)
    with scope("rows_y"):
        gather_rows(lambda p: pair_of(y_g, p), xr, 0, slice(None), False)
        w_copy(0).wait()
        w_copy(1).wait()
    with scope("forward_two"):
        for e in range(2):
            forward_expert(0, e)
    with scope("last_dy"):
        ring_last(S_DY, dy_g)
        ag_start(S_X, x_g.at[me], x_g)
    with scope("forward_two_b"):
        for e in range(2, E):
            forward_expert(0, e)
    with scope("wait_dy"):
        ag_finish(S_DY, dy_g)
    with scope("rows_dy"):
        gather_rows(lambda p: pair_of(dy_g, p), zr, 0, slice(None), True)
    with scope("hidden_two"):
        w_copy(2).wait()
        for e in range(E):
            hidden_expert(0, e, nt_dot(zr[0][e], w_vm[2][e]))
    for k in range(CH):
        with scope(f"chunk_two_{k}"):
            row_chunk(0, k)
        if k >= 1:
            with scope(f"near_{k - 1}"):
                near_start(k - 1)
    with scope(f"near_{CH - 1}"):
        near_start(CH - 1)
    with scope("last_0"):
        last_start(0)

    with scope("wait_x"):
        ag_pass_on(S_X, x_g)
    with scope("build_one"):
        build_routes(1)
    with scope("last_1"):
        last_start(1)
    with scope("rows_x"):
        ag_finish(S_X, x_g)
        gather_rows(lambda p: pair_of(x_g, p), xr, 1, slice(None), False)
    with scope("last_2"):
        last_start(2)
    with scope("forward_one_0"):
        for i in range(3, 6):
            w_copy(i).wait()
        forward_expert(1, 0)
    with scope("last_3"):
        last_start(3)

    def mid_grad(k):
        cols = slice(k * CW, (k + 1) * CW)
        near_copy(k, 1).wait_recv()
        last_copy(k).wait_recv()
        total = part[0, k, core, me // 2] + near_recv[k, 1] + last_recv[k]
        mine = (dy_g[me, :, cols].astype(F32) + total).astype(BF16)
        d1_ref[:, cols] = mine
        d1_g[k, me] = mine
        ag_start(S_D1 + k, d1_g.at[k, me], d1_g.at[k])

    def mid_rows(k):
        cols = slice(k * CW, (k + 1) * CW)
        gather_rows(lambda p: pair_of(d1_g.at[k], p), zr, 1, cols, True)

    def hidden_part(k):
        cols = slice(k * CW, (k + 1) * CW)
        for e in range(E):
            dh = nt_dot(zr[1][e, :, cols], w_vm[5][e, :, cols])
            if k > 0:
                dh = dh_sum[e] + dh
            if k < CH - 1:
                dh_sum[e] = dh
            else:
                hidden_expert(1, e, dh)

    def mid_step(k):
        with scope(f"mid_{k}"):
            mid_grad(k)

    def pass_step(k):
        with scope(f"pass_on_{k}"):
            ag_pass_on(S_D1 + k, d1_g.at[k])

    def rows_step(k):
        with scope(f"finish_{k}"):
            ag_finish(S_D1 + k, d1_g.at[k])
        with scope(f"rows_d1_{k}"):
            mid_rows(k)
            hidden_part(k)

    def forward_step(k):
        with scope(f"forward_one_{k}"):
            forward_expert(1, k)

    mid_step(0)
    mid_step(1)
    mid_step(2)
    forward_step(1)
    forward_step(2)
    forward_step(3)
    mid_step(3)
    pass_step(0)
    pass_step(1)
    pass_step(2)
    rows_step(0)
    pass_step(3)
    rows_step(1)
    rows_step(2)
    rows_step(3)
    for k in range(CH):
        with scope(f"chunk_one_{k}"):
            row_chunk(1, k)
        if k >= 2:
            with scope(f"mate_one_{k - 2}"):
                sums_out(k - 2)
    with scope("mate_one_late"):
        sums_out(CH - 2)
    with scope("mate_one_last"):
        sums_out(CH - 1)
    with scope("drain"):
        seven = pl.ds(0, DEVS - 1)
        sent = (
            (S_ROUTE, route_g.at[seven]), (S_Y, y_g.at[seven]), (S_DY, dy_g.at[seven]), (S_X, x_g.at[seven]), (S_D1, d1_g.at[:, seven]),
            (S_D1 + 1, mate_recv), (S_D1 + 2, near_recv), (S_D1 + 3, last_recv),
        )
        for i, whole in sent:
            remote(whole, whole, send_sem.at[i], ag_recv.at[0, 0], mate).wait_send()


def main_call(routing, x, y, dy, weights_two, weights_one):
    vm = pl.BlockSpec(memory_space=pltpu.VMEM)
    hbm = pl.BlockSpec(memory_space=pl.ANY)
    rows_d = pltpu.VMEM((E, ROWS, D), BF16)
    rows_f = pltpu.VMEM((E, ROWS, F), BF16)
    sums = pltpu.VMEM((TOK, D), F32)
    saved = (rows_d, rows_d, rows_f, rows_f, rows_f)
    w_up = pltpu.VMEM((E, D, F), BF16)
    w_dn = pltpu.VMEM((E, F, D), BF16)
    dma = pltpu.SemaphoreType.DMA
    return pl.pallas_call(
        main_kernel,
        out_shape=(sums, pltpu.VMEM((TOK, D), BF16), sums, sums, sums) + saved + saved,
        in_specs=[hbm] * 15,
        out_specs=(vm,) * 15,
        scratch_shapes=[
            (w_up, w_up, w_dn, w_up, w_up, w_dn),
            pltpu.VMEM((4, 8, TOK), jnp.int32),
            pltpu.VMEM((2, 8, TOK), F32),
            pltpu.VMEM((16, 2 * TOK), F32),
            pltpu.VMEM((DEVS, 16, 2 * TOK), F32),
            pltpu.VMEM((DEVS, TOK, D), BF16),
            pltpu.VMEM((DEVS, TOK, D), BF16),
            pltpu.VMEM((DEVS, TOK, D), BF16),
            pltpu.VMEM((CH, DEVS, TOK, CW), BF16),
            pltpu.VMEM((E, ROWS, F), F32),
            pltpu.VMEM((E, ROWS, F), F32),
            pltpu.VMEM((E, ROWS, F), F32),
            pltpu.VMEM((2, CHIPS, E, PAIR, CW), BF16),
            pltpu.VMEM((CHIPS, PROWS, 2 * TOK), BF16),
            pltpu.VMEM((CHIPS, 2 * TOK, PROWS), BF16),
            pltpu.VMEM((CHIPS, PROWS, 1), F32),
            pltpu.VMEM((2, CH, 2, CHIPS, TOK, CW), F32),
            pltpu.VMEM((2, CH, CHIPS, TOK, CW), F32),
            pltpu.VMEM((CH, 2, TOK, CW), F32),
            pltpu.VMEM((CH, TOK, CW), F32),
            dma((2,)),
            dma((3,)),
            dma((6,)),
            dma((S_D1 + 4,)),
            dma((N_STREAMS, 4)),
            dma((2, CH)),
            dma((CH, 2)),
            dma((CH,)),
        ],
        compiler_params=pltpu.CompilerParams(collective_id=0, has_side_effects=True, vmem_limit_bytes=MAIN_VMEM),
        name="moe_backward",
    )(*routing, x, y, dy, *weights_two, *weights_one)


def wgrad_kernel(*refs):
    saved, outs, bufs, out_sem = (refs[0:5], refs[5:10]), (refs[10:13], refs[13:16]), refs[16:19], refs[19]

    def out_copy(layer, m, e, slot, h):
        n = bufs[m].shape[1] // HALVES
        rows = pl.ds(h * n, n)
        return pltpu.make_async_copy(bufs[m].at[slot, rows], outs[layer][m].at[e, rows], out_sem.at[slot, m, h])

    for layer in range(2):
        xr, zr, hid, da, db = saved[layer]

        @pl.loop(0, E)
        def _(e):
            i = layer * E + e
            slot = lax.rem(i, SETS)
            for m, lhs, rhs in ((2, hid, zr), (0, xr, da), (1, xr, db)):
                n = bufs[m].shape[1] // HALVES
                for h in range(HALVES):
                    rows = slice(h * n, (h + 1) * n)

                    @pl.when(i >= SETS)
                    def _():
                        out_copy(layer, m, e, slot, h).wait()

                    bufs[m][slot, rows] = tn_dot(lhs[e, :, rows], rhs[e])
                    out_copy(layer, m, e, slot, h).start()

    for i in range(2 * E - SETS, 2 * E):
        for m in (2, 0, 1):
            for h in range(HALVES):
                out_copy(i // E, m, i % E, i % SETS, h).wait()


def wgrad_call(*saved):
    up = jax.ShapeDtypeStruct((E, D, F), F32)
    dn = jax.ShapeDtypeStruct((E, F, D), F32)
    hbm = pl.BlockSpec(memory_space=pl.ANY)
    return pl.pallas_call(
        wgrad_kernel,
        out_shape=(up, up, dn) * 2,
        in_specs=[pl.BlockSpec(memory_space=pltpu.VMEM)] * 10,
        out_specs=(hbm,) * 6,
        scratch_shapes=[
            pltpu.VMEM((SETS, D, F), F32),
            pltpu.VMEM((SETS, D, F), F32),
            pltpu.VMEM((SETS, F, D), F32),
            pltpu.SemaphoreType.DMA((SETS, 3, HALVES)),
        ],
        compiler_params=pltpu.CompilerParams(vmem_limit_bytes=WGRAD_VMEM),
        cost_estimate=pl.CostEstimate(flops=12 * E * ROWS * D * F, bytes_accessed=24 * E * D * F, transcendentals=0),
        name="weight_grads",
    )(*saved)


def solution(mesh):
    tok_spec = P(("data", "expert"), None)
    weight_spec = P("expert", None, None)
    grad_spec = P(("data", "expert"), None, None)

    def local_step(x_tokens, y_mid, dy_out, experts_one, gates_one, slots_one, experts_two, gates_two, slots_two, w_gate_one, w_up_one, w_down_one, w_gate_two, w_up_two, w_down_two):
        routing = [a.T for a in (experts_two, gates_two, slots_two, experts_one, gates_one, slots_one)]
        got = main_call(routing, x_tokens, y_mid, dy_out, (w_gate_two, w_up_two, w_down_two), (w_gate_one, w_up_one, w_down_one))
        own, d1 = got[0:2]
        far = [lax.ppermute(got[2 + i], "expert", [(d, d ^ flip) for d in range(DEVS)]) for i, flip in enumerate((2, 4, 6))]
        grads = wgrad_call(*got[5:15])
        dx = (d1.astype(F32) + (own + (far[0] + far[1] + far[2]))).astype(BF16)
        return (dx,) + tuple(grads[3:6]) + tuple(grads[0:3])

    return jax.shard_map(local_step, mesh=mesh, in_specs=(tok_spec,) * 9 + (weight_spec,) * 6, out_specs=(tok_spec,) + (grad_spec,) * 6, check_vma=False)
```

```python
import functools
import jax
import jax.numpy as jnp
from jax import lax
from jax.experimental import pallas as pl
from jax.experimental.pallas import tpu as pltpu
from jax.sharding import PartitionSpec as P

MESH = pl.DeviceIdType.MESH
scope = jax.named_scope
F32 = jnp.float32
BF16 = jnp.bfloat16

TOK = 64
CHIPS = 4
DEVS = 8
D = 1024
F = 512
E = 4
CAP = 24
PAIR = 2 * CAP
ROWS = CHIPS * PAIR
PROWS = E * PAIR
CH = 4
CW = D // CH
MAIN_VMEM = 48_000_000
WGRAD_VMEM = 40_000_000

S_ROUTE, S_Y, S_DY, S_X, S_D1 = 0, 1, 3, 5, 6
N_STREAMS = S_D1 + CH
HW = D // 2

SETS = 2
HALVES = 1


def nt_dot(a, b):
    return lax.dot_general(a, b, (((1,), (1,)), ((), ())), preferred_element_type=F32)


def tn_dot(a, b):
    return lax.dot_general(a, b, (((0,), (0,)), ((), ())), preferred_element_type=F32)


def nn_dot(a, b):
    return jnp.dot(a, b, preferred_element_type=F32)


def main_kernel(
    experts_b, gates_b, slots_b, experts_a, gates_a, slots_a,
    x_hbm, y_hbm, dy_hbm, w1b_hbm, w3b_hbm, w2b_hbm, w1a_hbm, w3a_hbm, w2a_hbm,
    own_ref, d1_ref, far0_ref, far1_ref, far2_ref,
    xr_two, zr_two, hid_two, da_two, db_two, xr_one, zr_one, hid_one, da_one, db_one,
    w_vm, choice_i, choice_f, route_own, route_g, y_g, dy_g, x_g, d1_g,
    act_s, act_f, dh_sum, dxp, perm, perm_t, gate,
    part, mate_recv, near_recv, last_recv,
    choice_sem, tile_sem, w_sem, send_sem, ag_recv, mate_sem, near_sem, last_sem,
):
    xr, zr, hid = (xr_two, xr_one), (zr_two, zr_one), (hid_two, hid_one)
    da, db = (da_two, da_one), (db_two, db_one)
    me = lax.axis_index("expert")
    core = lax.rem(me, 2)
    xpos = lax.rem(me // 2, 2)
    ypos = me // 4
    mate = me + 1 - 2 * core
    nx = me + 2 - 4 * xpos
    ny = me + 4 - 8 * ypos
    nd = ny + 2 - 4 * xpos
    na = nx + core * (ny - nx)
    nb = ny + core * (nx - ny)

    def remote(src, dst, send, recv, dev):
        return pltpu.make_async_remote_copy(src_ref=src, dst_ref=dst, send_sem=send, recv_sem=recv, device_id={"expert": dev}, device_id_type=MESH)

    barrier = pltpu.get_barrier_semaphore()
    for dev in (mate, nx, ny, nd):
        pl.semaphore_signal(barrier, inc=1, device_id={"expert": dev}, device_id_type=MESH)

    choices = [
        pltpu.make_async_copy(src, dst, choice_sem.at[i])
        for i, src, dst in (
            (0, experts_b, choice_i.at[0]), (0, slots_b, choice_i.at[1]), (1, gates_b, choice_f.at[0]),
            (0, experts_a, choice_i.at[2]), (0, slots_a, choice_i.at[3]), (1, gates_a, choice_f.at[1]),
        )
    ]
    tiles = [
        pltpu.make_async_copy(src, dst.at[me], tile_sem.at[i])
        for i, (src, dst) in enumerate((
            (y_hbm.at[:, pl.ds(0, HW)], y_g.at[0]), (y_hbm.at[:, pl.ds(HW, HW)], y_g.at[1]),
            (dy_hbm.at[:, pl.ds(0, HW)], dy_g.at[0]), (dy_hbm.at[:, pl.ds(HW, HW)], dy_g.at[1]), (x_hbm, x_g),
        ))
    ]
    w_hbm = (w1b_hbm, w3b_hbm, w2b_hbm, w1a_hbm, w3a_hbm, w2a_hbm)

    def w_copy(i):
        return pltpu.make_async_copy(w_hbm[i], w_vm[i], w_sem.at[i])

    for c in choices + tiles:
        c.start()

    for i, whole in enumerate((choice_i, choice_f)):
        pltpu.make_async_copy(whole, whole, choice_sem.at[i]).wait()
    for layer in range(2):
        lanes = slice(layer * TOK, (layer + 1) * TOK)
        slot = choice_i[2 * layer + 1]
        code = jnp.where(slot >= 0, choice_i[2 * layer] * PAIR + core * CAP + slot, -1).astype(F32)
        route_own[0:8, lanes] = code
        route_own[8:16, lanes] = choice_f[layer]
    route_g[me] = route_own[...]
    for c in tiles:
        c.wait()
    pl.semaphore_wait(barrier, 4)

    far = ((0, na), (1, nb), (3, nd))

    def ag_send(stream, k, src, dst, dev):
        remote(src, dst, send_sem.at[min(stream, S_D1)], ag_recv.at[stream, k], dev).start()

    def ag_start(stream, src, buf):
        for k, dev in far + ((2, mate),):
            ag_send(stream, k, src, buf.at[me], dev)

    def ag_got(stream, k, buf):
        remote(buf, buf, send_sem.at[min(stream, S_D1)], ag_recv.at[stream, k], mate).wait_recv()

    def ag_pass_on(stream, buf):
        for k, dev in far:
            ag_got(stream, k, buf.at[dev])
            ag_send(stream, 2, buf.at[dev], buf.at[dev], mate)

    def ag_finish(stream, buf):
        ag_got(stream, 2, buf.at[pl.ds(0, CHIPS)])

    def ring_start(stream, buf):
        for k, dev in ((0, na), (1, nb), (2, mate)):
            ag_send(stream, k, buf.at[me], buf.at[me], dev)

    def ring_step(stream, buf):
        ag_got(stream, 0, buf.at[na])
        ag_send(stream, 3, buf.at[na], buf.at[na], nb)
        ag_send(stream, 2, buf.at[na], buf.at[na], mate)
        ag_got(stream, 1, buf.at[nb])
        ag_send(stream, 2, buf.at[nb], buf.at[nb], mate)

    def ring_last(stream, buf):
        ag_got(stream, 3, buf.at[nd])
        ag_send(stream, 2, buf.at[nd], buf.at[nd], mate)

    def build_routes(layer):
        base = (me * PROWS).astype(F32)
        row_id = lax.broadcasted_iota(jnp.int32, (PROWS, 2 * TOK), 0).astype(F32)
        lane = lax.broadcasted_iota(jnp.int32, (16, 2 * TOK), 1)
        for p in range(CHIPS):
            halves = [route_g[2 * p], route_g[2 * p + 1]]
            halves[1 - layer] = pltpu.roll(halves[1 - layer], TOK, 1)
            both = jnp.where(lane < TOK, halves[0], halves[1])
            target = both[0:8] - base
            gates = both[8:16]
            hit = jnp.zeros((PROWS, 2 * TOK), F32)
            gsum = jnp.zeros((PROWS, 2 * TOK), F32)
            for j in range(8):
                m = row_id == target[j : j + 1, :]
                hit = jnp.where(m, 1.0, hit)
                gsum = jnp.where(m, gates[j : j + 1, :], gsum)
            perm[p] = hit.astype(BF16)
            perm_t[p] = hit.T.astype(BF16)
            gate[p] = jnp.sum(gsum, axis=1, keepdims=True)

    def gather_rows(tokens, dst, layer, cols, gated):
        for p in range(CHIPS):
            got = nn_dot(perm[p], tokens(p))
            if gated:
                got = got * gate[p]
            got = got.astype(BF16)
            for e in range(E):
                dst[layer][e, p * PAIR : (p + 1) * PAIR, cols] = got[e * PAIR : (e + 1) * PAIR]

    def activate(layer, e, a, b):
        a = a.astype(BF16).astype(F32)
        b = b.astype(BF16).astype(F32)
        sig = jax.nn.sigmoid(a)
        s = a * sig
        act_s[e] = s
        act_f[e] = b * (sig * (1.0 + a * (1.0 - sig)))
        hid[layer][e] = (s * b).astype(BF16)

    def forward_expert(layer, e):
        rows = xr[layer][e]
        activate(layer, e, nn_dot(rows, w_vm[3 * layer][e]), nn_dot(rows, w_vm[3 * layer + 1][e]))

    def forward_half(e, h):
        cols = slice(h * HW, (h + 1) * HW)
        a = nn_dot(xr[0][e, :, cols], w_vm[0][e, cols, :])
        b = nn_dot(xr[0][e, :, cols], w_vm[1][e, cols, :])
        if h == 0:
            act_s[e] = a
            act_f[e] = b
        else:
            activate(0, e, act_s[e] + a, act_f[e] + b)

    def hidden_expert(layer, e, dh):
        da[layer][e] = (dh * act_f[e]).astype(BF16)
        db[layer][e] = (dh * act_s[e]).astype(BF16)

    def row_chunk(layer, k):
        w1, w3 = w_vm[3 * layer], w_vm[3 * layer + 1]
        cols = slice(k * CW, (k + 1) * CW)
        for e in range(E):
            g = nt_dot(da[layer][e], w1[e, cols, :]) + nt_dot(db[layer][e], w3[e, cols, :])
            g = g.astype(BF16)
            for p in range(CHIPS):
                dxp[k % 2, p, e] = g[p * PAIR : (p + 1) * PAIR]
        for p in range(CHIPS):
            r = nn_dot(perm_t[p], dxp[k % 2, p].reshape(PROWS, CW))
            part[layer, k, 0, p] = r[:TOK]
            part[layer, k, 1, p] = r[TOK:]
        mate_copy(layer, k).start()

    def mate_copy(layer, k):
        return remote(part.at[layer, k, 1 - core], mate_recv.at[layer, k], send_sem.at[S_D1 + 1], mate_sem.at[layer, k], mate)

    def near_copy(k, i):
        return remote(part.at[0, k, core, (nd, na)[i] // 2], near_recv.at[k, i], send_sem.at[S_D1 + 2], near_sem.at[k, i], na)

    def last_copy(k):
        return remote(part.at[0, k, core, nb // 2], last_recv.at[k], send_sem.at[S_D1 + 3], last_sem.at[k], nb)

    def near_start(k):
        mate_copy(0, k).wait_recv()
        for p in range(CHIPS):
            part[0, k, core, p] = part[0, k, core, p] + mate_recv[0, k, p]
        near_copy(k, 0).start()
        near_copy(k, 1).start()

    def last_start(k):
        near_copy(k, 0).wait_recv()
        part[0, k, core, nb // 2] = part[0, k, core, nb // 2] + near_recv[k, 0]
        last_copy(k).start()

    def sums_out(k):
        mate_copy(1, k).wait_recv()
        cols = slice(k * CW, (k + 1) * CW)
        for dev, out in ((me, own_ref), (nx, far0_ref), (ny, far1_ref), (nd, far2_ref)):
            out[:, cols] = part[1, k, core, dev // 2] + mate_recv[1, k, dev // 2]

    def pair_of(buf, p):
        return buf[2 * p : 2 * p + 2].reshape(2 * TOK, buf.shape[-1])

    with scope("start"):
        ag_start(S_ROUTE, route_own, route_g)
        for h in range(2):
            ring_start(S_Y + h, y_g.at[h])
        for h in range(2):
            ring_start(S_DY + h, dy_g.at[h])
        for i in range(6):
            w_copy(i).start()

    def y_step(h):
        with scope(f"y_step_{h}"):
            ring_step(S_Y + h, y_g.at[h])

    def y_last(h):
        with scope(f"y_last_{h}"):
            ring_last(S_Y + h, y_g.at[h])

    def dy_step(h):
        with scope(f"dy_step_{h}"):
            ring_step(S_DY + h, dy_g.at[h])

    def dy_last(h):
        with scope(f"dy_last_{h}"):
            ring_last(S_DY + h, dy_g.at[h])

    def half_cols(h):
        return slice(h * HW, (h + 1) * HW)

    def y_rows(h):
        with scope(f"y_finish_{h}"):
            ag_finish(S_Y + h, y_g.at[h])
        with scope(f"rows_y_{h}"):
            gather_rows(lambda p: pair_of(y_g.at[h], p), xr, 0, half_cols(h), False)

    def dy_rows(h):
        with scope(f"dy_finish_{h}"):
            ag_finish(S_DY + h, dy_g.at[h])
        with scope(f"rows_dy_{h}"):
            gather_rows(lambda p: pair_of(dy_g.at[h], p), zr, 0, half_cols(h), True)

    def forward_part(h, experts):
        with scope(f"forward_two_{h}"):
            for e in experts:
                forward_half(e, h)

    with scope("route"):
        ag_pass_on(S_ROUTE, route_g)
        ag_finish(S_ROUTE, route_g)
    y_step(0)
    y_step(1)
    with scope("build_two"):
        build_routes(0)
    dy_step(0)
    y_last(0)
    dy_step(1)
    y_last(1)
    for i in range(3):
        w_copy(i).wait()
    y_rows(0)
    forward_part(0, range(E))
    dy_last(0)
    y_rows(1)
    forward_part(1, range(2))
    dy_last(1)
    with scope("x_start"):
        ag_start(S_X, x_g.at[me], x_g)
    forward_part(1, range(2, E))
    dy_rows(0)
    dy_rows(1)
    with scope("hidden_two"):
        for e in range(E):
            hidden_expert(0, e, nt_dot(zr[0][e], w_vm[2][e]))

    for k in range(CH):
        with scope(f"chunk_two_{k}"):
            row_chunk(0, k)
        if k >= 1:
            with scope(f"near_{k - 1}"):
                near_start(k - 1)
    with scope(f"near_{CH - 1}"):
        near_start(CH - 1)
    def last_step(k):
        with scope(f"last_{k}"):
            last_start(k)

    def x_wait():
        with scope("wait_x"):
            ag_pass_on(S_X, x_g)

    def x_build():
        with scope("build_one"):
            build_routes(1)

    def x_rows():
        with scope("rows_x"):
            ag_finish(S_X, x_g)
            gather_rows(lambda p: pair_of(x_g, p), xr, 1, slice(None), False)
            for i in range(3, 6):
                w_copy(i).wait()

    def ring_one(k):
        with scope(f"step_{k}"):
            ring_step(S_D1 + k, d1_g.at[k])

    def ring_two(k):
        with scope(f"last_d1_{k}"):
            ring_last(S_D1 + k, d1_g.at[k])

    def mid_grad(k):
        cols = slice(k * CW, (k + 1) * CW)
        near_copy(k, 1).wait_recv()
        last_copy(k).wait_recv()
        total = part[0, k, core, me // 2] + near_recv[k, 1] + last_recv[k]
        mine = (dy_g[k // 2, me, :, (k % 2) * CW : (k % 2 + 1) * CW].astype(F32) + total).astype(BF16)
        d1_ref[:, cols] = mine
        d1_g[k, me] = mine
        if k < 2:
            ring_start(S_D1 + k, d1_g.at[k])
        else:
            ag_start(S_D1 + k, d1_g.at[k, me], d1_g.at[k])

    def mid_rows(k):
        cols = slice(k * CW, (k + 1) * CW)
        gather_rows(lambda p: pair_of(d1_g.at[k], p), zr, 1, cols, True)

    def hidden_part(k):
        cols = slice(k * CW, (k + 1) * CW)
        for e in range(E):
            dh = nt_dot(zr[1][e, :, cols], w_vm[5][e, :, cols])
            if k > 0:
                dh = dh_sum[e] + dh
            if k < CH - 1:
                dh_sum[e] = dh
            else:
                hidden_expert(1, e, dh)

    def mid_step(k):
        with scope(f"mid_{k}"):
            mid_grad(k)

    def pass_step(k):
        with scope(f"pass_on_{k}"):
            ag_pass_on(S_D1 + k, d1_g.at[k])

    def rows_step(k):
        with scope(f"finish_{k}"):
            ag_finish(S_D1 + k, d1_g.at[k])
        with scope(f"rows_d1_{k}"):
            mid_rows(k)
            hidden_part(k)

    def forward_step(k):
        with scope(f"forward_one_{k}"):
            forward_expert(1, k)

    last_step(0)
    x_wait()
    x_build()
    last_step(1)
    x_rows()
    last_step(2)
    mid_step(0)
    forward_step(0)
    last_step(3)
    mid_step(1)
    mid_step(2)
    forward_step(1)
    ring_one(0)
    forward_step(2)
    forward_step(3)
    mid_step(3)
    ring_one(1)
    ring_two(0)
    pass_step(2)
    rows_step(0)
    ring_two(1)
    pass_step(3)
    rows_step(1)
    rows_step(2)
    rows_step(3)
    for k in range(CH):
        with scope(f"chunk_one_{k}"):
            row_chunk(1, k)
        if k >= 2:
            with scope(f"mate_one_{k - 2}"):
                sums_out(k - 2)
    with scope("mate_one_late"):
        sums_out(CH - 2)
    with scope("mate_one_last"):
        sums_out(CH - 1)
    with scope("drain"):
        seven = pl.ds(0, DEVS - 1)
        sent = (
            (S_ROUTE, route_g.at[seven]), (S_Y, y_g.at[0, seven]), (S_Y + 1, y_g.at[1, seven]), (S_DY, dy_g.at[0, seven]), (S_DY + 1, dy_g.at[1, seven]), (S_X, x_g.at[seven]), (S_D1, d1_g.at[:, seven]),
            (S_D1 + 1, mate_recv), (S_D1 + 2, near_recv), (S_D1 + 3, last_recv),
        )
        for i, whole in sent:
            remote(whole, whole, send_sem.at[i], ag_recv.at[0, 0], mate).wait_send()


def main_call(routing, x, y, dy, weights_two, weights_one):
    vm = pl.BlockSpec(memory_space=pltpu.VMEM)
    hbm = pl.BlockSpec(memory_space=pl.ANY)
    rows_d = pltpu.VMEM((E, ROWS, D), BF16)
    rows_f = pltpu.VMEM((E, ROWS, F), BF16)
    sums = pltpu.VMEM((TOK, D), F32)
    saved = (rows_d, rows_d, rows_f, rows_f, rows_f)
    w_up = pltpu.VMEM((E, D, F), BF16)
    w_dn = pltpu.VMEM((E, F, D), BF16)
    dma = pltpu.SemaphoreType.DMA
    return pl.pallas_call(
        main_kernel,
        out_shape=(sums, pltpu.VMEM((TOK, D), BF16), sums, sums, sums) + saved + saved,
        in_specs=[hbm] * 15,
        out_specs=(vm,) * 15,
        scratch_shapes=[
            (w_up, w_up, w_dn, w_up, w_up, w_dn),
            pltpu.VMEM((4, 8, TOK), jnp.int32),
            pltpu.VMEM((2, 8, TOK), F32),
            pltpu.VMEM((16, 2 * TOK), F32),
            pltpu.VMEM((DEVS, 16, 2 * TOK), F32),
            pltpu.VMEM((2, DEVS, TOK, HW), BF16),
            pltpu.VMEM((2, DEVS, TOK, HW), BF16),
            pltpu.VMEM((DEVS, TOK, D), BF16),
            pltpu.VMEM((CH, DEVS, TOK, CW), BF16),
            pltpu.VMEM((E, ROWS, F), F32),
            pltpu.VMEM((E, ROWS, F), F32),
            pltpu.VMEM((E, ROWS, F), F32),
            pltpu.VMEM((2, CHIPS, E, PAIR, CW), BF16),
            pltpu.VMEM((CHIPS, PROWS, 2 * TOK), BF16),
            pltpu.VMEM((CHIPS, 2 * TOK, PROWS), BF16),
            pltpu.VMEM((CHIPS, PROWS, 1), F32),
            pltpu.VMEM((2, CH, 2, CHIPS, TOK, CW), F32),
            pltpu.VMEM((2, CH, CHIPS, TOK, CW), F32),
            pltpu.VMEM((CH, 2, TOK, CW), F32),
            pltpu.VMEM((CH, TOK, CW), F32),
            dma((2,)),
            dma((5,)),
            dma((6,)),
            dma((S_D1 + 4,)),
            dma((N_STREAMS, 4)),
            dma((2, CH)),
            dma((CH, 2)),
            dma((CH,)),
        ],
        compiler_params=pltpu.CompilerParams(collective_id=0, has_side_effects=True, vmem_limit_bytes=MAIN_VMEM),
        name="moe_backward",
    )(*routing, x, y, dy, *weights_two, *weights_one)


def wgrad_kernel(*refs):
    saved, outs, bufs, out_sem = (refs[0:5], refs[5:10]), (refs[10:13], refs[13:16]), refs[16:19], refs[19]

    def out_copy(layer, m, e, slot, h):
        n = bufs[m].shape[1] // HALVES
        rows = pl.ds(h * n, n)
        return pltpu.make_async_copy(bufs[m].at[slot, rows], outs[layer][m].at[e, rows], out_sem.at[slot, m, h])

    for layer in range(2):
        xr, zr, hid, da, db = saved[layer]

        @pl.loop(0, E)
        def _(e):
            i = layer * E + e
            slot = lax.rem(i, SETS)
            for m, lhs, rhs in ((2, hid, zr), (0, xr, da), (1, xr, db)):
                n = bufs[m].shape[1] // HALVES
                for h in range(HALVES):
                    rows = slice(h * n, (h + 1) * n)

                    @pl.when(i >= SETS)
                    def _():
                        out_copy(layer, m, e, slot, h).wait()

                    bufs[m][slot, rows] = tn_dot(lhs[e, :, rows], rhs[e])
                    out_copy(layer, m, e, slot, h).start()

    for i in range(2 * E - SETS, 2 * E):
        for m in (2, 0, 1):
            for h in range(HALVES):
                out_copy(i // E, m, i % E, i % SETS, h).wait()


def wgrad_call(*saved):
    up = jax.ShapeDtypeStruct((E, D, F), F32)
    dn = jax.ShapeDtypeStruct((E, F, D), F32)
    hbm = pl.BlockSpec(memory_space=pl.ANY)
    return pl.pallas_call(
        wgrad_kernel,
        out_shape=(up, up, dn) * 2,
        in_specs=[pl.BlockSpec(memory_space=pltpu.VMEM)] * 10,
        out_specs=(hbm,) * 6,
        scratch_shapes=[
            pltpu.VMEM((SETS, D, F), F32),
            pltpu.VMEM((SETS, D, F), F32),
            pltpu.VMEM((SETS, F, D), F32),
            pltpu.SemaphoreType.DMA((SETS, 3, HALVES)),
        ],
        compiler_params=pltpu.CompilerParams(vmem_limit_bytes=WGRAD_VMEM),
        cost_estimate=pl.CostEstimate(flops=12 * E * ROWS * D * F, bytes_accessed=24 * E * D * F, transcendentals=0),
        name="weight_grads",
    )(*saved)


def solution(mesh):
    tok_spec = P(("data", "expert"), None)
    weight_spec = P("expert", None, None)
    grad_spec = P(("data", "expert"), None, None)

    def local_step(x_tokens, y_mid, dy_out, experts_one, gates_one, slots_one, experts_two, gates_two, slots_two, w_gate_one, w_up_one, w_down_one, w_gate_two, w_up_two, w_down_two):
        routing = [a.T for a in (experts_two, gates_two, slots_two, experts_one, gates_one, slots_one)]
        got = main_call(routing, x_tokens, y_mid, dy_out, (w_gate_two, w_up_two, w_down_two), (w_gate_one, w_up_one, w_down_one))
        own, d1 = got[0:2]
        far = [lax.ppermute(got[2 + i], "expert", [(d, d ^ flip) for d in range(DEVS)]) for i, flip in enumerate((2, 4, 6))]
        grads = wgrad_call(*got[5:15])
        dx = (d1.astype(F32) + (own + (far[0] + far[1] + far[2]))).astype(BF16)
        return (dx,) + tuple(grads[3:6]) + tuple(grads[0:3])

    return jax.shard_map(local_step, mesh=mesh, in_specs=(tok_spec,) * 9 + (weight_spec,) * 6, out_specs=(tok_spec,) + (grad_spec,) * 6, check_vma=False)
```

```python
import functools
import jax
import jax.numpy as jnp
from jax import lax
from jax.experimental import pallas as pl
from jax.experimental.pallas import tpu as pltpu
from jax.sharding import PartitionSpec as P

MESH = pl.DeviceIdType.MESH
scope = jax.named_scope
F32 = jnp.float32
BF16 = jnp.bfloat16

TOK = 64
CHIPS = 4
DEVS = 8
D = 1024
F = 512
E = 4
CAP = 24
PAIR = 2 * CAP
ROWS = CHIPS * PAIR
PROWS = E * PAIR
CH = 4
CW = D // CH
MAIN_VMEM = 51_000_000
WGRAD_VMEM = 40_000_000

S_ROUTE, S_Y, S_DY, S_X, S_D1 = 0, 1, 3, 5, 6
N_STREAMS = S_D1 + CH
HW = D // 2

SETS = 2
HALVES = 1


def nt_dot(a, b):
    return lax.dot_general(a, b, (((1,), (1,)), ((), ())), preferred_element_type=F32)


def tn_dot(a, b):
    return lax.dot_general(a, b, (((0,), (0,)), ((), ())), preferred_element_type=F32)


def nn_dot(a, b):
    return jnp.dot(a, b, preferred_element_type=F32)


def main_kernel(
    experts_b, gates_b, slots_b, experts_a, gates_a, slots_a,
    x_hbm, y_hbm, dy_hbm, w1b_hbm, w3b_hbm, w2b_hbm, w1a_hbm, w3a_hbm, w2a_hbm,
    own_ref, d1_ref, far0_ref, far1_ref, far2_ref,
    xr_two, zr_two, hid_two, da_two, db_two, xr_one, zr_one, hid_one, da_one, db_one,
    w_vm, w3_turned, choice_i, choice_f, route_own, route_g, y_g, dy_g, x_g, d1_g,
    act_s, act_f, dh_sum, dxp, perm, perm_t, gate,
    part, mate_recv, near_recv, last_recv,
    choice_sem, tile_sem, w_sem, send_sem, ag_recv, mate_sem, near_sem, last_sem,
):
    xr, zr, hid = (xr_two, xr_one), (zr_two, zr_one), (hid_two, hid_one)
    da, db = (da_two, da_one), (db_two, db_one)
    me = lax.axis_index("expert")
    core = lax.rem(me, 2)
    xpos = lax.rem(me // 2, 2)
    ypos = me // 4
    mate = me + 1 - 2 * core
    nx = me + 2 - 4 * xpos
    ny = me + 4 - 8 * ypos
    nd = ny + 2 - 4 * xpos
    na = nx + core * (ny - nx)
    nb = ny + core * (nx - ny)

    def remote(src, dst, send, recv, dev):
        return pltpu.make_async_remote_copy(src_ref=src, dst_ref=dst, send_sem=send, recv_sem=recv, device_id={"expert": dev}, device_id_type=MESH)

    barrier = pltpu.get_barrier_semaphore()
    for dev in (mate, nx, ny, nd):
        pl.semaphore_signal(barrier, inc=1, device_id={"expert": dev}, device_id_type=MESH)

    choices = [
        pltpu.make_async_copy(src, dst, choice_sem.at[i])
        for i, src, dst in (
            (0, experts_b, choice_i.at[0]), (0, slots_b, choice_i.at[1]), (1, gates_b, choice_f.at[0]),
            (0, experts_a, choice_i.at[2]), (0, slots_a, choice_i.at[3]), (1, gates_a, choice_f.at[1]),
        )
    ]
    tiles = [
        pltpu.make_async_copy(src, dst.at[me], tile_sem.at[i])
        for i, (src, dst) in enumerate((
            (y_hbm.at[:, pl.ds(0, HW)], y_g.at[0]), (y_hbm.at[:, pl.ds(HW, HW)], y_g.at[1]),
            (dy_hbm.at[:, pl.ds(0, HW)], dy_g.at[0]), (dy_hbm.at[:, pl.ds(HW, HW)], dy_g.at[1]), (x_hbm, x_g),
        ))
    ]
    w_hbm = (w1b_hbm, w3b_hbm, w2b_hbm, w1a_hbm, w3a_hbm, w2a_hbm)

    def w_copy(i):
        return pltpu.make_async_copy(w_hbm[i], w_vm[i], w_sem.at[i])

    for c in choices + tiles:
        c.start()

    for i, whole in enumerate((choice_i, choice_f)):
        pltpu.make_async_copy(whole, whole, choice_sem.at[i]).wait()
    for layer in range(2):
        lanes = slice(layer * TOK, (layer + 1) * TOK)
        slot = choice_i[2 * layer + 1]
        code = jnp.where(slot >= 0, choice_i[2 * layer] * PAIR + core * CAP + slot, -1).astype(F32)
        route_own[0:8, lanes] = code
        route_own[8:16, lanes] = choice_f[layer]
    route_g[me] = route_own[...]
    for c in tiles:
        c.wait()
    pl.semaphore_wait(barrier, 4)

    far = ((0, na), (1, nb), (3, nd))

    def ag_send(stream, k, src, dst, dev):
        remote(src, dst, send_sem.at[min(stream, S_D1)], ag_recv.at[stream, k], dev).start()

    def ag_start(stream, src, buf):
        for k, dev in far + ((2, mate),):
            ag_send(stream, k, src, buf.at[me], dev)

    def ag_got(stream, k, buf):
        remote(buf, buf, send_sem.at[min(stream, S_D1)], ag_recv.at[stream, k], mate).wait_recv()

    def ag_pass_on(stream, buf):
        for k, dev in far:
            ag_got(stream, k, buf.at[dev])
            ag_send(stream, 2, buf.at[dev], buf.at[dev], mate)

    def ag_finish(stream, buf):
        ag_got(stream, 2, buf.at[pl.ds(0, CHIPS)])

    def ring_start(stream, buf):
        for k, dev in ((0, na), (1, nb), (2, mate)):
            ag_send(stream, k, buf.at[me], buf.at[me], dev)

    def ring_step(stream, buf):
        ag_got(stream, 0, buf.at[na])
        ag_send(stream, 3, buf.at[na], buf.at[na], nb)
        ag_send(stream, 2, buf.at[na], buf.at[na], mate)
        ag_got(stream, 1, buf.at[nb])
        ag_send(stream, 2, buf.at[nb], buf.at[nb], mate)

    def ring_last(stream, buf):
        ag_got(stream, 3, buf.at[nd])
        ag_send(stream, 2, buf.at[nd], buf.at[nd], mate)

    def build_routes(layer):
        base = (me * PROWS).astype(F32)
        row_id = lax.broadcasted_iota(jnp.int32, (PROWS, 2 * TOK), 0).astype(F32)
        lane = lax.broadcasted_iota(jnp.int32, (16, 2 * TOK), 1)
        for p in range(CHIPS):
            halves = [route_g[2 * p], route_g[2 * p + 1]]
            halves[1 - layer] = pltpu.roll(halves[1 - layer], TOK, 1)
            both = jnp.where(lane < TOK, halves[0], halves[1])
            target = both[0:8] - base
            gates = both[8:16]
            hit = jnp.zeros((PROWS, 2 * TOK), F32)
            gsum = jnp.zeros((PROWS, 2 * TOK), F32)
            for j in range(8):
                m = row_id == target[j : j + 1, :]
                hit = jnp.where(m, 1.0, hit)
                gsum = jnp.where(m, gates[j : j + 1, :], gsum)
            perm[p] = hit.astype(BF16)
            perm_t[p] = hit.T.astype(BF16)
            gate[p] = jnp.sum(gsum, axis=1, keepdims=True)

    def gather_rows(tokens, dst, layer, cols, gated):
        for p in range(CHIPS):
            got = nn_dot(perm[p], tokens(p))
            if gated:
                got = got * gate[p]
            got = got.astype(BF16)
            for e in range(E):
                dst[layer][e, p * PAIR : (p + 1) * PAIR, cols] = got[e * PAIR : (e + 1) * PAIR]

    def activate(layer, e, a, b):
        a = a.astype(BF16).astype(F32)
        b = b.astype(BF16).astype(F32)
        sig = jax.nn.sigmoid(a)
        s = a * sig
        act_s[e] = s
        act_f[e] = b * (sig * (1.0 + a * (1.0 - sig)))
        hid[layer][e] = (s * b).astype(BF16)

    def forward_expert(layer, e):
        rows = xr[layer][e]
        activate(layer, e, nn_dot(rows, w_vm[3 * layer][e]), nn_dot(rows, w_vm[3 * layer + 1][e]))

    def forward_half(e, h):
        cols = slice(h * HW, (h + 1) * HW)
        a = nn_dot(xr[0][e, :, cols], w_vm[0][e, cols, :])
        b = nn_dot(xr[0][e, :, cols], w_vm[1][e, cols, :])
        if h == 0:
            act_s[e] = a
            act_f[e] = b
        else:
            activate(0, e, act_s[e] + a, act_f[e] + b)

    def hidden_expert(layer, e, dh):
        da[layer][e] = (dh * act_f[e]).astype(BF16)
        db[layer][e] = (dh * act_s[e]).astype(BF16)

    w2_turned, w1_turned = w_vm[3], w_vm[2]

    def turn_two(experts):
        with scope("turn_two"):
            for e in experts:
                w2_turned[e] = w_vm[2][e].T

    def turn_one(tasks):
        with scope("turn_one"):
            for e, src, dst in tasks:
                dst[e] = src[e].T

    def row_chunk(layer, k):
        w1, w3 = w_vm[3 * layer], w_vm[3 * layer + 1]
        cols = slice(k * CW, (k + 1) * CW)
        for e in range(E):
            if layer == 0:
                g = nt_dot(da[0][e], w1[e, cols, :]) + nt_dot(db[0][e], w3[e, cols, :])
            else:
                g = nn_dot(da[1][e], w1_turned[e, :, cols]) + nn_dot(db[1][e], w3_turned[e, :, cols])
            g = g.astype(BF16)
            for p in range(CHIPS):
                dxp[k % 2, p, e] = g[p * PAIR : (p + 1) * PAIR]
        for p in range(CHIPS):
            r = nn_dot(perm_t[p], dxp[k % 2, p].reshape(PROWS, CW))
            part[layer, k, 0, p] = r[:TOK]
            part[layer, k, 1, p] = r[TOK:]
        mate_copy(layer, k).start()

    def mate_copy(layer, k):
        return remote(part.at[layer, k, 1 - core], mate_recv.at[layer, k], send_sem.at[S_D1 + 1], mate_sem.at[layer, k], mate)

    def near_copy(k, i):
        return remote(part.at[0, k, core, (nd, na)[i] // 2], near_recv.at[k, i], send_sem.at[S_D1 + 2], near_sem.at[k, i], na)

    def last_copy(k):
        return remote(part.at[0, k, core, nb // 2], last_recv.at[k], send_sem.at[S_D1 + 3], last_sem.at[k], nb)

    def near_start(k):
        mate_copy(0, k).wait_recv()
        for p in range(CHIPS):
            part[0, k, core, p] = part[0, k, core, p] + mate_recv[0, k, p]
        near_copy(k, 0).start()
        near_copy(k, 1).start()

    def last_start(k):
        near_copy(k, 0).wait_recv()
        part[0, k, core, nb // 2] = part[0, k, core, nb // 2] + near_recv[k, 0]
        last_copy(k).start()

    def sums_out(k):
        mate_copy(1, k).wait_recv()
        cols = slice(k * CW, (k + 1) * CW)
        for dev, out in ((me, own_ref), (nx, far0_ref), (ny, far1_ref), (nd, far2_ref)):
            out[:, cols] = part[1, k, core, dev // 2] + mate_recv[1, k, dev // 2]

    def pair_of(buf, p):
        return buf[2 * p : 2 * p + 2].reshape(2 * TOK, buf.shape[-1])

    with scope("start"):
        ag_start(S_ROUTE, route_own, route_g)
        for h in range(2):
            ring_start(S_Y + h, y_g.at[h])
        for h in range(2):
            ring_start(S_DY + h, dy_g.at[h])
        for i in (2, 0, 1, 4, 5):
            w_copy(i).start()

    def y_step(h):
        with scope(f"y_step_{h}"):
            ring_step(S_Y + h, y_g.at[h])

    def y_last(h):
        with scope(f"y_last_{h}"):
            ring_last(S_Y + h, y_g.at[h])

    def dy_step(h):
        with scope(f"dy_step_{h}"):
            ring_step(S_DY + h, dy_g.at[h])

    def dy_last(h):
        with scope(f"dy_last_{h}"):
            ring_last(S_DY + h, dy_g.at[h])

    def half_cols(h):
        return slice(h * HW, (h + 1) * HW)

    def y_rows(h):
        with scope(f"y_finish_{h}"):
            ag_finish(S_Y + h, y_g.at[h])
        with scope(f"rows_y_{h}"):
            gather_rows(lambda p: pair_of(y_g.at[h], p), xr, 0, half_cols(h), False)

    def dy_rows(h):
        with scope(f"dy_finish_{h}"):
            ag_finish(S_DY + h, dy_g.at[h])
        with scope(f"rows_dy_{h}"):
            gather_rows(lambda p: pair_of(dy_g.at[h], p), zr, 0, half_cols(h), True)

    def forward_part(h, experts):
        with scope(f"forward_two_{h}"):
            for e in experts:
                forward_half(e, h)

    with scope("route"):
        ag_pass_on(S_ROUTE, route_g)
        ag_finish(S_ROUTE, route_g)
    y_step(0)
    y_step(1)
    with scope("build_two"):
        build_routes(0)
    w_copy(2).wait()
    turn_two((0,))
    dy_step(0)
    turn_two((1, 2))
    y_last(0)
    turn_two((3,))
    dy_step(1)
    y_last(1)
    for i in range(2):
        w_copy(i).wait()
    y_rows(0)
    forward_part(0, range(E))
    dy_last(0)
    y_rows(1)
    forward_part(1, range(2))
    dy_last(1)
    with scope("x_start"):
        ag_start(S_X, x_g.at[me], x_g)
    forward_part(1, range(2, E))
    dy_rows(0)
    dy_rows(1)
    with scope("hidden_two"):
        for e in range(E):
            hidden_expert(0, e, nn_dot(zr[0][e], w2_turned[e]))
        w_copy(3).start()

    turns = [(e, w_vm[4], w3_turned) for e in range(E)] + [(e, w_vm[3], w1_turned) for e in range(E)]
    for k in range(CH):
        with scope(f"chunk_two_{k}"):
            row_chunk(0, k)
        if k == 3:
            w_copy(4).wait()
            turn_one(turns[0:1])
        if k >= 1:
            with scope(f"near_{k - 1}"):
                near_start(k - 1)
    turn_one(turns[1:3])
    with scope(f"near_{CH - 1}"):
        near_start(CH - 1)

    def last_step(k):
        with scope(f"last_{k}"):
            last_start(k)

    def x_wait():
        with scope("wait_x"):
            ag_pass_on(S_X, x_g)

    def x_build():
        with scope("build_one"):
            build_routes(1)

    def x_rows():
        with scope("rows_x"):
            ag_finish(S_X, x_g)
            gather_rows(lambda p: pair_of(x_g, p), xr, 1, slice(None), False)
            w_copy(5).wait()

    def ring_one(k):
        with scope(f"step_{k}"):
            ring_step(S_D1 + k, d1_g.at[k])

    def ring_two(k):
        with scope(f"last_d1_{k}"):
            ring_last(S_D1 + k, d1_g.at[k])

    def mid_grad(k):
        cols = slice(k * CW, (k + 1) * CW)
        near_copy(k, 1).wait_recv()
        last_copy(k).wait_recv()
        total = part[0, k, core, me // 2] + near_recv[k, 1] + last_recv[k]
        mine = (dy_g[k // 2, me, :, (k % 2) * CW : (k % 2 + 1) * CW].astype(F32) + total).astype(BF16)
        d1_ref[:, cols] = mine
        d1_g[k, me] = mine
        if k < 1:
            ring_start(S_D1 + k, d1_g.at[k])
        else:
            ag_start(S_D1 + k, d1_g.at[k, me], d1_g.at[k])

    def mid_rows(k):
        cols = slice(k * CW, (k + 1) * CW)
        gather_rows(lambda p: pair_of(d1_g.at[k], p), zr, 1, cols, True)

    parts_done = []

    def hidden_part(k):
        cols = slice(k * CW, (k + 1) * CW)
        parts_done.append(k)
        for e in range(E):
            dh = nt_dot(zr[1][e, :, cols], w_vm[5][e, :, cols])
            if len(parts_done) > 1:
                dh = dh_sum[e] + dh
            if len(parts_done) < CH:
                dh_sum[e] = dh
            else:
                hidden_expert(1, e, dh)

    def mid_step(k):
        with scope(f"mid_{k}"):
            mid_grad(k)

    def pass_step(k):
        with scope(f"pass_on_{k}"):
            ag_pass_on(S_D1 + k, d1_g.at[k])

    def rows_step(k):
        with scope(f"finish_{k}"):
            ag_finish(S_D1 + k, d1_g.at[k])
        with scope(f"rows_d1_{k}"):
            mid_rows(k)
            hidden_part(k)

    def forward_step(k):
        with scope(f"forward_one_{k}"):
            forward_expert(1, k)

    last_step(0)
    x_wait()
    x_build()
    turn_one(turns[3:4])
    w_copy(3).wait()
    last_step(1)
    turn_one(turns[4:5])
    x_rows()
    turn_one(turns[5:6])
    last_step(2)
    turn_one(turns[6:7])
    mid_step(0)
    forward_step(0)
    turn_one(turns[7:8])
    last_step(3)
    mid_step(1)
    mid_step(2)
    forward_step(1)
    ring_one(0)
    forward_step(2)
    forward_step(3)
    mid_step(3)
    pass_step(1)
    pass_step(2)
    ring_two(0)
    rows_step(1)
    rows_step(0)
    pass_step(3)
    rows_step(2)
    rows_step(3)
    for k in range(CH):
        with scope(f"chunk_one_{k}"):
            row_chunk(1, k)
        if k >= 2:
            with scope(f"mate_one_{k - 2}"):
                sums_out(k - 2)
    with scope("mate_one_late"):
        sums_out(CH - 2)
    with scope("mate_one_last"):
        sums_out(CH - 1)
    with scope("drain"):
        seven = pl.ds(0, DEVS - 1)
        sent = (
            (S_ROUTE, route_g.at[seven]), (S_Y, y_g.at[0, seven]), (S_Y + 1, y_g.at[1, seven]), (S_DY, dy_g.at[0, seven]), (S_DY + 1, dy_g.at[1, seven]), (S_X, x_g.at[seven]), (S_D1, d1_g.at[:, seven]),
            (S_D1 + 1, mate_recv), (S_D1 + 2, near_recv), (S_D1 + 3, last_recv),
        )
        for i, whole in sent:
            remote(whole, whole, send_sem.at[i], ag_recv.at[0, 0], mate).wait_send()


def main_call(routing, x, y, dy, weights_two, weights_one):
    vm = pl.BlockSpec(memory_space=pltpu.VMEM)
    hbm = pl.BlockSpec(memory_space=pl.ANY)
    rows_d = pltpu.VMEM((E, ROWS, D), BF16)
    rows_f = pltpu.VMEM((E, ROWS, F), BF16)
    sums = pltpu.VMEM((TOK, D), F32)
    saved = (rows_d, rows_d, rows_f, rows_f, rows_f)
    w_up = pltpu.VMEM((E, D, F), BF16)
    w_dn = pltpu.VMEM((E, F, D), BF16)
    dma = pltpu.SemaphoreType.DMA
    return pl.pallas_call(
        main_kernel,
        out_shape=(sums, pltpu.VMEM((TOK, D), BF16), sums, sums, sums) + saved + saved,
        in_specs=[hbm] * 15,
        out_specs=(vm,) * 15,
        scratch_shapes=[
            (w_up, w_up, w_dn, w_up, w_up, w_dn),
            w_dn,
            pltpu.VMEM((4, 8, TOK), jnp.int32),
            pltpu.VMEM((2, 8, TOK), F32),
            pltpu.VMEM((16, 2 * TOK), F32),
            pltpu.VMEM((DEVS, 16, 2 * TOK), F32),
            pltpu.VMEM((2, DEVS, TOK, HW), BF16),
            pltpu.VMEM((2, DEVS, TOK, HW), BF16),
            pltpu.VMEM((DEVS, TOK, D), BF16),
            pltpu.VMEM((CH, DEVS, TOK, CW), BF16),
            pltpu.VMEM((E, ROWS, F), F32),
            pltpu.VMEM((E, ROWS, F), F32),
            pltpu.VMEM((E, ROWS, F), F32),
            pltpu.VMEM((2, CHIPS, E, PAIR, CW), BF16),
            pltpu.VMEM((CHIPS, PROWS, 2 * TOK), BF16),
            pltpu.VMEM((CHIPS, 2 * TOK, PROWS), BF16),
            pltpu.VMEM((CHIPS, PROWS, 1), F32),
            pltpu.VMEM((2, CH, 2, CHIPS, TOK, CW), F32),
            pltpu.VMEM((2, CH, CHIPS, TOK, CW), F32),
            pltpu.VMEM((CH, 2, TOK, CW), F32),
            pltpu.VMEM((CH, TOK, CW), F32),
            dma((2,)),
            dma((5,)),
            dma((6,)),
            dma((S_D1 + 4,)),
            dma((N_STREAMS, 4)),
            dma((2, CH)),
            dma((CH, 2)),
            dma((CH,)),
        ],
        compiler_params=pltpu.CompilerParams(collective_id=0, has_side_effects=True, vmem_limit_bytes=MAIN_VMEM),
        name="moe_backward",
    )(*routing, x, y, dy, *weights_two, *weights_one)


def wgrad_kernel(*refs):
    saved, outs, bufs, out_sem = (refs[0:5], refs[5:10]), (refs[10:13], refs[13:16]), refs[16:19], refs[19]

    def out_copy(layer, m, e, slot, h):
        n = bufs[m].shape[1] // HALVES
        rows = pl.ds(h * n, n)
        return pltpu.make_async_copy(bufs[m].at[slot, rows], outs[layer][m].at[e, rows], out_sem.at[slot, m, h])

    for layer in range(2):
        xr, zr, hid, da, db = saved[layer]

        @pl.loop(0, E)
        def _(e):
            i = layer * E + e
            slot = lax.rem(i, SETS)
            for m, lhs, rhs in ((2, hid, zr), (0, xr, da), (1, xr, db)):
                n = bufs[m].shape[1] // HALVES
                for h in range(HALVES):
                    rows = slice(h * n, (h + 1) * n)

                    @pl.when(i >= SETS)
                    def _():
                        out_copy(layer, m, e, slot, h).wait()

                    bufs[m][slot, rows] = tn_dot(lhs[e, :, rows], rhs[e])
                    out_copy(layer, m, e, slot, h).start()

    for i in range(2 * E - SETS, 2 * E):
        for m in (2, 0, 1):
            for h in range(HALVES):
                out_copy(i // E, m, i % E, i % SETS, h).wait()


def wgrad_call(*saved):
    up = jax.ShapeDtypeStruct((E, D, F), F32)
    dn = jax.ShapeDtypeStruct((E, F, D), F32)
    hbm = pl.BlockSpec(memory_space=pl.ANY)
    return pl.pallas_call(
        wgrad_kernel,
        out_shape=(up, up, dn) * 2,
        in_specs=[pl.BlockSpec(memory_space=pltpu.VMEM)] * 10,
        out_specs=(hbm,) * 6,
        scratch_shapes=[
            pltpu.VMEM((SETS, D, F), F32),
            pltpu.VMEM((SETS, D, F), F32),
            pltpu.VMEM((SETS, F, D), F32),
            pltpu.SemaphoreType.DMA((SETS, 3, HALVES)),
        ],
        compiler_params=pltpu.CompilerParams(vmem_limit_bytes=WGRAD_VMEM),
        cost_estimate=pl.CostEstimate(flops=12 * E * ROWS * D * F, bytes_accessed=24 * E * D * F, transcendentals=0),
        name="weight_grads",
    )(*saved)


def solution(mesh):
    tok_spec = P(("data", "expert"), None)
    weight_spec = P("expert", None, None)
    grad_spec = P(("data", "expert"), None, None)

    def local_step(x_tokens, y_mid, dy_out, experts_one, gates_one, slots_one, experts_two, gates_two, slots_two, w_gate_one, w_up_one, w_down_one, w_gate_two, w_up_two, w_down_two):
        routing = [a.T for a in (experts_two, gates_two, slots_two, experts_one, gates_one, slots_one)]
        got = main_call(routing, x_tokens, y_mid, dy_out, (w_gate_two, w_up_two, w_down_two), (w_gate_one, w_up_one, w_down_one))
        own, d1 = got[0:2]
        far = [lax.ppermute(got[2 + i], "expert", [(d, d ^ flip) for d in range(DEVS)]) for i, flip in enumerate((2, 4, 6))]
        grads = wgrad_call(*got[5:15])
        dx = (d1.astype(F32) + (own + (far[0] + far[1] + far[2]))).astype(BF16)
        return (dx,) + tuple(grads[3:6]) + tuple(grads[0:3])

    return jax.shard_map(local_step, mesh=mesh, in_specs=(tok_spec,) * 9 + (weight_spec,) * 6, out_specs=(tok_spec,) + (grad_spec,) * 6, check_vma=False)
```

```python
import functools
import jax
import jax.numpy as jnp
from jax import lax
from jax.experimental import pallas as pl
from jax.experimental.pallas import tpu as pltpu
from jax.sharding import PartitionSpec as P

MESH = pl.DeviceIdType.MESH
scope = jax.named_scope
F32 = jnp.float32
BF16 = jnp.bfloat16

TOK = 64
CHIPS = 4
DEVS = 8
D = 1024
F = 512
E = 4
CAP = 24
PAIR = 2 * CAP
ROWS = CHIPS * PAIR
PROWS = E * PAIR
CH = 4
CW = D // CH
MAIN_VMEM = 51_000_000
WGRAD_VMEM = 40_000_000

S_ROUTE, S_Y, S_DY, S_X, S_D1 = 0, 1, 3, 5, 6
N_STREAMS = S_D1 + CH
HW = D // 2

SETS = 2
HALVES = 1


def nt_dot(a, b):
    return lax.dot_general(a, b, (((1,), (1,)), ((), ())), preferred_element_type=F32)


def tn_dot(a, b):
    return lax.dot_general(a, b, (((0,), (0,)), ((), ())), preferred_element_type=F32)


def nn_dot(a, b):
    return jnp.dot(a, b, preferred_element_type=F32)


def main_kernel(
    experts_b, gates_b, slots_b, experts_a, gates_a, slots_a,
    x_hbm, y_hbm, dy_hbm, w1b_hbm, w3b_hbm, w2b_hbm, w1a_hbm, w3a_hbm, w2a_hbm,
    own_ref, d1_ref, far0_ref, far1_ref, far2_ref,
    xr_two, zr_two, hid_two, da_two, db_two, xr_one, zr_one, hid_one, da_one, db_one,
    w_vm, w3_turned, choice_i, choice_f, route_own, route_g, y_g, dy_g, x_g, d1_g,
    act_s, act_f, dh_sum, dxp, perm, perm_t, gate,
    part, mate_recv, near_recv, last_recv,
    choice_sem, tile_sem, w_sem, send_sem, ag_recv, mate_sem, near_sem, last_sem,
):
    xr, zr, hid = (xr_two, xr_one), (zr_two, zr_one), (hid_two, hid_one)
    da, db = (da_two, da_one), (db_two, db_one)
    me = lax.axis_index("expert")
    core = lax.rem(me, 2)
    xpos = lax.rem(me // 2, 2)
    ypos = me // 4
    mate = me + 1 - 2 * core
    nx = me + 2 - 4 * xpos
    ny = me + 4 - 8 * ypos
    nd = ny + 2 - 4 * xpos
    na = nx + core * (ny - nx)
    nb = ny + core * (nx - ny)

    def remote(src, dst, send, recv, dev):
        return pltpu.make_async_remote_copy(src_ref=src, dst_ref=dst, send_sem=send, recv_sem=recv, device_id={"expert": dev}, device_id_type=MESH)

    barrier = pltpu.get_barrier_semaphore()
    for dev in (mate, nx, ny, nd):
        pl.semaphore_signal(barrier, inc=1, device_id={"expert": dev}, device_id_type=MESH)

    choices = [
        pltpu.make_async_copy(src, dst, choice_sem.at[i])
        for i, src, dst in (
            (0, experts_b, choice_i.at[0]), (0, slots_b, choice_i.at[1]), (1, gates_b, choice_f.at[0]),
            (0, experts_a, choice_i.at[2]), (0, slots_a, choice_i.at[3]), (1, gates_a, choice_f.at[1]),
        )
    ]
    tiles = [
        pltpu.make_async_copy(src, dst.at[me], tile_sem.at[i])
        for i, (src, dst) in enumerate((
            (y_hbm.at[:, pl.ds(0, HW)], y_g.at[0]), (y_hbm.at[:, pl.ds(HW, HW)], y_g.at[1]),
            (dy_hbm.at[:, pl.ds(0, HW)], dy_g.at[0]), (dy_hbm.at[:, pl.ds(HW, HW)], dy_g.at[1]), (x_hbm, x_g),
        ))
    ]
    w_hbm = (w1b_hbm, w3b_hbm, w2b_hbm, w1a_hbm, w3a_hbm, w2a_hbm)

    def w_copy(i):
        return pltpu.make_async_copy(w_hbm[i], w_vm[i], w_sem.at[i])

    for c in choices + tiles:
        c.start()

    for i, whole in enumerate((choice_i, choice_f)):
        pltpu.make_async_copy(whole, whole, choice_sem.at[i]).wait()
    for layer in range(2):
        lanes = slice(layer * TOK, (layer + 1) * TOK)
        slot = choice_i[2 * layer + 1]
        code = jnp.where(slot >= 0, choice_i[2 * layer] * PAIR + core * CAP + slot, -1).astype(F32)
        route_own[0:8, lanes] = code
        route_own[8:16, lanes] = choice_f[layer]
    route_g[me] = route_own[...]
    for c in tiles:
        c.wait()
    pl.semaphore_wait(barrier, 4)

    far = ((0, na), (1, nb), (3, nd))

    def ag_send(stream, k, src, dst, dev):
        remote(src, dst, send_sem.at[min(stream, S_D1)], ag_recv.at[stream, k], dev).start()

    def ag_start(stream, src, buf):
        for k, dev in far + ((2, mate),):
            ag_send(stream, k, src, buf.at[me], dev)

    def ag_got(stream, k, buf):
        remote(buf, buf, send_sem.at[min(stream, S_D1)], ag_recv.at[stream, k], mate).wait_recv()

    def ag_pass_on(stream, buf):
        for k, dev in far:
            ag_got(stream, k, buf.at[dev])
            ag_send(stream, 2, buf.at[dev], buf.at[dev], mate)

    def ag_finish(stream, buf):
        ag_got(stream, 2, buf.at[pl.ds(0, CHIPS)])

    def ring_start(stream, buf):
        for k, dev in ((0, na), (1, nb), (2, mate)):
            ag_send(stream, k, buf.at[me], buf.at[me], dev)

    def ring_step(stream, buf):
        ag_got(stream, 0, buf.at[na])
        ag_send(stream, 3, buf.at[na], buf.at[na], nb)
        ag_send(stream, 2, buf.at[na], buf.at[na], mate)
        ag_got(stream, 1, buf.at[nb])
        ag_send(stream, 2, buf.at[nb], buf.at[nb], mate)

    def ring_last(stream, buf):
        ag_got(stream, 3, buf.at[nd])
        ag_send(stream, 2, buf.at[nd], buf.at[nd], mate)

    def build_routes(layer):
        base = (me * PROWS).astype(F32)
        row_id = lax.broadcasted_iota(jnp.int32, (PROWS, 2 * TOK), 0).astype(F32)
        lane = lax.broadcasted_iota(jnp.int32, (16, 2 * TOK), 1)
        for p in range(CHIPS):
            halves = [route_g[2 * p], route_g[2 * p + 1]]
            halves[1 - layer] = pltpu.roll(halves[1 - layer], TOK, 1)
            both = jnp.where(lane < TOK, halves[0], halves[1])
            target = both[0:8] - base
            gates = both[8:16]
            hit = jnp.zeros((PROWS, 2 * TOK), F32)
            gsum = jnp.zeros((PROWS, 2 * TOK), F32)
            for j in range(8):
                m = row_id == target[j : j + 1, :]
                hit = jnp.where(m, 1.0, hit)
                gsum = jnp.where(m, gates[j : j + 1, :], gsum)
            perm[p] = hit.astype(BF16)
            perm_t[p] = hit.T.astype(BF16)
            gate[p] = jnp.sum(gsum, axis=1, keepdims=True)

    def gather_rows(tokens, dst, layer, cols, gated):
        for p in range(CHIPS):
            got = nn_dot(perm[p], tokens(p))
            if gated:
                got = got * gate[p]
            got = got.astype(BF16)
            for e in range(E):
                dst[layer][e, p * PAIR : (p + 1) * PAIR, cols] = got[e * PAIR : (e + 1) * PAIR]

    def activate(layer, e, a, b):
        a = a.astype(BF16).astype(F32)
        b = b.astype(BF16).astype(F32)
        sig = jax.nn.sigmoid(a)
        s = a * sig
        act_s[e] = s
        act_f[e] = b * (sig * (1.0 + a * (1.0 - sig)))
        hid[layer][e] = (s * b).astype(BF16)

    def forward_expert(layer, e):
        rows = xr[layer][e]
        activate(layer, e, nn_dot(rows, w_vm[3 * layer][e]), nn_dot(rows, w_vm[3 * layer + 1][e]))

    def forward_half(e, h):
        cols = slice(h * HW, (h + 1) * HW)
        a = nn_dot(xr[0][e, :, cols], w_vm[0][e, cols, :])
        b = nn_dot(xr[0][e, :, cols], w_vm[1][e, cols, :])
        if h == 0:
            act_s[e] = a
            act_f[e] = b
        else:
            activate(0, e, act_s[e] + a, act_f[e] + b)

    def hidden_expert(layer, e, dh):
        da[layer][e] = (dh * act_f[e]).astype(BF16)
        db[layer][e] = (dh * act_s[e]).astype(BF16)

    w2_turned, w1_turned = w_vm[3], w_vm[2]

    def turn_two(experts):
        with scope("turn_two"):
            for e in experts:
                w2_turned[e] = w_vm[2][e].T

    def turn_one(tasks):
        with scope("turn_one"):
            for e, src, dst in tasks:
                dst[e] = src[e].T

    def row_chunk(layer, k):
        w1, w3 = w_vm[3 * layer], w_vm[3 * layer + 1]
        cols = slice(k * CW, (k + 1) * CW)
        for e in range(E):
            if layer == 0:
                g = nt_dot(da[0][e], w1[e, cols, :]) + nt_dot(db[0][e], w3[e, cols, :])
            else:
                g = nn_dot(da[1][e], w1_turned[e, :, cols]) + nn_dot(db[1][e], w3_turned[e, :, cols])
            g = g.astype(BF16)
            for p in range(CHIPS):
                dxp[k % 2, p, e] = g[p * PAIR : (p + 1) * PAIR]
        for p in range(CHIPS):
            r = nn_dot(perm_t[p], dxp[k % 2, p].reshape(PROWS, CW))
            part[layer, k, 0, p] = r[:TOK]
            part[layer, k, 1, p] = r[TOK:]
        mate_copy(layer, k).start()

    def mate_copy(layer, k):
        return remote(part.at[layer, k, 1 - core], mate_recv.at[layer, k], send_sem.at[S_D1 + 1], mate_sem.at[layer, k], mate)

    def near_copy(k, i):
        return remote(part.at[0, k, core, (nd, na)[i] // 2], near_recv.at[k, i], send_sem.at[S_D1 + 2], near_sem.at[k, i], na)

    def last_copy(k):
        return remote(part.at[0, k, core, nb // 2], last_recv.at[k], send_sem.at[S_D1 + 3], last_sem.at[k], nb)

    def near_start(k):
        mate_copy(0, k).wait_recv()
        for p in range(CHIPS):
            part[0, k, core, p] = part[0, k, core, p] + mate_recv[0, k, p]
        near_copy(k, 0).start()
        near_copy(k, 1).start()

    def last_start(k):
        near_copy(k, 0).wait_recv()
        part[0, k, core, nb // 2] = part[0, k, core, nb // 2] + near_recv[k, 0]
        last_copy(k).start()

    def sums_out(k):
        mate_copy(1, k).wait_recv()
        cols = slice(k * CW, (k + 1) * CW)
        for dev, out in ((me, own_ref), (nx, far0_ref), (ny, far1_ref), (nd, far2_ref)):
            out[:, cols] = part[1, k, core, dev // 2] + mate_recv[1, k, dev // 2]

    def pair_of(buf, p):
        return buf[2 * p : 2 * p + 2].reshape(2 * TOK, buf.shape[-1])

    with scope("start"):
        ag_start(S_ROUTE, route_own, route_g)
        for h in range(2):
            ring_start(S_Y + h, y_g.at[h])
        for h in range(2):
            ring_start(S_DY + h, dy_g.at[h])
        for i in (2, 0, 1, 4, 5):
            w_copy(i).start()

    def y_step(h):
        with scope(f"y_step_{h}"):
            ring_step(S_Y + h, y_g.at[h])

    def y_last(h):
        with scope(f"y_last_{h}"):
            ring_last(S_Y + h, y_g.at[h])

    def dy_step(h):
        with scope(f"dy_step_{h}"):
            ring_step(S_DY + h, dy_g.at[h])

    def dy_last(h):
        with scope(f"dy_last_{h}"):
            ring_last(S_DY + h, dy_g.at[h])

    def half_cols(h):
        return slice(h * HW, (h + 1) * HW)

    def y_rows(h):
        with scope(f"y_finish_{h}"):
            ag_finish(S_Y + h, y_g.at[h])
        with scope(f"rows_y_{h}"):
            gather_rows(lambda p: pair_of(y_g.at[h], p), xr, 0, half_cols(h), False)

    def dy_rows(h):
        with scope(f"dy_finish_{h}"):
            ag_finish(S_DY + h, dy_g.at[h])
        with scope(f"rows_dy_{h}"):
            gather_rows(lambda p: pair_of(dy_g.at[h], p), zr, 0, half_cols(h), True)

    def forward_part(h, experts):
        with scope(f"forward_two_{h}"):
            for e in experts:
                forward_half(e, h)

    with scope("route"):
        ag_pass_on(S_ROUTE, route_g)
        ag_finish(S_ROUTE, route_g)
    y_step(0)
    y_step(1)
    with scope("build_two"):
        build_routes(0)
    w_copy(2).wait()
    turn_two((0,))
    dy_step(0)
    turn_two((1, 2))
    y_last(0)
    turn_two((3,))
    dy_step(1)
    y_last(1)
    for i in range(2):
        w_copy(i).wait()
    y_rows(0)
    forward_part(0, range(E))
    dy_last(0)
    with scope("x_start"):
        ag_start(S_X, x_g.at[me], x_g)
    y_rows(1)
    forward_part(1, range(2))
    dy_last(1)
    forward_part(1, range(2, E))
    dy_rows(0)
    dy_rows(1)
    with scope("hidden_two"):
        for e in range(E):
            hidden_expert(0, e, nn_dot(zr[0][e], w2_turned[e]))
        w_copy(3).start()

    turns = [(e, w_vm[4], w3_turned) for e in range(E)] + [(e, w_vm[3], w1_turned) for e in range(E)]
    for k in range(CH):
        with scope(f"chunk_two_{k}"):
            row_chunk(0, k)
        if k == 3:
            w_copy(4).wait()
            turn_one(turns[0:1])
        if k >= 1:
            with scope(f"near_{k - 1}"):
                near_start(k - 1)
    turn_one(turns[1:3])
    with scope(f"near_{CH - 1}"):
        near_start(CH - 1)

    def last_step(k):
        with scope(f"last_{k}"):
            last_start(k)

    def x_wait():
        with scope("wait_x"):
            ag_pass_on(S_X, x_g)

    def x_build():
        with scope("build_one"):
            build_routes(1)

    def x_rows():
        with scope("rows_x"):
            ag_finish(S_X, x_g)
            gather_rows(lambda p: pair_of(x_g, p), xr, 1, slice(None), False)
            w_copy(5).wait()

    def ring_one(k):
        with scope(f"step_{k}"):
            ring_step(S_D1 + k, d1_g.at[k])

    def ring_two(k):
        with scope(f"last_d1_{k}"):
            ring_last(S_D1 + k, d1_g.at[k])

    def mid_grad(k):
        cols = slice(k * CW, (k + 1) * CW)
        near_copy(k, 1).wait_recv()
        last_copy(k).wait_recv()
        total = part[0, k, core, me // 2] + near_recv[k, 1] + last_recv[k]
        mine = (dy_g[k // 2, me, :, (k % 2) * CW : (k % 2 + 1) * CW].astype(F32) + total).astype(BF16)
        d1_ref[:, cols] = mine
        d1_g[k, me] = mine
        if k < 1:
            ring_start(S_D1 + k, d1_g.at[k])
        else:
            ag_start(S_D1 + k, d1_g.at[k, me], d1_g.at[k])

    def mid_rows(k):
        cols = slice(k * CW, (k + 1) * CW)
        gather_rows(lambda p: pair_of(d1_g.at[k], p), zr, 1, cols, True)

    parts_done = []

    def hidden_part(k):
        cols = slice(k * CW, (k + 1) * CW)
        parts_done.append(k)
        for e in range(E):
            dh = nt_dot(zr[1][e, :, cols], w_vm[5][e, :, cols])
            if len(parts_done) > 1:
                dh = dh_sum[e] + dh
            if len(parts_done) < CH:
                dh_sum[e] = dh
            else:
                hidden_expert(1, e, dh)

    def mid_step(k):
        with scope(f"mid_{k}"):
            mid_grad(k)

    def pass_step(k):
        with scope(f"pass_on_{k}"):
            ag_pass_on(S_D1 + k, d1_g.at[k])

    def rows_step(k):
        with scope(f"finish_{k}"):
            ag_finish(S_D1 + k, d1_g.at[k])
        with scope(f"rows_d1_{k}"):
            mid_rows(k)
            hidden_part(k)

    def forward_step(k):
        with scope(f"forward_one_{k}"):
            forward_expert(1, k)

    last_step(0)
    x_wait()
    x_build()
    turn_one(turns[3:4])
    w_copy(3).wait()
    last_step(1)
    turn_one(turns[4:5])
    x_rows()
    turn_one(turns[5:6])
    last_step(2)
    turn_one(turns[6:7])
    mid_step(0)
    forward_step(0)
    turn_one(turns[7:8])
    last_step(3)
    mid_step(1)
    mid_step(2)
    forward_step(1)
    ring_one(0)
    forward_step(2)
    mid_step(3)
    forward_step(3)
    pass_step(1)
    pass_step(2)
    ring_two(0)
    rows_step(1)
    pass_step(3)
    rows_step(2)
    rows_step(0)
    rows_step(3)
    for k in range(CH):
        with scope(f"chunk_one_{k}"):
            row_chunk(1, k)
        if k >= 2:
            with scope(f"mate_one_{k - 2}"):
                sums_out(k - 2)
    with scope("mate_one_late"):
        sums_out(CH - 2)
    with scope("mate_one_last"):
        sums_out(CH - 1)
    with scope("drain"):
        seven = pl.ds(0, DEVS - 1)
        sent = (
            (S_ROUTE, route_g.at[seven]), (S_Y, y_g.at[0, seven]), (S_Y + 1, y_g.at[1, seven]), (S_DY, dy_g.at[0, seven]), (S_DY + 1, dy_g.at[1, seven]), (S_X, x_g.at[seven]), (S_D1, d1_g.at[:, seven]),
            (S_D1 + 1, mate_recv), (S_D1 + 2, near_recv), (S_D1 + 3, last_recv),
        )
        for i, whole in sent:
            remote(whole, whole, send_sem.at[i], ag_recv.at[0, 0], mate).wait_send()


def main_call(routing, x, y, dy, weights_two, weights_one):
    vm = pl.BlockSpec(memory_space=pltpu.VMEM)
    hbm = pl.BlockSpec(memory_space=pl.ANY)
    rows_d = pltpu.VMEM((E, ROWS, D), BF16)
    rows_f = pltpu.VMEM((E, ROWS, F), BF16)
    sums = pltpu.VMEM((TOK, D), F32)
    saved = (rows_d, rows_d, rows_f, rows_f, rows_f)
    w_up = pltpu.VMEM((E, D, F), BF16)
    w_dn = pltpu.VMEM((E, F, D), BF16)
    dma = pltpu.SemaphoreType.DMA
    return pl.pallas_call(
        main_kernel,
        out_shape=(sums, pltpu.VMEM((TOK, D), BF16), sums, sums, sums) + saved + saved,
        in_specs=[hbm] * 15,
        out_specs=(vm,) * 15,
        scratch_shapes=[
            (w_up, w_up, w_dn, w_up, w_up, w_dn),
            w_dn,
            pltpu.VMEM((4, 8, TOK), jnp.int32),
            pltpu.VMEM((2, 8, TOK), F32),
            pltpu.VMEM((16, 2 * TOK), F32),
            pltpu.VMEM((DEVS, 16, 2 * TOK), F32),
            pltpu.VMEM((2, DEVS, TOK, HW), BF16),
            pltpu.VMEM((2, DEVS, TOK, HW), BF16),
            pltpu.VMEM((DEVS, TOK, D), BF16),
            pltpu.VMEM((CH, DEVS, TOK, CW), BF16),
            pltpu.VMEM((E, ROWS, F), F32),
            pltpu.VMEM((E, ROWS, F), F32),
            pltpu.VMEM((E, ROWS, F), F32),
            pltpu.VMEM((2, CHIPS, E, PAIR, CW), BF16),
            pltpu.VMEM((CHIPS, PROWS, 2 * TOK), BF16),
            pltpu.VMEM((CHIPS, 2 * TOK, PROWS), BF16),
            pltpu.VMEM((CHIPS, PROWS, 1), F32),
            pltpu.VMEM((2, CH, 2, CHIPS, TOK, CW), F32),
            pltpu.VMEM((2, CH, CHIPS, TOK, CW), F32),
            pltpu.VMEM((CH, 2, TOK, CW), F32),
            pltpu.VMEM((CH, TOK, CW), F32),
            dma((2,)),
            dma((5,)),
            dma((6,)),
            dma((S_D1 + 4,)),
            dma((N_STREAMS, 4)),
            dma((2, CH)),
            dma((CH, 2)),
            dma((CH,)),
        ],
        compiler_params=pltpu.CompilerParams(collective_id=0, has_side_effects=True, vmem_limit_bytes=MAIN_VMEM),
        name="moe_backward",
    )(*routing, x, y, dy, *weights_two, *weights_one)


def wgrad_kernel(*refs):
    saved, outs, bufs, out_sem = (refs[0:5], refs[5:10]), (refs[10:13], refs[13:16]), refs[16:19], refs[19]

    def out_copy(layer, m, e, slot, h):
        n = bufs[m].shape[1] // HALVES
        rows = pl.ds(h * n, n)
        return pltpu.make_async_copy(bufs[m].at[slot, rows], outs[layer][m].at[e, rows], out_sem.at[slot, m, h])

    for layer in range(2):
        xr, zr, hid, da, db = saved[layer]

        @pl.loop(0, E)
        def _(e):
            i = layer * E + e
            slot = lax.rem(i, SETS)
            for m, lhs, rhs in ((2, hid, zr), (0, xr, da), (1, xr, db)):
                n = bufs[m].shape[1] // HALVES
                for h in range(HALVES):
                    rows = slice(h * n, (h + 1) * n)

                    @pl.when(i >= SETS)
                    def _():
                        out_copy(layer, m, e, slot, h).wait()

                    bufs[m][slot, rows] = tn_dot(lhs[e, :, rows], rhs[e])
                    out_copy(layer, m, e, slot, h).start()

    for i in range(2 * E - SETS, 2 * E):
        for m in (2, 0, 1):
            for h in range(HALVES):
                out_copy(i // E, m, i % E, i % SETS, h).wait()


def wgrad_call(*saved):
    up = jax.ShapeDtypeStruct((E, D, F), F32)
    dn = jax.ShapeDtypeStruct((E, F, D), F32)
    hbm = pl.BlockSpec(memory_space=pl.ANY)
    return pl.pallas_call(
        wgrad_kernel,
        out_shape=(up, up, dn) * 2,
        in_specs=[pl.BlockSpec(memory_space=pltpu.VMEM)] * 10,
        out_specs=(hbm,) * 6,
        scratch_shapes=[
            pltpu.VMEM((SETS, D, F), F32),
            pltpu.VMEM((SETS, D, F), F32),
            pltpu.VMEM((SETS, F, D), F32),
            pltpu.SemaphoreType.DMA((SETS, 3, HALVES)),
        ],
        compiler_params=pltpu.CompilerParams(vmem_limit_bytes=WGRAD_VMEM),
        cost_estimate=pl.CostEstimate(flops=12 * E * ROWS * D * F, bytes_accessed=24 * E * D * F, transcendentals=0),
        name="weight_grads",
    )(*saved)


def solution(mesh):
    tok_spec = P(("data", "expert"), None)
    weight_spec = P("expert", None, None)
    grad_spec = P(("data", "expert"), None, None)

    def local_step(x_tokens, y_mid, dy_out, experts_one, gates_one, slots_one, experts_two, gates_two, slots_two, w_gate_one, w_up_one, w_down_one, w_gate_two, w_up_two, w_down_two):
        routing = [a.T for a in (experts_two, gates_two, slots_two, experts_one, gates_one, slots_one)]
        got = main_call(routing, x_tokens, y_mid, dy_out, (w_gate_two, w_up_two, w_down_two), (w_gate_one, w_up_one, w_down_one))
        own, d1 = got[0:2]
        far = [lax.ppermute(got[2 + i], "expert", [(d, d ^ flip) for d in range(DEVS)]) for i, flip in enumerate((2, 4, 6))]
        grads = wgrad_call(*got[5:15])
        dx = (d1.astype(F32) + (own + (far[0] + far[1] + far[2]))).astype(BF16)
        return (dx,) + tuple(grads[3:6]) + tuple(grads[0:3])

    return jax.shard_map(local_step, mesh=mesh, in_specs=(tok_spec,) * 9 + (weight_spec,) * 6, out_specs=(tok_spec,) + (grad_spec,) * 6, check_vma=False)
```

```python
import functools
import jax
import jax.numpy as jnp
from jax import lax
from jax.experimental import pallas as pl
from jax.experimental.pallas import tpu as pltpu
from jax.sharding import PartitionSpec as P

MESH = pl.DeviceIdType.MESH
scope = jax.named_scope
F32 = jnp.float32
BF16 = jnp.bfloat16

TOK = 64
CHIPS = 4
DEVS = 8
D = 1024
F = 512
E = 4
CAP = 24
PAIR = 2 * CAP
ROWS = CHIPS * PAIR
PROWS = E * PAIR
CH = 4
CW = D // CH
MAIN_VMEM = 51_000_000
WGRAD_VMEM = 40_000_000

S_ROUTE, S_Y, S_DY, S_X, S_D1 = 0, 1, 3, 5, 6
N_STREAMS = S_D1 + CH
HW = D // 2

SETS = 2
HALVES = 1


def nt_dot(a, b):
    return lax.dot_general(a, b, (((1,), (1,)), ((), ())), preferred_element_type=F32)


def tn_dot(a, b):
    return lax.dot_general(a, b, (((0,), (0,)), ((), ())), preferred_element_type=F32)


def nn_dot(a, b):
    return jnp.dot(a, b, preferred_element_type=F32)


def main_kernel(
    experts_b, gates_b, slots_b, experts_a, gates_a, slots_a,
    x_hbm, y_hbm, dy_hbm, w1b_hbm, w3b_hbm, w2b_hbm, w1a_hbm, w3a_hbm, w2a_hbm,
    own_ref, d1_ref, far0_ref, far1_ref, far2_ref,
    xr_two, zr_two, hid_two, da_two, db_two, xr_one, zr_one, hid_one, da_one, db_one,
    w_vm, w3_turned, choice_i, choice_f, route_own, route_g, y_g, dy_g, x_g, d1_g,
    act_s, act_f, dh_sum, dxp, perm, perm_t, gate,
    part, mate_recv, near_recv, last_recv,
    choice_sem, tile_sem, w_sem, send_sem, ag_recv, mate_sem, near_sem, last_sem,
):
    xr, zr, hid = (xr_two, xr_one), (zr_two, zr_one), (hid_two, hid_one)
    da, db = (da_two, da_one), (db_two, db_one)
    me = lax.axis_index("expert")
    core = lax.rem(me, 2)
    xpos = lax.rem(me // 2, 2)
    ypos = me // 4
    mate = me + 1 - 2 * core
    nx = me + 2 - 4 * xpos
    ny = me + 4 - 8 * ypos
    nd = ny + 2 - 4 * xpos
    na = nx + core * (ny - nx)
    nb = ny + core * (nx - ny)

    def remote(src, dst, send, recv, dev):
        return pltpu.make_async_remote_copy(src_ref=src, dst_ref=dst, send_sem=send, recv_sem=recv, device_id={"expert": dev}, device_id_type=MESH)

    barrier = pltpu.get_barrier_semaphore()
    for dev in (mate, nx, ny, nd):
        pl.semaphore_signal(barrier, inc=1, device_id={"expert": dev}, device_id_type=MESH)

    choices = [
        pltpu.make_async_copy(src, dst, choice_sem.at[i])
        for i, src, dst in (
            (0, experts_b, choice_i.at[0]), (0, slots_b, choice_i.at[1]), (1, gates_b, choice_f.at[0]),
            (0, experts_a, choice_i.at[2]), (0, slots_a, choice_i.at[3]), (1, gates_a, choice_f.at[1]),
        )
    ]
    tiles = [
        pltpu.make_async_copy(src, dst.at[me], tile_sem.at[i])
        for i, (src, dst) in enumerate((
            (y_hbm.at[:, pl.ds(0, HW)], y_g.at[0]), (y_hbm.at[:, pl.ds(HW, HW)], y_g.at[1]),
            (dy_hbm.at[:, pl.ds(0, HW)], dy_g.at[0]), (dy_hbm.at[:, pl.ds(HW, HW)], dy_g.at[1]), (x_hbm, x_g),
        ))
    ]
    w_hbm = (w1b_hbm, w3b_hbm, w2b_hbm, w1a_hbm, w3a_hbm, w2a_hbm)

    def w_copy(i):
        return pltpu.make_async_copy(w_hbm[i], w_vm[i], w_sem.at[i])

    for c in choices + tiles:
        c.start()

    for i, whole in enumerate((choice_i, choice_f)):
        pltpu.make_async_copy(whole, whole, choice_sem.at[i]).wait()
    for layer in range(2):
        lanes = slice(layer * TOK, (layer + 1) * TOK)
        slot = choice_i[2 * layer + 1]
        code = jnp.where(slot >= 0, choice_i[2 * layer] * PAIR + core * CAP + slot, -1).astype(F32)
        route_own[0:8, lanes] = code
        route_own[8:16, lanes] = choice_f[layer]
    route_g[me] = route_own[...]
    for c in tiles:
        c.wait()
    pl.semaphore_wait(barrier, 4)

    far = ((0, na), (1, nb), (3, nd))

    def ag_send(stream, k, src, dst, dev):
        remote(src, dst, send_sem.at[min(stream, S_D1)], ag_recv.at[stream, k], dev).start()

    def ag_start(stream, src, buf):
        for k, dev in far + ((2, mate),):
            ag_send(stream, k, src, buf.at[me], dev)

    def ag_got(stream, k, buf):
        remote(buf, buf, send_sem.at[min(stream, S_D1)], ag_recv.at[stream, k], mate).wait_recv()

    def ag_pass_on(stream, buf):
        for k, dev in far:
            ag_got(stream, k, buf.at[dev])
            ag_send(stream, 2, buf.at[dev], buf.at[dev], mate)

    def ag_finish(stream, buf):
        ag_got(stream, 2, buf.at[pl.ds(0, CHIPS)])

    def ring_start(stream, buf):
        for k, dev in ((0, na), (1, nb), (2, mate)):
            ag_send(stream, k, buf.at[me], buf.at[me], dev)

    def ring_step(stream, buf):
        ag_got(stream, 0, buf.at[na])
        ag_send(stream, 3, buf.at[na], buf.at[na], nb)
        ag_send(stream, 2, buf.at[na], buf.at[na], mate)
        ag_got(stream, 1, buf.at[nb])
        ag_send(stream, 2, buf.at[nb], buf.at[nb], mate)

    def ring_last(stream, buf):
        ag_got(stream, 3, buf.at[nd])
        ag_send(stream, 2, buf.at[nd], buf.at[nd], mate)

    def build_routes(layer):
        base = (me * PROWS).astype(F32)
        row_id = lax.broadcasted_iota(jnp.int32, (PROWS, 2 * TOK), 0).astype(F32)
        lane = lax.broadcasted_iota(jnp.int32, (16, 2 * TOK), 1)
        for p in range(CHIPS):
            halves = [route_g[2 * p], route_g[2 * p + 1]]
            halves[1 - layer] = pltpu.roll(halves[1 - layer], TOK, 1)
            both = jnp.where(lane < TOK, halves[0], halves[1])
            target = both[0:8] - base
            gates = both[8:16]
            hit = jnp.zeros((PROWS, 2 * TOK), F32)
            gsum = jnp.zeros((PROWS, 2 * TOK), F32)
            for j in range(8):
                m = row_id == target[j : j + 1, :]
                hit = jnp.where(m, 1.0, hit)
                gsum = jnp.where(m, gates[j : j + 1, :], gsum)
            perm[p] = hit.astype(BF16)
            perm_t[p] = hit.T.astype(BF16)
            gate[p] = jnp.sum(gsum, axis=1, keepdims=True)

    def gather_rows(tokens, dst, layer, cols, gated):
        for p in range(CHIPS):
            got = nn_dot(perm[p], tokens(p))
            if gated:
                got = got * gate[p]
            got = got.astype(BF16)
            for e in range(E):
                dst[layer][e, p * PAIR : (p + 1) * PAIR, cols] = got[e * PAIR : (e + 1) * PAIR]

    def activate(layer, e, a, b):
        a = a.astype(BF16).astype(F32)
        b = b.astype(BF16).astype(F32)
        sig = jax.nn.sigmoid(a)
        s = a * sig
        act_s[e] = s
        act_f[e] = b * (sig * (1.0 + a * (1.0 - sig)))
        hid[layer][e] = (s * b).astype(BF16)

    def forward_expert(layer, e):
        rows = xr[layer][e]
        activate(layer, e, nn_dot(rows, w_vm[3 * layer][e]), nn_dot(rows, w_vm[3 * layer + 1][e]))

    def forward_half(e, h):
        cols = slice(h * HW, (h + 1) * HW)
        a = nn_dot(xr[0][e, :, cols], w_vm[0][e, cols, :])
        b = nn_dot(xr[0][e, :, cols], w_vm[1][e, cols, :])
        if h == 0:
            act_s[e] = a
            act_f[e] = b
        else:
            activate(0, e, act_s[e] + a, act_f[e] + b)

    def hidden_expert(layer, e, dh):
        da[layer][e] = (dh * act_f[e]).astype(BF16)
        db[layer][e] = (dh * act_s[e]).astype(BF16)

    w2_turned, w1_turned = w_vm[3], w_vm[2]

    def turn_two(experts):
        with scope("turn_two"):
            for e in experts:
                w2_turned[e] = w_vm[2][e].T

    def turn_one(tasks):
        with scope("turn_one"):
            for e, src, dst in tasks:
                dst[e] = src[e].T

    def row_chunk(layer, k):
        w1, w3 = w_vm[3 * layer], w_vm[3 * layer + 1]
        cols = slice(k * CW, (k + 1) * CW)
        for e in range(E):
            if layer == 0:
                g = nt_dot(da[0][e], w1[e, cols, :]) + nt_dot(db[0][e], w3[e, cols, :])
            else:
                g = nn_dot(da[1][e], w1_turned[e, :, cols]) + nn_dot(db[1][e], w3_turned[e, :, cols])
            g = g.astype(BF16)
            for p in range(CHIPS):
                dxp[k % 2, p, e] = g[p * PAIR : (p + 1) * PAIR]
        for p in range(CHIPS):
            r = nn_dot(perm_t[p], dxp[k % 2, p].reshape(PROWS, CW))
            part[layer, k, 0, p] = r[:TOK]
            part[layer, k, 1, p] = r[TOK:]
        mate_copy(layer, k).start()

    def mate_copy(layer, k):
        return remote(part.at[layer, k, 1 - core], mate_recv.at[layer, k], send_sem.at[S_D1 + 1], mate_sem.at[layer, k], mate)

    def near_copy(k, i):
        return remote(part.at[0, k, core, (nd, na)[i] // 2], near_recv.at[k, i], send_sem.at[S_D1 + 2], near_sem.at[k, i], na)

    def last_copy(k):
        return remote(part.at[0, k, core, nb // 2], last_recv.at[k], send_sem.at[S_D1 + 3], last_sem.at[k], nb)

    def near_start(k):
        mate_copy(0, k).wait_recv()
        for p in range(CHIPS):
            part[0, k, core, p] = part[0, k, core, p] + mate_recv[0, k, p]
        near_copy(k, 0).start()
        near_copy(k, 1).start()

    def last_start(k):
        near_copy(k, 0).wait_recv()
        part[0, k, core, nb // 2] = part[0, k, core, nb // 2] + near_recv[k, 0]
        last_copy(k).start()

    def sums_out(k):
        mate_copy(1, k).wait_recv()
        cols = slice(k * CW, (k + 1) * CW)
        for dev, out in ((me, own_ref), (nx, far0_ref), (ny, far1_ref), (nd, far2_ref)):
            out[:, cols] = part[1, k, core, dev // 2] + mate_recv[1, k, dev // 2]

    def pair_of(buf, p):
        return buf[2 * p : 2 * p + 2].reshape(2 * TOK, buf.shape[-1])

    with scope("start"):
        ag_start(S_ROUTE, route_own, route_g)
        for h in range(2):
            ring_start(S_Y + h, y_g.at[h])
        for h in range(2):
            ring_start(S_DY + h, dy_g.at[h])
        for i in (2, 0, 1, 4, 5):
            w_copy(i).start()

    def y_step(h):
        with scope(f"y_step_{h}"):
            ring_step(S_Y + h, y_g.at[h])

    def y_last(h):
        with scope(f"y_last_{h}"):
            ring_last(S_Y + h, y_g.at[h])

    def dy_step(h):
        with scope(f"dy_step_{h}"):
            ring_step(S_DY + h, dy_g.at[h])

    def dy_last(h):
        with scope(f"dy_last_{h}"):
            ring_last(S_DY + h, dy_g.at[h])

    def half_cols(h):
        return slice(h * HW, (h + 1) * HW)

    def y_rows(h):
        with scope(f"y_finish_{h}"):
            ag_finish(S_Y + h, y_g.at[h])
        with scope(f"rows_y_{h}"):
            gather_rows(lambda p: pair_of(y_g.at[h], p), xr, 0, half_cols(h), False)

    def dy_rows(h):
        with scope(f"dy_finish_{h}"):
            ag_finish(S_DY + h, dy_g.at[h])
        with scope(f"rows_dy_{h}"):
            gather_rows(lambda p: pair_of(dy_g.at[h], p), zr, 0, half_cols(h), True)

    def forward_part(h, experts):
        with scope(f"forward_two_{h}"):
            for e in experts:
                forward_half(e, h)

    with scope("route"):
        ag_pass_on(S_ROUTE, route_g)
        ag_finish(S_ROUTE, route_g)
    y_step(0)
    y_step(1)
    with scope("build_two"):
        build_routes(0)
    w_copy(2).wait()
    turn_two((0,))
    dy_step(0)
    turn_two((1, 2))
    y_last(0)
    turn_two((3,))
    dy_step(1)
    y_last(1)
    for i in range(2):
        w_copy(i).wait()
    y_rows(0)
    forward_part(0, range(E))
    dy_last(0)
    with scope("x_start"):
        ag_start(S_X, x_g.at[me], x_g)
    y_rows(1)
    forward_part(1, range(2))
    dy_last(1)
    forward_part(1, range(2, E))
    dy_rows(0)
    dy_rows(1)
    with scope("hidden_two"):
        for e in range(E):
            hidden_expert(0, e, nn_dot(zr[0][e], w2_turned[e]))
        w_copy(3).start()

    turns = [(e, w_vm[4], w3_turned) for e in range(E)] + [(e, w_vm[3], w1_turned) for e in range(E)]
    for k in range(CH):
        with scope(f"chunk_two_{k}"):
            row_chunk(0, k)
        if k == 3:
            w_copy(4).wait()
            turn_one(turns[0:1])
        if k >= 1:
            with scope(f"near_{k - 1}"):
                near_start(k - 1)
    turn_one(turns[1:3])
    with scope(f"near_{CH - 1}"):
        near_start(CH - 1)

    def last_step(k):
        with scope(f"last_{k}"):
            last_start(k)

    def x_wait():
        with scope("wait_x"):
            ag_pass_on(S_X, x_g)

    def x_build():
        with scope("build_one"):
            build_routes(1)

    def x_rows():
        with scope("rows_x"):
            ag_finish(S_X, x_g)
            gather_rows(lambda p: pair_of(x_g, p), xr, 1, slice(None), False)
            w_copy(5).wait()

    def ring_one(k):
        with scope(f"step_{k}"):
            ring_step(S_D1 + k, d1_g.at[k])

    def ring_two(k):
        with scope(f"last_d1_{k}"):
            ring_last(S_D1 + k, d1_g.at[k])

    def mid_grad(k):
        cols = slice(k * CW, (k + 1) * CW)
        near_copy(k, 1).wait_recv()
        last_copy(k).wait_recv()
        total = part[0, k, core, me // 2] + near_recv[k, 1] + last_recv[k]
        mine = (dy_g[k // 2, me, :, (k % 2) * CW : (k % 2 + 1) * CW].astype(F32) + total).astype(BF16)
        d1_ref[:, cols] = mine
        d1_g[k, me] = mine
        if k < 1:
            ring_start(S_D1 + k, d1_g.at[k])
        else:
            ag_start(S_D1 + k, d1_g.at[k, me], d1_g.at[k])

    def mid_rows(k):
        cols = slice(k * CW, (k + 1) * CW)
        gather_rows(lambda p: pair_of(d1_g.at[k], p), zr, 1, cols, True)

    parts_done = []

    def hidden_part(k):
        cols = slice(k * CW, (k + 1) * CW)
        parts_done.append(k)
        for e in range(E):
            dh = nt_dot(zr[1][e, :, cols], w_vm[5][e, :, cols])
            if len(parts_done) > 1:
                dh = dh_sum[e] + dh
            if len(parts_done) < CH:
                dh_sum[e] = dh
            else:
                hidden_expert(1, e, dh)

    def mid_step(k):
        with scope(f"mid_{k}"):
            mid_grad(k)

    def pass_step(k):
        with scope(f"pass_on_{k}"):
            ag_pass_on(S_D1 + k, d1_g.at[k])

    def rows_step(k):
        with scope(f"finish_{k}"):
            ag_finish(S_D1 + k, d1_g.at[k])
        with scope(f"rows_d1_{k}"):
            mid_rows(k)
            hidden_part(k)

    def forward_step(k):
        with scope(f"forward_one_{k}"):
            forward_expert(1, k)

    last_step(0)
    x_wait()
    x_build()
    turn_one(turns[3:4])
    w_copy(3).wait()
    last_step(1)
    turn_one(turns[4:5])
    x_rows()
    turn_one(turns[5:6])
    last_step(2)
    turn_one(turns[6:7])
    mid_step(0)
    forward_step(0)
    turn_one(turns[7:8])
    last_step(3)
    mid_step(1)
    mid_step(2)
    forward_step(1)
    ring_one(0)
    forward_step(2)
    mid_step(3)
    forward_step(3)
    pass_step(1)
    pass_step(2)
    ring_two(0)
    rows_step(1)
    pass_step(3)
    rows_step(2)
    rows_step(0)
    rows_step(3)
    for k in range(CH):
        with scope(f"chunk_one_{k}"):
            row_chunk(1, k)
        if k >= 2:
            with scope(f"mate_one_{k - 2}"):
                sums_out(k - 2)
    with scope("mate_one_late"):
        sums_out(CH - 2)
    with scope("mate_one_last"):
        sums_out(CH - 1)
    with scope("drain"):
        seven = pl.ds(0, DEVS - 1)
        sent = (
            (S_ROUTE, route_g.at[seven]), (S_Y, y_g.at[0, seven]), (S_Y + 1, y_g.at[1, seven]), (S_DY, dy_g.at[0, seven]), (S_DY + 1, dy_g.at[1, seven]), (S_X, x_g.at[seven]), (S_D1, d1_g.at[:, seven]),
            (S_D1 + 1, mate_recv), (S_D1 + 2, near_recv), (S_D1 + 3, last_recv),
        )
        for i, whole in sent:
            remote(whole, whole, send_sem.at[i], ag_recv.at[0, 0], mate).wait_send()


def main_call(routing, x, y, dy, weights_two, weights_one):
    vm = pl.BlockSpec(memory_space=pltpu.VMEM)
    hbm = pl.BlockSpec(memory_space=pl.ANY)
    rows_d = pltpu.VMEM((E, ROWS, D), BF16)
    rows_f = pltpu.VMEM((E, ROWS, F), BF16)
    sums = pltpu.VMEM((TOK, D), F32)
    saved = (rows_d, rows_d, rows_f, rows_f, rows_f)
    w_up = pltpu.VMEM((E, D, F), BF16)
    w_dn = pltpu.VMEM((E, F, D), BF16)
    dma = pltpu.SemaphoreType.DMA
    return pl.pallas_call(
        main_kernel,
        out_shape=(sums, pltpu.VMEM((TOK, D), BF16), sums, sums, sums) + saved + saved,
        in_specs=[hbm] * 15,
        out_specs=(vm,) * 15,
        scratch_shapes=[
            (w_up, w_up, w_dn, w_up, w_up, w_dn),
            w_dn,
            pltpu.VMEM((4, 8, TOK), jnp.int32),
            pltpu.VMEM((2, 8, TOK), F32),
            pltpu.VMEM((16, 2 * TOK), F32),
            pltpu.VMEM((DEVS, 16, 2 * TOK), F32),
            pltpu.VMEM((2, DEVS, TOK, HW), BF16),
            pltpu.VMEM((2, DEVS, TOK, HW), BF16),
            pltpu.VMEM((DEVS, TOK, D), BF16),
            pltpu.VMEM((CH, DEVS, TOK, CW), BF16),
            pltpu.VMEM((E, ROWS, F), F32),
            pltpu.VMEM((E, ROWS, F), F32),
            pltpu.VMEM((E, ROWS, F), F32),
            pltpu.VMEM((2, CHIPS, E, PAIR, CW), BF16),
            pltpu.VMEM((CHIPS, PROWS, 2 * TOK), BF16),
            pltpu.VMEM((CHIPS, 2 * TOK, PROWS), BF16),
            pltpu.VMEM((CHIPS, PROWS, 1), F32),
            pltpu.VMEM((2, CH, 2, CHIPS, TOK, CW), F32),
            pltpu.VMEM((2, CH, CHIPS, TOK, CW), F32),
            pltpu.VMEM((CH, 2, TOK, CW), F32),
            pltpu.VMEM((CH, TOK, CW), F32),
            dma((2,)),
            dma((5,)),
            dma((6,)),
            dma((S_D1 + 4,)),
            dma((N_STREAMS, 4)),
            dma((2, CH)),
            dma((CH, 2)),
            dma((CH,)),
        ],
        compiler_params=pltpu.CompilerParams(collective_id=0, has_side_effects=True, vmem_limit_bytes=MAIN_VMEM),
        name="moe_backward",
    )(*routing, x, y, dy, *weights_two, *weights_one)


def wgrad_kernel(*refs):
    saved, outs, bufs, out_sem = (refs[0:5], refs[5:10]), (refs[10:13], refs[13:16]), refs[16:19], refs[19]

    def out_copy(layer, m, e, slot, h):
        n = bufs[m].shape[1] // HALVES
        rows = pl.ds(h * n, n)
        return pltpu.make_async_copy(bufs[m].at[slot, rows], outs[layer][m].at[e, rows], out_sem.at[slot, m, h])

    quarter = F // 4
    for q in range(4):
        rows = slice(q * quarter, (q + 1) * quarter)
        bufs[2][0, rows] = tn_dot(saved[0][2][0, :, rows], saved[0][1][0])
        pltpu.make_async_copy(bufs[2].at[0, pl.ds(q * quarter, quarter)], outs[0][2].at[0, pl.ds(q * quarter, quarter)], out_sem.at[0, 2, 0]).start()

    for layer in range(2):
        xr, zr, hid, da, db = saved[layer]

        @pl.loop(0, E)
        def _(e):
            i = layer * E + e
            slot = lax.rem(i, SETS)
            for m, lhs, rhs in ((2, hid, zr), (0, xr, da), (1, xr, db)):
                n = bufs[m].shape[1] // HALVES
                for h in range(HALVES):
                    rows = slice(h * n, (h + 1) * n)

                    @pl.when(i >= SETS)
                    def _():
                        out_copy(layer, m, e, slot, h).wait()

                    def make():
                        bufs[m][slot, rows] = tn_dot(lhs[e, :, rows], rhs[e])
                        out_copy(layer, m, e, slot, h).start()

                    if (layer, m) == (0, 2):
                        pl.when(e > 0)(make)
                    else:
                        make()

    for i in range(2 * E - SETS, 2 * E):
        for m in (2, 0, 1):
            for h in range(HALVES):
                out_copy(i // E, m, i % E, i % SETS, h).wait()


def wgrad_call(*saved):
    up = jax.ShapeDtypeStruct((E, D, F), F32)
    dn = jax.ShapeDtypeStruct((E, F, D), F32)
    hbm = pl.BlockSpec(memory_space=pl.ANY)
    return pl.pallas_call(
        wgrad_kernel,
        out_shape=(up, up, dn) * 2,
        in_specs=[pl.BlockSpec(memory_space=pltpu.VMEM)] * 10,
        out_specs=(hbm,) * 6,
        scratch_shapes=[
            pltpu.VMEM((SETS, D, F), F32),
            pltpu.VMEM((SETS, D, F), F32),
            pltpu.VMEM((SETS, F, D), F32),
            pltpu.SemaphoreType.DMA((SETS, 3, HALVES)),
        ],
        compiler_params=pltpu.CompilerParams(vmem_limit_bytes=WGRAD_VMEM),
        cost_estimate=pl.CostEstimate(flops=12 * E * ROWS * D * F, bytes_accessed=24 * E * D * F, transcendentals=0),
        name="weight_grads",
    )(*saved)


def solution(mesh):
    tok_spec = P(("data", "expert"), None)
    weight_spec = P("expert", None, None)
    grad_spec = P(("data", "expert"), None, None)

    def local_step(x_tokens, y_mid, dy_out, experts_one, gates_one, slots_one, experts_two, gates_two, slots_two, w_gate_one, w_up_one, w_down_one, w_gate_two, w_up_two, w_down_two):
        routing = [a.T for a in (experts_two, gates_two, slots_two, experts_one, gates_one, slots_one)]
        got = main_call(routing, x_tokens, y_mid, dy_out, (w_gate_two, w_up_two, w_down_two), (w_gate_one, w_up_one, w_down_one))
        own, d1 = got[0:2]
        far = [lax.ppermute(got[2 + i], "expert", [(d, d ^ flip) for d in range(DEVS)]) for i, flip in enumerate((2, 4, 6))]
        grads = wgrad_call(*got[5:15])
        dx = (d1.astype(F32) + (own + (far[0] + far[1] + far[2]))).astype(BF16)
        return (dx,) + tuple(grads[3:6]) + tuple(grads[0:3])

    return jax.shard_map(local_step, mesh=mesh, in_specs=(tok_spec,) * 9 + (weight_spec,) * 6, out_specs=(tok_spec,) + (grad_spec,) * 6, check_vma=False)
```
